16 devices in a mesh: dp: 2 (over z), tp: 8 (over y, x, core).
Axes of the slice: x: 2, y: 2, z: 2, core: 2. Of those that a mesh axis runs over, the one named last changes fastest.
Arguments:
- ids: int32 [4, 256], P('dp'), parts along dimension 0
- emb: bfloat16 [32768, 3072], P('tp')
- g: bfloat16 [3072], replicated
- w: bfloat16 [3072, 12288], P(None, 'tp')
- du: bfloat16 [4, 256, 12288], P('dp', None, 'tp'), parts along dimension 0
- dres: bfloat16 [4, 256, 3072], P('dp', 'tp'), parts along dimension 0
Outputs:
- output 1: bfloat16 [4, 256, 12288], P('dp', None, 'tp'), parts along dimension 0
- output 2: bfloat16 [4, 256, 3072], P('dp', 'tp'), parts along dimension 0
- output 3: float32 [65536, 3072], P(('dp', 'tp')), parts along dimension 0
- output 4: float32 [3072, 24576], P(None, ('dp', 'tp')), parts along dimension 1
- output 5: float32 [6144], P('dp'), parts along dimension 0
There are 2 independent parts. The reference program is written for one: setup_inputs(seed, part) draws one part's arguments, and reference() takes and returns one part's arrays. A program takes and returns all parts, laid end to end along the dimension named above; an argument that names none is the same for every part.
All inputs are finite; a program needn't handle non-finite values.
Results may differ from the reference program's by a relative error of at most 0.001.
Values are sent between devices in bfloat16 or wider.
A program may use at most 1 GiB of HBM per device.

```python
import jax
import jax.numpy as jnp
from jax import lax

K = 2
T = 256
V = 32768
D = 3072
FC = 12288
GROUP = 8
EPS = 1e-6
NPOOL = K * T // 16
FCG = FC // GROUP


def setup_inputs(seed: int = 0, part: int = 0) -> dict:
    key = jax.random.key(seed)
    kp = jax.random.fold_in(key, part)
    ke, kg, kw = jax.random.split(key, 3)
    k1, k2, k3, k4, k5, k6 = jax.random.split(kp, 6)
    ka, kb, kc = jax.random.split(jax.random.fold_in(kp, 7), 3)
    a = jax.random.randint(ka, (K, T), 0, V)
    b = jax.random.randint(kb, (K, T), 0, V)
    coin = jax.random.bernoulli(kc, 0.4, (K, T))
    ids = jnp.where(coin, a, jnp.minimum(a, b)).astype(jnp.int32)
    emb = jax.random.normal(ke, (V, D), jnp.float32).astype(jnp.bfloat16)
    g = (1.0 + 0.5 * jax.random.normal(kg, (D,), jnp.float32)).astype(jnp.bfloat16)
    w = (jax.random.normal(kw, (D, FC), jnp.float32) * D ** -0.5).astype(jnp.bfloat16)
    du = (jax.random.normal(k5, (K, T, FC), jnp.float32) * (D / FC) ** 0.5).astype(jnp.bfloat16)
    dres = jax.random.normal(k6, (K, T, D), jnp.float32).astype(jnp.bfloat16)
    return {"ids": ids, "emb": emb, "g": g, "w": w, "du": du, "dres": dres}


def reference(ids, emb, g, w, du, dres):
    gf = g.astype(jnp.float32)

    def micro(carry, inp):
        de, dw, dg = carry
        idm, dum, drm = inp
        x = emb[idm]
        xf = x.astype(jnp.float32)
        rs = lax.rsqrt(jnp.mean(xf * xf, axis=-1, keepdims=True) + EPS)
        nh = xf * rs
        n = (nh * gf).astype(jnp.bfloat16)
        u = jnp.dot(n, w, preferred_element_type=jnp.float32).astype(jnp.bfloat16)
        dn = jnp.zeros((T, D), jnp.float32)
        for j in range(GROUP):
            pb = jnp.dot(dum[:, j * FCG:(j + 1) * FCG], w[:, j * FCG:(j + 1) * FCG].T, preferred_element_type=jnp.float32)
            dn = dn + pb.astype(jnp.bfloat16).astype(jnp.float32)
        gdn = gf * dn
        dxn = rs * (gdn - nh * jnp.mean(nh * gdn, axis=-1, keepdims=True))
        dx = (drm.astype(jnp.float32) + dxn).astype(jnp.bfloat16)
        de = de.at[idm].add(dx.astype(jnp.float32))
        dw = dw + jnp.dot(n.T, dum, preferred_element_type=jnp.float32)
        dg = dg + jnp.sum(dn * nh, axis=0)
        return (de, dw, dg), (u, x)

    init = (jnp.zeros((V, D), jnp.float32), jnp.zeros((D, FC), jnp.float32), jnp.zeros((D,), jnp.float32))
    (de, dw, dg), (u, x) = lax.scan(micro, init, (ids, du, dres))
    return u, x, de, dw, dg
```

```python
import functools

import jax
import jax.numpy as jnp
from jax import lax
from jax.experimental import pallas as pl
from jax.experimental.pallas import tpu as pltpu
from jax.sharding import PartitionSpec as P

EPS = 1e-6
MESH = pl.DeviceIdType.MESH
F32 = jnp.float32
BF16 = jnp.bfloat16
ANY = pl.BlockSpec(memory_space=pl.ANY)
VM = pl.BlockSpec(memory_space=pltpu.VMEM)
SM = pl.BlockSpec(memory_space=pltpu.SMEM)
LIMIT = 60 * 1024 * 1024
NC = 6
HC = NC // 2


def gather_kernel(ids_ref, emb_ref, xp_ref, lst_ref, cnt_ref, buf, xf, sem):
    nt = ids_ref.shape[0]
    vl, d = emb_ref.shape
    cw = d // NC
    tm = nt // 2
    lo = lax.axis_index("tp") * vl

    def scan(t, n):
        loc = ids_ref[t] - lo
        lst_ref[n] = t
        own = jnp.logical_and(loc >= 0, loc < vl)
        return n + own.astype(jnp.int32)

    cnt = lax.fori_loop(0, nt, scan, jnp.int32(0), unroll=8)
    cnt_ref[0] = cnt

    def group(j):
        loc = ids_ref[lst_ref[j]] - lo
        return pltpu.make_async_copy(emb_ref.at[pl.ds(pl.multiple_of(loc // 8 * 8, 8), 8)], buf.at[j], sem)

    @pl.loop(0, cnt)
    def _(j):
        group(j).start()

    @pl.loop(0, nt // 16)
    def _(i):
        xf[pl.ds(pl.multiple_of(i * 16, 16), 16), :] = jnp.zeros((16, d), F32)

    @pl.loop(0, cnt)
    def _(j):
        group(j).wait()

    @pl.loop(0, cnt)
    def _(j):
        t = lst_ref[j]
        r = (ids_ref[t] - lo) % 8
        s = t % 8
        v = pltpu.roll(buf[j].astype(F32), (s - r + 8) % 8, 0)
        rows = pl.ds(pl.multiple_of(t // 8 * 8, 8), 8)
        mine = lax.broadcasted_iota(jnp.int32, (8, d), 0) == s
        xf[rows, :] = jnp.where(mine, v, xf[rows, :])

    for m in range(2):
        for k in range(NC):

            @pl.loop(0, tm // 64)
            def _(i):
                rows = pl.ds(pl.multiple_of(i * 64, 64), 64)
                src = pl.ds(pl.multiple_of(m * tm + i * 64, 64), 64)
                xp_ref[m, k, rows, :] = xf[src, k * cw : (k + 1) * cw].astype(BF16)


def rs_kernel(
    xp_ref, du_ref, w_ref, g_ref, dres_ref,
    xo_ref, na_ref, nb_ref, dxa_ref, dxb_ref, dgp_ref,
    xs, xr, xfw, x1, x2, xh, xpr, drr, drw, wv, duv, ps, po, pr, sf, rf, r1, r2,
    xv_s, du_s, w_s, dr_s, dr_r, xd_s, xd_r, xo_s, xo_r, pd_s, pd_r,
    xa_s, xb_s, xc_s, xa_r, xb_r, xc_r, da_s, db_s, dc_s, da_r, db_r, dc_r,
):
    me = lax.axis_index("tp")
    c = me % 2
    q = me // 2
    xq = q % 2
    yq = q // 2
    qx = q + 1 - 2 * xq
    qy = q + 2 - 4 * yq
    qd = 3 - q
    part = me + 1 - 2 * c
    dx_ = me + 2 - 4 * xq
    dy_ = me + 4 - 8 * yq
    oc = 1 - c
    d = w_ref.shape[0]
    cw = d // NC
    tq = xs.shape[2]
    th = tq // 2

    xv_copy = pltpu.make_async_copy(xp_ref.at[c], xs, xv_s)
    du_copy = pltpu.make_async_copy(du_ref, duv, du_s)

    def w_copy(k):
        rows = pl.ds(pl.multiple_of(k * cw, cw), cw)
        return pltpu.make_async_copy(w_ref.at[rows], wv.at[k], w_s.at[k])

    def chunk(i):
        return i % 2 * HC + i // 2

    xv_copy.start()
    du_copy.start()

    @pl.loop(0, NC)
    def _(i):
        w_copy(chunk(i)).start()

    barrier = pltpu.get_barrier_semaphore()
    for dev in (part, dx_, dy_):
        pl.semaphore_signal(barrier, inc=1, device_id={"tp": dev}, device_id_type=MESH)
    pl.semaphore_wait(barrier, 3)

    def remote(src, dst, ss, rs, dev):
        return pltpu.make_async_remote_copy(
            src_ref=src, dst_ref=dst, send_sem=ss, recv_sem=rs, device_id={"tp": dev}, device_id_type=MESH
        )

    def xd(k):
        return remote(xp_ref.at[oc, k], xr.at[k], xd_s.at[k], xd_r.at[k], part)

    dr = remote(dres_ref.at[oc], drr, dr_s, dr_r, part)

    @pl.loop(0, NC)
    def _(i):
        xd(chunk(i)).start()

    dr.start()

    def first(k):
        b = k // HC
        return qx + (qy - qx) * b, dx_ + (dy_ - dx_) * b

    def second(k):
        b = k // HC
        return qy + (qx - qy) * b, dy_ + (dx_ - dy_) * b

    def xa(k):
        return remote(xs.at[k, qd], xfw.at[k], xa_s.at[k], xa_r.at[k], first(k)[1])

    def xb(k):
        return remote(xs.at[k, first(k)[0]], x1.at[k], xb_s.at[k], xb_r.at[k], first(k)[1])

    def xc(k):
        return remote(xs.at[k, second(k)[0]], x2.at[k], xc_s.at[k], xc_r.at[k], second(k)[1])

    def da(k):
        return remote(sf.at[k, qd], rf.at[k], da_s.at[k], da_r.at[k], first(k)[1])

    def db(k):
        return remote(sf.at[k, first(k)[0]], r1.at[k], db_s.at[k], db_r.at[k], first(k)[1])

    def dc(k):
        return remote(sf.at[k, second(k)[0]], r2.at[k], dc_s.at[k], dc_r.at[k], second(k)[1])

    def pd(k):
        return remote(ps.at[k], pr.at[k], pd_s.at[k], pd_r.at[k], part)

    xv_copy.wait()

    @pl.loop(0, NC)
    def _(i):
        k = chunk(i)
        xd(k).wait_recv()
        xs[k] = xs[k] + xr[k]
        xa(k).start()

    @pl.loop(0, NC)
    def _(i):
        xb(chunk(i)).start()

    du_copy.wait()

    def matmul(i):
        k = chunk(i)
        w_copy(k).wait()
        nt = (((1,), (1,)), ((), ()))
        mine = lax.dot_general(duv[oc], wv[k], nt, preferred_element_type=F32)
        ps[k] = mine.astype(BF16).reshape(4, tq, cw)
        pd(k).start()
        mine = lax.dot_general(duv[c], wv[k], nt, preferred_element_type=F32)
        po[k] = mine.astype(BF16).reshape(4, tq, cw)

    def combine(i):
        k = chunk(i)
        pd(k).wait_recv()
        for s in range(4):
            sf[k, s] = po[k, s].astype(F32) + pr[k, s].astype(F32)
        da(k).start()
        db(k).start()

    matmul(0)

    @pl.loop(1, NC)
    def _(i):
        matmul(i)
        combine(i - 1)

    combine(NC - 1)

    @pl.loop(0, NC)
    def _(i):
        k = chunk(i)
        s = second(k)[0]
        xa(k).wait_recv()
        xs[k, s] = xs[k, s] + xfw[k]
        xc(k).start()

    @pl.loop(0, NC)
    def _(i):
        k = chunk(i)
        s = second(k)[0]
        da(k).wait_recv()
        sf[k, s] = sf[k, s] + rf[k]
        dc(k).start()

    sq = jnp.zeros((tq, 1), F32)
    for k in range(NC):
        xb(k).wait_recv()
        xc(k).wait_recv()
        xk = xs[k, q] + x1[k] + x2[k]
        xh[k] = xk
        xk = xk.astype(F32)
        sq = sq + jnp.sum(xk * xk, axis=-1, keepdims=True)
    xo = remote(xh.at[:, pl.ds(pl.multiple_of(oc * th, th), th), :], xpr, xo_s, xo_r, part)
    xo.start()
    rs = lax.rsqrt(sq * (1.0 / d) + EPS)
    for k in range(NC):
        cols = slice(k * cw, (k + 1) * cw)
        nk = ((xh[k].astype(F32) * rs) * g_ref[:, cols].astype(F32)).astype(BF16)
        if k < HC:
            na_ref[k] = nk
        else:
            nb_ref[k - HC] = nk
        xo_ref[c, :, cols] = xh[k, pl.ds(pl.multiple_of(c * th, th), th), :]
    dr.wait_recv()
    drw[c] = dres_ref[c]
    drw[oc] = drr[...]
    xo.wait_recv()
    for k in range(NC):
        xo_ref[oc, :, k * cw : (k + 1) * cw] = xpr[k]

    m = jnp.zeros((tq, 1), F32)
    for k in range(NC):
        cols = slice(k * cw, (k + 1) * cw)
        db(k).wait_recv()
        dc(k).wait_recv()
        dn = sf[k, q] + r1[k] + r2[k]
        r1[k] = dn
        nh = xh[k].astype(F32) * rs
        dnh = dn * nh
        dgp_ref[:, cols] = jnp.sum(dnh, axis=0, keepdims=True)
        m = m + jnp.sum(dnh * g_ref[:, cols].astype(F32), axis=-1, keepdims=True)
    m = m * (1.0 / d)
    for k in range(NC):
        cols = slice(k * cw, (k + 1) * cw)
        nh = xh[k].astype(F32) * rs
        dxn = rs * (g_ref[:, cols].astype(F32) * r1[k] - nh * m)
        dr2 = drw[:, :, cols].reshape(tq, cw).astype(F32)
        dxk = (dr2 + dxn).astype(BF16)
        if k < HC:
            dxa_ref[k] = dxk
        else:
            dxb_ref[k - HC] = dxk

    dr.wait_send()
    xo.wait_send()

    @pl.loop(0, NC)
    def _(k):
        xd(k).wait_send()
        pd(k).wait_send()
        xa(k).wait_send()
        xb(k).wait_send()
        xc(k).wait_send()
        da(k).wait_send()
        db(k).wait_send()
        dc(k).wait_send()


def zero_kernel(out_ref, z, sem):
    z[...] = jnp.zeros_like(z)
    n = out_ref.shape[0] // z.shape[0]

    def put(i):
        rows = pl.ds(pl.multiple_of(i * z.shape[0], z.shape[0]), z.shape[0])
        return pltpu.make_async_copy(z, out_ref.at[rows], sem)

    @pl.loop(0, n)
    def _(i):
        put(i).start()

    @pl.loop(0, n)
    def _(i):
        put(i).wait()


def pieces(refs, dst, sem):
    me = lax.axis_index("tp")
    c = me % 2
    q = me // 2
    qx = q + 1 - 2 * (q % 2)
    qy = q + 2 - 4 * (q // 2)
    where = []
    for b in (c, 1 - c):
        for s in (q, qx, qy, 3 - q):
            for h in range(2):
                where.append((h, b, s))
    return [
        pltpu.make_async_copy(r, dst.at[pl.ds(h * HC, HC), b, s], sem) for r, (h, b, s) in zip(refs, where)
    ]


def uw_kernel(*refs):
    n_refs = refs[:16]
    w_ref, du_ref, u_ref, dw_ref, nv, wv, duv, acc, st, n_s, w_s, du_s, o_s = refs[16:]
    cw = wv.shape[1]
    nt = duv.shape[0]
    loads = pieces(n_refs, nv, n_s)
    for cp in loads:
        cp.start()
    du_copy = pltpu.make_async_copy(du_ref, duv, du_s)
    du_copy.start()

    def w_copy(k):
        rows = pl.ds(pl.multiple_of(k * cw, cw), cw)
        return pltpu.make_async_copy(w_ref.at[rows], wv.at[k], w_s.at[k])

    def out(k):
        rows = pl.ds(pl.multiple_of(k * cw, cw), cw)
        return pltpu.make_async_copy(st.at[k % 2], dw_ref.at[rows], o_s.at[k % 2])

    for k in range(NC):
        w_copy(k).start()
    for cp in loads:
        cp.wait()
    du_copy.wait()

    @pl.loop(0, NC)
    def _(k):
        nk = nv[k].reshape(nt, cw)

        @pl.when(k >= 2)
        def _():
            out(k - 2).wait()

        st[k % 2] = lax.dot_general(nk, duv[...], (((0,), (0,)), ((), ())), preferred_element_type=F32)
        out(k).start()
        w_copy(k).wait()
        part = jnp.dot(nk, wv[k], preferred_element_type=F32)

        @pl.when(k == 0)
        def _():
            acc[...] = part

        @pl.when(k > 0)
        def _():
            acc[...] += part

    u_ref[...] = acc[...].astype(BF16)
    out(NC - 2).wait()
    out(NC - 1).wait()


def rows_kernel(*refs):
    lst_ref, cnt_ref, ids_ref, one_ref, idr_ref, idc_ref = refs[:6]
    dx_refs = refs[6:22]
    _, de_ref, dxv, dxs, d_s, o_s = refs[22:]
    nt = ids_ref.shape[0]
    vl = de_ref.shape[0]
    cw = dxv.shape[-1]
    lo = lax.axis_index("tp") * vl
    loads = pieces(dx_refs, dxv, d_s)
    for cp in loads:
        cp.start()
    same = (idc_ref[...] == idr_ref[...]).astype(BF16)
    for cp in loads:
        cp.wait()
    for k in range(NC):
        dxs[:, k * cw : (k + 1) * cw] = jnp.dot(same, dxv[k].reshape(nt, cw), preferred_element_type=F32)
    cnt = cnt_ref[0]

    def put(j):
        t = lst_ref[j]
        return pltpu.make_async_copy(dxs.at[pl.ds(t, 1)], de_ref.at[pl.ds(ids_ref[t] - lo, 1)], o_s)

    @pl.loop(0, cnt)
    def _(j):
        @pl.when(one_ref[lst_ref[j]] > 0)
        def _():
            put(j).start()

    @pl.loop(0, cnt)
    def _(j):
        @pl.when(one_ref[lst_ref[j]] > 0)
        def _():
            put(j).wait()


def solution(mesh):
    groups = mesh.shape["tp"]

    def shift(bit):
        return [(r, r ^ bit) for r in range(groups)]

    def send(a, bit):
        return lax.ppermute(a, "tp", shift(bit))

    def spread(a, b):
        ax, bx, ay, by = send(a, 2), send(b, 2), send(a, 4), send(b, 4)
        ad, bd = send(ax, 4), send(by, 2)
        mine = [a, b, ax, bx, ay, by, ad, bd]
        return mine + [send(v, 1) for v in mine]

    def local(ids, emb, g, w, du, dres):
        mb, t = ids.shape
        vl, d = emb.shape
        f = w.shape[1]
        nt = mb * t
        cw = d // NC
        tq = t // 4
        flat = ids.reshape(nt)
        dma = pltpu.SemaphoreType.DMA

        xp, lst, cnt = pl.pallas_call(
            gather_kernel,
            out_shape=(
                jax.ShapeDtypeStruct((2, NC, t, cw), BF16),
                jax.ShapeDtypeStruct((nt + 8,), jnp.int32),
                jax.ShapeDtypeStruct((1,), jnp.int32),
            ),
            in_specs=[SM, ANY],
            out_specs=(VM, SM, SM),
            scratch_shapes=[pltpu.VMEM((nt, 8, d), BF16), pltpu.VMEM((nt, d), F32), dma(())],
            compiler_params=pltpu.CompilerParams(vmem_limit_bytes=LIMIT),
            name="gather",
        )(flat, emb)

        half = jax.ShapeDtypeStruct((HC, tq, cw), BF16)
        vb = lambda *s: pltpu.VMEM(s, BF16)
        vf = lambda *s: pltpu.VMEM(s, F32)
        x, na, nb, dxa, dxb, dgp = pl.pallas_call(
            rs_kernel,
            out_shape=(
                jax.ShapeDtypeStruct((2, tq // 2, d), BF16),
                half, half, half, half,
                jax.ShapeDtypeStruct((1, d), F32),
            ),
            in_specs=[ANY, ANY, ANY, VM, VM],
            out_specs=(VM,) * 6,
            scratch_shapes=[
                vb(NC, 4, tq, cw), vb(NC, 4, tq, cw), vb(NC, tq, cw), vb(NC, tq, cw), vb(NC, tq, cw),
                vb(NC, tq, cw), vb(NC, tq // 2, cw), vb(tq // 2, d), vb(2, tq // 2, d),
                vb(NC, cw, f), vb(2, t, f),
                vb(NC, 4, tq, cw), vb(NC, 4, tq, cw), vb(NC, 4, tq, cw),
                vf(NC, 4, tq, cw), vf(NC, tq, cw), vf(NC, tq, cw), vf(NC, tq, cw),
                dma(()), dma(()), dma((NC,)), dma(()), dma(()), dma((NC,)), dma((NC,)), dma(()), dma(()),
                dma((NC,)), dma((NC,)),
            ] + [dma((NC,))] * 12,
            compiler_params=pltpu.CompilerParams(
                collective_id=0, has_side_effects=True, vmem_limit_bytes=LIMIT
            ),
            name="reduce",
        )(xp.reshape(2, NC, 4, tq, cw), du, w, g.reshape(1, d), dres)

        de0 = pl.pallas_call(
            zero_kernel,
            out_shape=jax.ShapeDtypeStruct((vl, d), F32),
            out_specs=ANY,
            scratch_shapes=[vf(128, d), dma(())],
            compiler_params=pltpu.CompilerParams(vmem_limit_bytes=LIMIT, has_side_effects=True),
            cost_estimate=pl.CostEstimate(flops=14_000_000_000, bytes_accessed=vl * d * 4, transcendentals=0),
            name="zero",
        )()

        np_ = spread(na, nb)
        dp_ = spread(dxa, dxb)

        u, dw = pl.pallas_call(
            uw_kernel,
            out_shape=(jax.ShapeDtypeStruct((nt, f), BF16), jax.ShapeDtypeStruct((d, f), F32)),
            in_specs=[ANY] * 18,
            out_specs=(VM, ANY),
            scratch_shapes=[
                vb(NC, 2, 4, tq, cw), vb(NC, cw, f), vb(nt, f), vf(nt, f), vf(2, cw, f),
                dma(()), dma((NC,)), dma(()), dma((2,)),
            ],
            compiler_params=pltpu.CompilerParams(vmem_limit_bytes=LIMIT),
            cost_estimate=pl.CostEstimate(flops=10_000_000_000, bytes_accessed=d * f * 6, transcendentals=0),
            name="uw",
        )(*np_, w, du.reshape(nt, f))

        s1 = dgp + send(dgp, 1)
        s2 = s1 + send(s1, 2)
        dg = (s2 + send(s2, 4)).reshape(d)

        pos = lax.broadcasted_iota(jnp.int32, (nt, nt), 1)
        same = flat[:, None] == flat[None, :]
        one = jnp.min(jnp.where(same, pos, nt), axis=1) == jnp.arange(nt)

        de = pl.pallas_call(
            rows_kernel,
            out_shape=jax.ShapeDtypeStruct((vl, d), F32),
            in_specs=[SM, SM, SM, SM, VM, VM] + [ANY] * 17,
            out_specs=ANY,
            input_output_aliases={22: 0},
            scratch_shapes=[vb(NC, 2, 4, tq, cw), vf(nt, d), dma(()), dma(())],
            compiler_params=pltpu.CompilerParams(vmem_limit_bytes=LIMIT),
            name="rows",
        )(lst, cnt, flat, one.astype(jnp.int32), flat.reshape(1, nt), flat.reshape(nt, 1), *dp_, de0)
        return u.reshape(mb, t, f), x, de, dw, dg

    return jax.shard_map(
        local,
        mesh=mesh,
        in_specs=(P("dp", None), P("tp", None), P(None), P(None, "tp"), P("dp", None, "tp"), P("dp", "tp", None)),
        out_specs=(P("dp", None, "tp"), P("dp", "tp", None), P(("dp", "tp"), None), P(None, ("dp", "tp")), P("dp")),
        check_vma=False,
    )
```

```python
import functools

import jax
import jax.numpy as jnp
from jax import lax
from jax.experimental import pallas as pl
from jax.experimental.pallas import tpu as pltpu
from jax.sharding import PartitionSpec as P

EPS = 1e-6
MESH = pl.DeviceIdType.MESH
F32 = jnp.float32
BF16 = jnp.bfloat16
ANY = pl.BlockSpec(memory_space=pl.ANY)
VM = pl.BlockSpec(memory_space=pltpu.VMEM)
SM = pl.BlockSpec(memory_space=pltpu.SMEM)
LIMIT = 60 * 1024 * 1024
NC = 6
HC = NC // 2


def gather_kernel(lst_ref, cnt_ref, ids_ref, emb_ref, xp_ref, buf, xf, sem):
    nt = ids_ref.shape[0]
    vl, d = emb_ref.shape
    cw = d // NC
    tm = nt // 2
    lo = lax.axis_index("tp") * vl
    cnt = cnt_ref[0]

    def group(j):
        loc = ids_ref[lst_ref[j]] - lo
        return pltpu.make_async_copy(emb_ref.at[pl.ds(pl.multiple_of(loc // 8 * 8, 8), 8)], buf.at[j], sem)

    @pl.loop(0, cnt)
    def _(j):
        group(j).start()

    @pl.loop(0, nt // 16)
    def _(i):
        xf[pl.ds(pl.multiple_of(i * 16, 16), 16), :] = jnp.zeros((16, d), F32)

    @pl.loop(0, cnt)
    def _(j):
        group(j).wait()

    @pl.loop(0, cnt)
    def _(j):
        t = lst_ref[j]
        r = (ids_ref[t] - lo) % 8
        s = t % 8
        v = pltpu.roll(buf[j].astype(F32), (s - r + 8) % 8, 0)
        rows = pl.ds(pl.multiple_of(t // 8 * 8, 8), 8)
        mine = lax.broadcasted_iota(jnp.int32, (8, d), 0) == s
        xf[rows, :] = jnp.where(mine, v, xf[rows, :])

    for m in range(2):
        for k in range(NC):

            @pl.loop(0, tm // 64)
            def _(i):
                rows = pl.ds(pl.multiple_of(i * 64, 64), 64)
                src = pl.ds(pl.multiple_of(m * tm + i * 64, 64), 64)
                xp_ref[m, k, rows, :] = xf[src, k * cw : (k + 1) * cw].astype(BF16)


def main_kernel(
    xp_ref, du_ref, w_ref, g_ref, dres_ref,
    xo_ref, n_ref, u_ref, dxo_ref, dxp_ref, dg_ref,
    xs, xr, xfw, x1, x2, xh, xpr, drw, gv, wv, duv, ps, po, pr, sf, rf, r1, r2, nall, acc, dxs, dxr,
    dgm, dgr, dgc, dgn,
    xv_s, du_s, g_s, w_s, dl_s, dr_s, dr_r, xd_s, xd_r, xo_s, xo_r, pd_s, pd_r,
    xa_s, xb_s, xc_s, xa_r, xb_r, xc_r, da_s, db_s, dc_s, da_r, db_r, dc_r,
    ga_s, gb_s, gc_s, ga_r, gb_r, gc_r, h0_s, h0_r, h1_s, h2_s, h3_s, h1_r, h2_r, h3_r,
    no_s, dx_s, dx_r, ox_s, dg_s, dg_r,
):
    me = lax.axis_index("tp")
    c = me % 2
    q = me // 2
    xq = q % 2
    yq = q // 2
    qx = q + 1 - 2 * xq
    qy = q + 2 - 4 * yq
    qd = 3 - q
    part = me + 1 - 2 * c
    dx_ = me + 2 - 4 * xq
    dy_ = me + 4 - 8 * yq
    dd_ = 2 * qd + c
    oc = 1 - c
    d = w_ref.shape[0]
    cw = d // NC
    tq = xs.shape[2]
    th = tq // 2

    def w_copy(k):
        rows = pl.ds(pl.multiple_of(k * cw, cw), cw)
        return pltpu.make_async_copy(w_ref.at[rows], wv.at[k], w_s.at[k])

    def chunk(i):
        return i % 2 * HC + i // 2

    barrier = pltpu.get_barrier_semaphore()
    for dev in (part, dx_, dy_, dd_):
        pl.semaphore_signal(barrier, inc=1, device_id={"tp": dev}, device_id_type=MESH)

    xv_copy = pltpu.make_async_copy(xp_ref.at[c], xs, xv_s)
    du_copy = pltpu.make_async_copy(du_ref, duv, du_s)
    g_copy = pltpu.make_async_copy(g_ref, gv, g_s)
    dl_copy = pltpu.make_async_copy(dres_ref.at[c], drw.at[c], dl_s)
    xv_copy.start()
    du_copy.start()

    @pl.loop(0, NC)
    def _(i):
        w_copy(chunk(i)).start()

    g_copy.start()
    dl_copy.start()
    pl.semaphore_wait(barrier, 4)

    def remote(src, dst, ss, rs, dev):
        return pltpu.make_async_remote_copy(
            src_ref=src, dst_ref=dst, send_sem=ss, recv_sem=rs, device_id={"tp": dev}, device_id_type=MESH
        )

    def xd(k):
        return remote(xp_ref.at[oc, k], xr.at[k], xd_s.at[k], xd_r.at[k], part)

    dr = remote(dres_ref.at[oc], drw.at[c], dr_s, dr_r, part)

    @pl.loop(0, NC)
    def _(i):
        xd(chunk(i)).start()

    dr.start()

    def first(k):
        b = k // HC
        return qx + (qy - qx) * b, dx_ + (dy_ - dx_) * b

    def second(k):
        b = k // HC
        return qy + (qx - qy) * b, dy_ + (dx_ - dy_) * b

    def xa(k):
        return remote(xs.at[k, qd], xfw.at[k], xa_s.at[k], xa_r.at[k], first(k)[1])

    def xb(k):
        return remote(xs.at[k, first(k)[0]], x1.at[k], xb_s.at[k], xb_r.at[k], first(k)[1])

    def xc(k):
        return remote(xs.at[k, second(k)[0]], x2.at[k], xc_s.at[k], xc_r.at[k], second(k)[1])

    def da(k):
        return remote(sf.at[k, qd], rf.at[k], da_s.at[k], da_r.at[k], first(k)[1])

    def db(k):
        return remote(sf.at[k, first(k)[0]], r1.at[k], db_s.at[k], db_r.at[k], first(k)[1])

    def dc(k):
        return remote(sf.at[k, second(k)[0]], r2.at[k], dc_s.at[k], dc_r.at[k], second(k)[1])

    def pd(k):
        return remote(ps.at[k], pr.at[k], pd_s.at[k], pd_r.at[k], part)

    def ga(k):
        return remote(nall.at[k, c, q], nall.at[k, c, q], ga_s.at[k], ga_r.at[k], first(k)[1])

    def gb(k):
        return remote(nall.at[k, c, q], nall.at[k, c, q], gb_s.at[k], gb_r.at[k], second(k)[1])

    def gc(k):
        s = first(k)[0]
        return remote(nall.at[k, c, s], nall.at[k, c, s], gc_s.at[k], gc_r.at[k], second(k)[1])

    def over(k, s, ss, rs):
        return remote(nall.at[k, c, s], nall.at[k, c, s], ss.at[k], rs.at[k], part)

    def h1(k):
        return over(k, first(k)[0], h1_s, h1_r)

    def h2(k):
        return over(k, second(k)[0], h2_s, h2_r)

    def h3(k):
        return over(k, qd, h3_s, h3_r)

    h0 = remote(nall.at[:, c, q], nall.at[:, c, q], h0_s, h0_r, part)

    xv_copy.wait()

    @pl.loop(0, NC)
    def _(i):
        k = chunk(i)
        xd(k).wait_recv()
        xs[k] = xs[k] + xr[k]
        xa(k).start()

    @pl.loop(0, NC)
    def _(i):
        xb(chunk(i)).start()

    du_copy.wait()

    def matmul(i):
        k = chunk(i)
        w_copy(k).wait()
        nt = (((1,), (1,)), ((), ()))
        mine = lax.dot_general(duv[oc], wv[k], nt, preferred_element_type=F32)
        ps[k] = mine.astype(BF16).reshape(4, tq, cw)
        pd(k).start()
        mine = lax.dot_general(duv[c], wv[k], nt, preferred_element_type=F32)
        po[k] = mine.astype(BF16).reshape(4, tq, cw)

    def combine(i):
        k = chunk(i)
        pd(k).wait_recv()
        for s in range(4):
            sf[k, s] = po[k, s].astype(F32) + pr[k, s].astype(F32)
        da(k).start()

    matmul(0)

    @pl.loop(1, NC)
    def _(i):
        matmul(i)
        combine(i - 1)

    combine(NC - 1)

    @pl.loop(0, NC)
    def _(i):
        k = chunk(i)
        s = second(k)[0]
        xa(k).wait_recv()
        xs[k, s] = xs[k, s] + xfw[k]
        xc(k).start()

    @pl.loop(0, NC)
    def _(i):
        db(chunk(i)).start()

    acc[...] = jnp.zeros_like(acc)

    @pl.loop(0, NC)
    def _(i):
        k = chunk(i)
        s = second(k)[0]
        da(k).wait_recv()
        sf[k, s] = sf[k, s] + rf[k]
        dc(k).start()

    g_copy.wait()
    sq = jnp.zeros((tq, 1), F32)
    for k in range(NC):
        xb(k).wait_recv()
        xc(k).wait_recv()
        xk = xs[k, q] + x1[k] + x2[k]
        xh[k] = xk
        xk = xk.astype(F32)
        sq = sq + jnp.sum(xk * xk, axis=-1, keepdims=True)
    xo = remote(xh.at[:, pl.ds(pl.multiple_of(oc * th, th), th), :], xpr, xo_s, xo_r, part)
    xo.start()
    rs = lax.rsqrt(sq * (1.0 / d) + EPS)
    for k in (0, 3, 1, 4, 2, 5):
        cols = slice(k * cw, (k + 1) * cw)
        nall[k, c, q] = ((xh[k].astype(F32) * rs) * gv[:, cols].astype(F32)).astype(BF16)
        ga(k).start()
    for k in (0, 3, 1, 4, 2, 5):
        gb(k).start()
    h0.start()
    for k in range(NC):
        xo_ref[c, :, k * cw : (k + 1) * cw] = xh[k, pl.ds(pl.multiple_of(c * th, th), th), :]
    dl_copy.wait()
    dr.wait_recv()
    xo.wait_recv()
    for k in range(NC):
        xo_ref[oc, :, k * cw : (k + 1) * cw] = xpr[k]

    m = jnp.zeros((tq, 1), F32)
    for k in range(NC):
        cols = slice(k * cw, (k + 1) * cw)
        db(k).wait_recv()
        dc(k).wait_recv()
        dn = sf[k, q] + r1[k] + r2[k]
        r1[k] = dn
        nh = xh[k].astype(F32) * rs
        dnh = dn * nh
        dgm[:, cols] = jnp.sum(dnh, axis=0, keepdims=True)
        m = m + jnp.sum(dnh * gv[:, cols].astype(F32), axis=-1, keepdims=True)
    dg0 = remote(dgm, dgr, dg_s.at[0], dg_r.at[0], part)
    dg0.start()
    m = m * (1.0 / d)
    for k in range(NC):
        cols = slice(k * cw, (k + 1) * cw)
        nh = xh[k].astype(F32) * rs
        dxn = rs * (gv[:, cols].astype(F32) * r1[k] - nh * m)
        dxs[k] = (drw[:, :, cols].reshape(tq, cw).astype(F32) + dxn).astype(BF16)
    dxc = remote(dxs, dxr, dx_s, dx_r, part)
    dxc.start()
    ox = pltpu.make_async_copy(dxs, dxo_ref, ox_s.at[0])
    ox.start()
    dg0.wait_recv()
    dgc[...] = dgm[...] + dgr[...]
    dgs = [remote(dgc, dgn.at[j], dg_s.at[1 + j], dg_r.at[1 + j], dev) for j, dev in enumerate((dx_, dy_, dd_))]
    for cp in dgs:
        cp.start()

    @pl.loop(0, NC)
    def _(i):
        k = chunk(i)
        ga(k).wait_recv()
        gc(k).start()
        h1(k).start()

    @pl.loop(0, NC)
    def _(i):
        k = chunk(i)
        gb(k).wait_recv()
        h2(k).start()

    dxc.wait_recv()
    oy = pltpu.make_async_copy(dxr, dxp_ref, ox_s.at[1])
    oy.start()
    for cp in dgs:
        cp.wait_recv()
    dg_ref[...] = (dgc[...] + dgn[0]) + (dgn[1] + dgn[2])

    def n_out(k):
        return pltpu.make_async_copy(nall.at[k], n_ref.at[k], no_s.at[k])

    def arrive(i):
        for k in (i, i + HC):
            gc(k).wait_recv()
            h3(k).start()

    def project(i):
        for k in (i, i + HC):
            h1(k).wait_recv()
            h2(k).wait_recv()
            h3(k).wait_recv()
            n_out(k).start()
        nt = 8 * tq
        acc[...] += jnp.dot(nall[i].reshape(nt, cw), wv[i], preferred_element_type=F32) + jnp.dot(
            nall[i + HC].reshape(nt, cw), wv[i + HC], preferred_element_type=F32
        )

    h0.wait_recv()
    arrive(0)

    @pl.loop(1, HC)
    def _(i):
        arrive(i)
        project(i - 1)

    project(HC - 1)
    u_ref[...] = acc[...].astype(BF16)

    ox.wait()
    oy.wait()
    dr.wait_send()
    xo.wait_send()
    h0.wait_send()
    dg0.wait_send()
    dxc.wait_send()
    for cp in dgs:
        cp.wait_send()

    @pl.loop(0, NC)
    def _(k):
        n_out(k).wait()
        for f in (xd, pd, xa, xb, xc, da, db, dc, ga, gb, gc, h1, h2, h3):
            f(k).wait_send()


def zero_kernel(_, out_ref, z, sem):
    z[...] = jnp.zeros_like(z)
    n = out_ref.shape[0] // z.shape[0]

    def put(i):
        rows = pl.ds(pl.multiple_of(i * z.shape[0], z.shape[0]), z.shape[0])
        return pltpu.make_async_copy(z, out_ref.at[rows], sem)

    @pl.loop(0, n)
    def _(i):
        put(i).start()

    @pl.loop(0, n)
    def _(i):
        put(i).wait()


def dw_kernel(n_ref, du_ref, dw_ref, nv, duv, st, n_s, du_s, o_s):
    cw = nv.shape[2]
    du_copy = pltpu.make_async_copy(du_ref, duv, du_s)
    du_copy.start()

    def n_copy(k):
        return pltpu.make_async_copy(n_ref.at[k], nv.at[k], n_s.at[k])

    def out(k):
        rows = pl.ds(pl.multiple_of(k * cw, cw), cw)
        return pltpu.make_async_copy(st.at[k % 2], dw_ref.at[rows], o_s.at[k % 2])

    for k in range(NC):
        n_copy(k).start()
    du_copy.wait()

    @pl.loop(0, NC)
    def _(k):
        n_copy(k).wait()

        @pl.when(k >= 2)
        def _():
            out(k - 2).wait()

        st[k % 2] = lax.dot_general(nv[k], duv[...], (((0,), (0,)), ((), ())), preferred_element_type=F32)
        out(k).start()

    out(NC - 2).wait()
    out(NC - 1).wait()


def rows_kernel(*refs):
    lst_ref, cnt_ref, ids_ref, idr_ref, idc_ref = refs[:5]
    dx_refs = refs[5:13]
    _, de_ref, dxv, dxs, d_s, o_s = refs[13:]
    nt = ids_ref.shape[0]
    vl = de_ref.shape[0]
    cw = dxv.shape[-1]
    me = lax.axis_index("tp")
    lo = me * vl
    c = me % 2
    q = me // 2
    qx = q + 1 - 2 * (q % 2)
    qy = q + 2 - 4 * (q // 2)
    where = [(b, s) for b in (c, 1 - c) for s in (q, qx, qy, 3 - q)]
    loads = [pltpu.make_async_copy(r, dxv.at[:, b, s], d_s) for r, (b, s) in zip(dx_refs, where)]
    for cp in loads:
        cp.start()
    same = (idc_ref[...] == idr_ref[...]).astype(BF16)
    for cp in loads:
        cp.wait()
    for k in range(NC):
        dxs[:, k * cw : (k + 1) * cw] = jnp.dot(same, dxv[k].reshape(nt, cw), preferred_element_type=F32)
    cnt = cnt_ref[0]

    def put(j):
        t = lst_ref[j]
        return pltpu.make_async_copy(dxs.at[pl.ds(t, 1)], de_ref.at[pl.ds(ids_ref[t] - lo, 1)], o_s)

    @pl.loop(0, cnt)
    def _(j):
        put(j).start()

    @pl.loop(0, cnt)
    def _(j):
        put(j).wait()


def compact(flags):
    n = flags.shape[0]
    pos = jnp.arange(n, dtype=jnp.int32)
    before = jnp.sum(jnp.where(flags[None, :] & (pos[None, :] < pos[:, None]), 1, 0), axis=1)
    rank = jnp.where(flags, before, -1)
    lst = jnp.sum(jnp.where(rank[None, :] == pos[:, None], pos[None, :], 0), axis=1)
    return lst.astype(jnp.int32), jnp.sum(flags.astype(jnp.int32)).reshape(1)


def solution(mesh):
    groups = mesh.shape["tp"]

    def shift(bit):
        return [(r, r ^ bit) for r in range(groups)]

    def send(a, bit):
        return lax.ppermute(a, "tp", shift(bit))

    def local(ids, emb, g, w, du, dres):
        mb, t = ids.shape
        vl, d = emb.shape
        f = w.shape[1]
        nt = mb * t
        cw = d // NC
        tq = t // 4
        flat = ids.reshape(nt)
        dma = pltpu.SemaphoreType.DMA
        sds = jax.ShapeDtypeStruct
        vb = lambda *s: pltpu.VMEM(s, BF16)
        vf = lambda *s: pltpu.VMEM(s, F32)
        local_only = pltpu.CompilerParams(vmem_limit_bytes=LIMIT)

        loc = flat - lax.axis_index("tp") * vl
        own = (loc >= 0) & (loc < vl)
        lst, cnt = compact(own)

        xp = pl.pallas_call(
            gather_kernel,
            out_shape=sds((2, NC, t, cw), BF16),
            in_specs=[SM, SM, SM, ANY],
            out_specs=VM,
            scratch_shapes=[vb(nt, 8, d), vf(nt, d), dma(())],
            compiler_params=local_only,
            name="gather",
        )(lst, cnt, flat, emb)

        blk = (NC, tq, cw)
        x, n, u, dxo, dxp, dg = pl.pallas_call(
            main_kernel,
            out_shape=(
                sds((2, tq // 2, d), BF16),
                sds((NC, 2, 4, tq, cw), BF16),
                sds((nt, f), BF16),
                sds(blk, BF16),
                sds(blk, BF16),
                sds((1, d), F32),
            ),
            in_specs=[ANY] * 5,
            out_specs=(VM, ANY, VM, ANY, ANY, VM),
            scratch_shapes=[
                vb(NC, 4, tq, cw), vb(NC, 4, tq, cw), vb(*blk), vb(*blk), vb(*blk),
                vb(*blk), vb(NC, tq // 2, cw), vb(2, tq // 2, d), vb(1, d),
                vb(NC, cw, f), vb(2, t, f),
                vb(NC, 4, tq, cw), vb(NC, 4, tq, cw), vb(NC, 4, tq, cw),
                vf(NC, 4, tq, cw), vf(*blk), vf(*blk), vf(*blk),
                vb(NC, 2, 4, tq, cw), vf(nt, f), vb(*blk), vb(*blk),
                vf(1, d), vf(1, d), vf(1, d), vf(3, 1, d),
                dma(()), dma(()), dma(()), dma((NC,)), dma(()), dma(()), dma(()), dma((NC,)), dma((NC,)),
                dma(()), dma(()), dma((NC,)), dma((NC,)),
            ]
            + [dma((NC,))] * 18
            + [dma(())] * 2
            + [dma((NC,))] * 7
            + [dma(()), dma(()), dma((2,)), dma((4,)), dma((4,))],
            compiler_params=pltpu.CompilerParams(collective_id=0, has_side_effects=True, vmem_limit_bytes=LIMIT),
            name="main",
        )(xp.reshape(2, NC, 4, tq, cw), du, w, g.reshape(1, d), dres)

        near = [send(dxo, b) for b in (2, 4, 6)]
        de0 = pl.pallas_call(
            zero_kernel,
            out_shape=sds((vl, d), F32),
            in_specs=[ANY],
            out_specs=ANY,
            scratch_shapes=[vf(128, d), dma(())],
            compiler_params=local_only,
            cost_estimate=pl.CostEstimate(flops=16_000_000_000, bytes_accessed=vl * d * 4, transcendentals=0),
            name="zero",
        )(dg)
        far = [send(a, 1) for a in near]

        dw = pl.pallas_call(
            dw_kernel,
            out_shape=sds((d, f), F32),
            in_specs=[ANY] * 2,
            out_specs=ANY,
            scratch_shapes=[vb(NC, nt, cw), vb(nt, f), vf(2, cw, f), dma((NC,)), dma(()), dma((2,))],
            compiler_params=local_only,
            cost_estimate=pl.CostEstimate(flops=10_000_000_000, bytes_accessed=d * f * 5, transcendentals=0),
            name="dw",
        )(n.reshape(NC, nt, cw), du.reshape(nt, f))

        same = flat[:, None] == flat[None, :]
        pos = jnp.arange(nt, dtype=jnp.int32)
        one = jnp.min(jnp.where(same, pos[None, :], nt), axis=1) == pos
        lst1, cnt1 = compact(own & one)
        de = pl.pallas_call(
            rows_kernel,
            out_shape=sds((vl, d), F32),
            in_specs=[SM, SM, SM, VM, VM] + [ANY] * 9,
            out_specs=ANY,
            input_output_aliases={13: 0},
            scratch_shapes=[vb(NC, 2, 4, tq, cw), vf(nt, d), dma(()), dma(())],
            compiler_params=local_only,
            name="rows",
        )(lst1, cnt1, flat, flat.reshape(1, nt), flat.reshape(nt, 1), dxo, *near, dxp, *far, de0)
        return u.reshape(mb, t, f), x, de, dw, dg.reshape(d)

    return jax.shard_map(
        local,
        mesh=mesh,
        in_specs=(P("dp", None), P("tp", None), P(None), P(None, "tp"), P("dp", None, "tp"), P("dp", "tp", None)),
        out_specs=(P("dp", None, "tp"), P("dp", "tp", None), P(("dp", "tp"), None), P(None, ("dp", "tp")), P("dp")),
        check_vma=False,
    )
```

```python
import functools

import jax
import jax.numpy as jnp
from jax import lax
from jax.experimental import pallas as pl
from jax.experimental.pallas import tpu as pltpu
from jax.sharding import PartitionSpec as P

EPS = 1e-6
MESH = pl.DeviceIdType.MESH
F32 = jnp.float32
BF16 = jnp.bfloat16
ANY = pl.BlockSpec(memory_space=pl.ANY)
VM = pl.BlockSpec(memory_space=pltpu.VMEM)
SM = pl.BlockSpec(memory_space=pltpu.SMEM)
LIMIT = 60 * 1024 * 1024
NC = 6
HC = NC // 2


def main_kernel(
    ids_ref, emb_ref, du_ref, w_ref, g_ref, dres_ref,
    xo_ref, n_ref, u_ref, dxo_ref, dxp_ref, dg_ref,
    idv, ev, oh, xp, xr, xfw, x1, x2, xh, xpr, drw, gv, wv, duv, pb, pr, sf, rf, r1, r2, nall, acc, dxs, dxr,
    dgm, dgr, dgc, dgn,
    id_s, e_s, du_s, g_s, w_s, dl_s, dr_s, dr_r, xd_s, xd_r, xo_s, xo_r, pd_s, pd_r,
    xa_s, xb_s, xc_s, xa_r, xb_r, xc_r, da_s, db_s, dc_s, da_r, db_r, dc_r,
    ga_s, gb_s, gc_s, ga_r, gb_r, gc_r, h0_s, h0_r, h1_s, h2_s, h3_s, h1_r, h2_r, h3_r,
    no_s, dx_s, dx_r, ox_s, dg_s, dg_r,
):
    me = lax.axis_index("tp")
    c = me % 2
    q = me // 2
    xq = q % 2
    yq = q // 2
    qx = q + 1 - 2 * xq
    qy = q + 2 - 4 * yq
    qd = 3 - q
    part = me + 1 - 2 * c
    dx_ = me + 2 - 4 * xq
    dy_ = me + 4 - 8 * yq
    dd_ = 2 * qd + c
    oc = 1 - c
    d = w_ref.shape[0]
    cw = d // NC
    vl = emb_ref.shape[0]
    tq = xr.shape[2]
    nt = 8 * tq
    th = tq // 2

    def w_copy(k):
        rows = pl.ds(pl.multiple_of(k * cw, cw), cw)
        return pltpu.make_async_copy(w_ref.at[rows], wv.at[k], w_s.at[k])

    def chunk(i):
        return i % 2 * HC + i // 2

    barrier = pltpu.get_barrier_semaphore()
    for dev in (part, dx_, dy_, dd_):
        pl.semaphore_signal(barrier, inc=1, device_id={"tp": dev}, device_id_type=MESH)

    id_copy = pltpu.make_async_copy(ids_ref, idv, id_s)
    du_copy = pltpu.make_async_copy(du_ref, duv, du_s)
    g_copy = pltpu.make_async_copy(g_ref, gv, g_s)
    dl_copy = pltpu.make_async_copy(dres_ref.at[c], drw.at[c], dl_s)
    def e_copy(i):
        cols = pl.ds(pl.multiple_of(chunk(i) * cw, cw), cw)
        return pltpu.make_async_copy(emb_ref.at[:, cols], ev.at[i % 2], e_s.at[i % 2])

    du_copy.start()

    @pl.loop(0, NC)
    def _(i):
        w_copy(chunk(i)).start()

    id_copy.start()
    g_copy.start()
    dl_copy.start()
    e_copy(0).start()
    e_copy(1).start()
    pl.semaphore_wait(barrier, 4)

    def remote(src, dst, ss, rs, dev):
        return pltpu.make_async_remote_copy(
            src_ref=src, dst_ref=dst, send_sem=ss, recv_sem=rs, device_id={"tp": dev}, device_id_type=MESH
        )

    def xd(k):
        return remote(xp.at[k, oc], xr.at[k], xd_s.at[k], xd_r.at[k], part)

    dr = remote(dres_ref.at[oc], drw.at[c], dr_s, dr_r, part)

    def first(k):
        b = k // HC
        return qx + (qy - qx) * b, dx_ + (dy_ - dx_) * b

    def second(k):
        b = k // HC
        return qy + (qx - qy) * b, dy_ + (dx_ - dy_) * b

    def xa(k):
        return remote(xp.at[k, c, qd], xfw.at[k], xa_s.at[k], xa_r.at[k], first(k)[1])

    def xb(k):
        return remote(xp.at[k, c, first(k)[0]], x1.at[k], xb_s.at[k], xb_r.at[k], first(k)[1])

    def xc(k):
        return remote(xp.at[k, c, second(k)[0]], x2.at[k], xc_s.at[k], xc_r.at[k], second(k)[1])

    def da(k):
        return remote(sf.at[k, qd], rf.at[k], da_s.at[k], da_r.at[k], first(k)[1])

    def db(k):
        return remote(sf.at[k, first(k)[0]], r1.at[k], db_s.at[k], db_r.at[k], first(k)[1])

    def dc(k):
        return remote(sf.at[k, second(k)[0]], r2.at[k], dc_s.at[k], dc_r.at[k], second(k)[1])

    def pd(k):
        return remote(pb.at[k, oc], pr.at[k], pd_s.at[k], pd_r.at[k], part)

    def ga(k):
        return remote(nall.at[k, c, q], nall.at[k, c, q], ga_s.at[k], ga_r.at[k], first(k)[1])

    def gb(k):
        return remote(nall.at[k, c, q], nall.at[k, c, q], gb_s.at[k], gb_r.at[k], second(k)[1])

    def gc(k):
        s = first(k)[0]
        return remote(nall.at[k, c, s], nall.at[k, c, s], gc_s.at[k], gc_r.at[k], second(k)[1])

    def over(k, s, ss, rs):
        return remote(nall.at[k, c, s], nall.at[k, c, s], ss.at[k], rs.at[k], part)

    def h1(k):
        return over(k, first(k)[0], h1_s, h1_r)

    def h2(k):
        return over(k, second(k)[0], h2_s, h2_r)

    def h3(k):
        return over(k, qd, h3_s, h3_r)

    h0 = remote(nall.at[:, c, q], nall.at[:, c, q], h0_s, h0_r, part)

    du_copy.wait()

    def matmul(i):
        k = chunk(i)
        w_copy(k).wait()
        p = lax.dot_general(
            duv[...].reshape(nt, -1), wv[k], (((1,), (1,)), ((), ())), preferred_element_type=F32
        )
        pb[k] = p.astype(BF16).reshape(2, 4, tq, cw)
        pd(k).start()

    def combine(i):
        k = chunk(i)
        pd(k).wait_recv()
        for s in range(4):
            sf[k, s] = pb[k, c, s].astype(F32) + pr[k, s].astype(F32)
        da(k).start()
        db(k).start()

    matmul(0)

    @pl.loop(1, NC)
    def _(i):
        matmul(i)
        combine(i - 1)

    id_copy.wait()
    lo = me * vl
    for b in range(nt // 128):
        m, t0 = divmod(b * 128, 4 * tq)
        row = idv[m : m + 1, t0 : t0 + 128] - lo
        col = jnp.broadcast_to(row, (128, 128)).T

        @pl.loop(0, vl // 128)
        def _(j):
            lanes = lax.broadcasted_iota(jnp.int32, (128, 128), 1) + j * 128
            cols = pl.ds(pl.multiple_of(j * 128, 128), 128)
            oh[b * 128 : (b + 1) * 128, cols] = jnp.where(lanes == col, 1.0, 0.0).astype(BF16)

    combine(NC - 1)
    dr.start()

    def lookup(i):
        k = chunk(i)
        e_copy(i).wait()
        p = jnp.dot(oh[...], ev[i % 2], preferred_element_type=F32)
        xp[k] = p.astype(BF16).reshape(2, 4, tq, cw)
        xd(k).start()

        @pl.when(i + 2 < NC)
        def _():
            e_copy(i + 2).start()

    def pair(i):
        k = chunk(i)
        xd(k).wait_recv()
        xp[k, c] = xp[k, c] + xr[k]
        xa(k).start()
        xb(k).start()

    lookup(0)

    @pl.loop(1, NC)
    def _(i):
        lookup(i)
        pair(i - 1)

    pair(NC - 1)
    acc[...] = jnp.zeros_like(acc)

    @pl.loop(0, NC)
    def _(i):
        k = chunk(i)
        s = second(k)[0]
        xa(k).wait_recv()
        xp[k, c, s] = xp[k, c, s] + xfw[k]
        xc(k).start()

    @pl.loop(0, NC)
    def _(i):
        k = chunk(i)
        s = second(k)[0]
        da(k).wait_recv()
        sf[k, s] = sf[k, s] + rf[k]
        dc(k).start()

    g_copy.wait()
    sq = jnp.zeros((tq, 1), F32)
    for k in range(NC):
        xb(k).wait_recv()
        xc(k).wait_recv()
        xk = xp[k, c, q] + x1[k] + x2[k]
        xh[k] = xk
        xk = xk.astype(F32)
        sq = sq + jnp.sum(xk * xk, axis=-1, keepdims=True)
    xo = remote(xh.at[:, pl.ds(pl.multiple_of(oc * th, th), th), :], xpr, xo_s, xo_r, part)
    xo.start()
    rs = lax.rsqrt(sq * (1.0 / d) + EPS)
    for k in (0, 3, 1, 4, 2, 5):
        cols = slice(k * cw, (k + 1) * cw)
        nall[k, c, q] = ((xh[k].astype(F32) * rs) * gv[:, cols].astype(F32)).astype(BF16)
        ga(k).start()
    for k in (0, 3, 1, 4, 2, 5):
        gb(k).start()
    h0.start()
    for k in range(NC):
        xo_ref[c, :, k * cw : (k + 1) * cw] = xh[k, pl.ds(pl.multiple_of(c * th, th), th), :]
    dl_copy.wait()
    dr.wait_recv()
    xo.wait_recv()
    for k in range(NC):
        xo_ref[oc, :, k * cw : (k + 1) * cw] = xpr[k]

    m = jnp.zeros((tq, 1), F32)
    for k in range(NC):
        cols = slice(k * cw, (k + 1) * cw)
        db(k).wait_recv()
        dc(k).wait_recv()
        dn = sf[k, q] + r1[k] + r2[k]
        r1[k] = dn
        nh = xh[k].astype(F32) * rs
        dnh = dn * nh
        dgm[:, cols] = jnp.sum(dnh, axis=0, keepdims=True)
        m = m + jnp.sum(dnh * gv[:, cols].astype(F32), axis=-1, keepdims=True)
    dg0 = remote(dgm, dgr, dg_s.at[0], dg_r.at[0], part)
    dg0.start()
    m = m * (1.0 / d)
    for k in range(NC):
        cols = slice(k * cw, (k + 1) * cw)
        nh = xh[k].astype(F32) * rs
        dxn = rs * (gv[:, cols].astype(F32) * r1[k] - nh * m)
        dxs[k] = (drw[:, :, cols].reshape(tq, cw).astype(F32) + dxn).astype(BF16)
    dxc = remote(dxs, dxr, dx_s, dx_r, part)
    dxc.start()
    ox = pltpu.make_async_copy(dxs, dxo_ref, ox_s.at[0])
    ox.start()
    dg0.wait_recv()
    dgc[...] = dgm[...] + dgr[...]
    dgs = [remote(dgc, dgn.at[j], dg_s.at[1 + j], dg_r.at[1 + j], dev) for j, dev in enumerate((dx_, dy_, dd_))]
    for cp in dgs:
        cp.start()

    @pl.loop(0, NC)
    def _(i):
        k = chunk(i)
        ga(k).wait_recv()
        gc(k).start()
        h1(k).start()

    @pl.loop(0, NC)
    def _(i):
        k = chunk(i)
        gb(k).wait_recv()
        h2(k).start()

    dxc.wait_recv()
    oy = pltpu.make_async_copy(dxr, dxp_ref, ox_s.at[1])
    oy.start()
    for cp in dgs:
        cp.wait_recv()
    dg_ref[...] = (dgc[...] + dgn[0]) + (dgn[1] + dgn[2])

    def n_out(k):
        return pltpu.make_async_copy(nall.at[k], n_ref.at[k], no_s.at[k])

    def arrive(i):
        k = chunk(i)
        gc(k).wait_recv()
        h3(k).start()

    def project(i):
        k = chunk(i)
        h1(k).wait_recv()
        h2(k).wait_recv()
        h3(k).wait_recv()
        n_out(k).start()
        acc[...] += jnp.dot(nall[k].reshape(nt, cw), wv[k], preferred_element_type=F32)

    h0.wait_recv()
    arrive(0)

    @pl.loop(1, NC)
    def _(i):
        arrive(i)
        project(i - 1)

    project(NC - 1)
    u_ref[...] = acc[...].astype(BF16)

    ox.wait()
    oy.wait()
    dr.wait_send()
    xo.wait_send()
    h0.wait_send()
    dg0.wait_send()
    dxc.wait_send()
    for cp in dgs:
        cp.wait_send()

    @pl.loop(0, NC)
    def _(k):
        n_out(k).wait()
        for f in (xd, pd, xa, xb, xc, da, db, dc, ga, gb, gc, h1, h2, h3):
            f(k).wait_send()


def fill_kernel(
    n_ref, du_ref, u_ref, x_ref, dg_ref, dw_ref, de_ref, uo_ref, xo_ref, dgo_ref,
    nv, duv, st, z, uv, xv, gv, n_s, du_s, o_s, z_s, p_s, *, rows,
):
    cw = nv.shape[2]
    zr = z.shape[0]
    du_copy = pltpu.make_async_copy(du_ref, duv, du_s)
    du_copy.start()

    def n_copy(k):
        return pltpu.make_async_copy(n_ref.at[k], nv.at[k], n_s.at[k])

    def out(k):
        r = pl.ds(pl.multiple_of(k * cw, cw), cw)
        return pltpu.make_async_copy(st.at[k % 2], dw_ref.at[r], o_s.at[k % 2])

    def put(i):
        return pltpu.make_async_copy(z, de_ref.at[pl.ds(pl.multiple_of(i * zr, zr), zr)], z_s)

    for k in range(NC):
        n_copy(k).start()
    small = ((u_ref, uv, uo_ref), (x_ref, xv, xo_ref), (dg_ref, gv, dgo_ref))
    ins = [pltpu.make_async_copy(a, v, p_s.at[j]) for j, (a, v, _) in enumerate(small)]
    outs = [pltpu.make_async_copy(v, o, p_s.at[j]) for j, (_, v, o) in enumerate(small)]
    for cp in ins:
        cp.start()
    z[...] = jnp.zeros_like(z)
    per = rows // zr // NC
    du_copy.wait()

    @pl.loop(0, NC)
    def _(k):
        n_copy(k).wait()
        for j in range(per):
            put(k * per + j).start()

        @pl.when(k >= 2)
        def _():
            out(k - 2).wait()

        st[k % 2] = lax.dot_general(nv[k], duv[...], (((0,), (0,)), ((), ())), preferred_element_type=F32)
        out(k).start()

    for cp, co in zip(ins, outs):
        cp.wait()
        co.start()
    for co in outs:
        co.wait()
    out(NC - 2).wait()
    out(NC - 1).wait()

    @pl.loop(0, per * NC)
    def _(i):
        put(i).wait()


def list_kernel(flag_ref, ids_ref, idv_ref, _, lst_ref, cnt_ref, sel_ref, de_ref, z, sel, z_s, *, rows):
    zr = z.shape[0]
    nt = ids_ref.shape[0]
    left = (de_ref.shape[0] - rows) // zr

    def put(i):
        return pltpu.make_async_copy(z, de_ref.at[pl.ds(pl.multiple_of(rows + i * zr, zr), zr)], z_s)

    z[...] = jnp.zeros_like(z)

    @pl.loop(0, left)
    def _(i):
        put(i).start()

    def scan(t, n):
        lst_ref[n] = t
        return n + flag_ref[t]

    cnt = lax.fori_loop(0, nt, scan, jnp.int32(0), unroll=8)
    cnt_ref[0] = cnt
    sel[...] = jnp.zeros_like(sel)
    tm = nt // 2

    @pl.loop(0, cnt)
    def _(j):
        v = ids_ref[lst_ref[j]]
        for m in range(2):
            hit = idv_ref[m : m + 1, :] == v
            sel[pl.ds(j, 1), m * tm : (m + 1) * tm] = jnp.where(hit, 1.0, 0.0)

    sel_ref[...] = sel[...].astype(BF16)

    @pl.loop(0, left)
    def _(i):
        put(i).wait()


def rows_kernel(*refs):
    lst_ref, cnt_ref, ids_ref, sel_ref = refs[:4]
    dx_refs = refs[4:12]
    _, de_ref, dxv, dxs, d_s, o_s = refs[12:]
    nt = ids_ref.shape[0]
    vl = de_ref.shape[0]
    cw = dxv.shape[-1]
    rb = 128
    me = lax.axis_index("tp")
    lo = me * vl
    c = me % 2
    q = me // 2
    qx = q + 1 - 2 * (q % 2)
    qy = q + 2 - 4 * (q // 2)
    where = [(b, s) for b in (c, 1 - c) for s in (q, qx, qy, 3 - q)]
    loads = [pltpu.make_async_copy(r, dxv.at[:, b, s], d_s) for r, (b, s) in zip(dx_refs, where)]
    for cp in loads:
        cp.start()
    cnt = cnt_ref[0]
    for cp in loads:
        cp.wait()

    def put(j):
        return pltpu.make_async_copy(dxs.at[pl.ds(j, 1)], de_ref.at[pl.ds(ids_ref[lst_ref[j]] - lo, 1)], o_s)

    @pl.loop(0, (cnt + rb - 1) // rb)
    def _(b):
        r = pl.ds(pl.multiple_of(b * rb, rb), rb)
        for k in range(NC):
            dxs[r, k * cw : (k + 1) * cw] = jnp.dot(
                sel_ref[r, :], dxv[k].reshape(nt, cw), preferred_element_type=F32
            )

        @pl.loop(b * rb, jnp.minimum(b * rb + rb, cnt))
        def _(j):
            put(j).start()

    @pl.loop(0, cnt)
    def _(j):
        put(j).wait()


def solution(mesh):
    groups = mesh.shape["tp"]

    def shift(bit):
        return [(r, r ^ bit) for r in range(groups)]

    def send(a, bit):
        return lax.ppermute(a, "tp", shift(bit))

    def local(ids, emb, g, w, du, dres):
        mb, t = ids.shape
        vl, d = emb.shape
        f = w.shape[1]
        nt = mb * t
        cw = d // NC
        tq = t // 4
        flat = ids.reshape(nt)
        dma = pltpu.SemaphoreType.DMA
        sds = jax.ShapeDtypeStruct
        vb = lambda *s: pltpu.VMEM(s, BF16)
        vf = lambda *s: pltpu.VMEM(s, F32)
        local_only = pltpu.CompilerParams(vmem_limit_bytes=LIMIT)

        blk = (NC, tq, cw)
        x, n, u, dxo, dxp, dg = pl.pallas_call(
            main_kernel,
            out_shape=(
                sds((2, tq // 2, d), BF16),
                sds((NC, 2, 4, tq, cw), BF16),
                sds((nt, f), BF16),
                sds(blk, BF16),
                sds(blk, BF16),
                sds((1, d), F32),
            ),
            in_specs=[ANY] * 6,
            out_specs=(VM, ANY, VM, ANY, ANY, VM),
            scratch_shapes=[
                pltpu.VMEM((mb, t), jnp.int32), vb(2, vl, cw), vb(nt, vl),
                vb(NC, 2, 4, tq, cw), vb(NC, 4, tq, cw), vb(*blk), vb(*blk), vb(*blk),
                vb(*blk), vb(NC, tq // 2, cw), vb(2, tq // 2, d), vb(1, d),
                vb(NC, cw, f), vb(2, t, f),
                vb(NC, 2, 4, tq, cw), vb(NC, 4, tq, cw),
                vf(NC, 4, tq, cw), vf(*blk), vf(*blk), vf(*blk),
                vb(NC, 2, 4, tq, cw), vf(nt, f), vb(*blk), vb(*blk),
                vf(1, d), vf(1, d), vf(1, d), vf(3, 1, d),
                dma(()), dma((2,)), dma(()), dma(()), dma((NC,)), dma(()), dma(()), dma(()), dma((NC,)), dma((NC,)),
                dma(()), dma(()), dma((NC,)), dma((NC,)),
            ]
            + [dma((NC,))] * 18
            + [dma(())] * 2
            + [dma((NC,))] * 7
            + [dma(()), dma(()), dma((2,)), dma((4,)), dma((4,))],
            compiler_params=pltpu.CompilerParams(collective_id=0, has_side_effects=True, vmem_limit_bytes=LIMIT),
            name="main",
        )(ids, emb, du, w, g.reshape(1, d), dres)

        zr = 128
        rows = vl // zr * 3 // 4 // NC * NC * zr
        near = [send(dxo, b) for b in (2, 4, 6)]
        dw, de, u, x, dg = pl.pallas_call(
            functools.partial(fill_kernel, rows=rows),
            out_shape=(sds((d, f), F32), sds((vl, d), F32), sds((nt, f), BF16), sds(x.shape, BF16), sds((1, d), F32)),
            in_specs=[ANY] * 5,
            out_specs=(ANY,) * 5,
            scratch_shapes=[
                vb(NC, nt, cw), vb(nt, f), vf(2, cw, f), vf(zr, d), vb(nt, f), vb(*x.shape), vf(1, d),
                dma((NC,)), dma(()), dma((2,)), dma(()), dma((3,)),
            ],
            compiler_params=local_only,
            cost_estimate=pl.CostEstimate(flops=18_000_000_000, bytes_accessed=vl * d * 4, transcendentals=0),
            name="fill",
        )(n.reshape(NC, nt, cw), du.reshape(nt, f), u, x, dg)
        far = [send(a, 1) for a in near]

        loc = flat - lax.axis_index("tp") * vl
        same = flat[:, None] == flat[None, :]
        pos = jnp.arange(nt, dtype=jnp.int32)
        one = jnp.min(jnp.where(same, pos[None, :], nt), axis=1) == pos
        flag = (one & (loc >= 0) & (loc < vl)).astype(jnp.int32)
        lst, cnt, sel, de = pl.pallas_call(
            functools.partial(list_kernel, rows=rows),
            out_shape=(sds((nt + 8,), jnp.int32), sds((1,), jnp.int32), sds((nt, nt), BF16), sds((vl, d), F32)),
            in_specs=[SM, SM, VM, ANY],
            out_specs=(SM, SM, VM, ANY),
            input_output_aliases={3: 3},
            scratch_shapes=[vf(zr, d), vf(nt, nt), dma(())],
            compiler_params=local_only,
            cost_estimate=pl.CostEstimate(flops=5_000_000_000, bytes_accessed=(vl - rows) * d * 4, transcendentals=0),
            name="list",
        )(flag, flat, ids, de)
        de = pl.pallas_call(
            rows_kernel,
            out_shape=sds((vl, d), F32),
            in_specs=[SM, SM, SM, VM] + [ANY] * 9,
            out_specs=ANY,
            input_output_aliases={12: 0},
            scratch_shapes=[vb(NC, 2, 4, tq, cw), vf(nt, d), dma(()), dma(())],
            compiler_params=local_only,
            name="rows",
        )(lst, cnt, flat, sel, dxo, *near, dxp, *far, de)
        return u.reshape(mb, t, f), x, de, dw, dg.reshape(d)

    return jax.shard_map(
        local,
        mesh=mesh,
        in_specs=(P("dp", None), P("tp", None), P(None), P(None, "tp"), P("dp", None, "tp"), P("dp", "tp", None)),
        out_specs=(P("dp", None, "tp"), P("dp", "tp", None), P(("dp", "tp"), None), P(None, ("dp", "tp")), P("dp")),
        check_vma=False,
    )
```

```python
import functools

import jax
import jax.numpy as jnp
from jax import lax
from jax.experimental import pallas as pl
from jax.experimental.pallas import tpu as pltpu
from jax.sharding import PartitionSpec as P

EPS = 1e-6
MESH = pl.DeviceIdType.MESH
F32 = jnp.float32
BF16 = jnp.bfloat16
ANY = pl.BlockSpec(memory_space=pl.ANY)
VM = pl.BlockSpec(memory_space=pltpu.VMEM)
SM = pl.BlockSpec(memory_space=pltpu.SMEM)
LIMIT = 60 * 1024 * 1024
NC = 6
HC = NC // 2
EARLY = 2


def main_kernel(
    ids_ref, emb_ref, du_ref, w_ref, g_ref, dres_ref,
    xo_ref, n_ref, u_ref, dxo_ref, dxp_ref, dg_ref,
    idv, ev, oh, xp, xr, xfw, x1, x2, xh, xpr, drw, gv, wv, duv, pb, pr, sf, rf, r1, r2, nall, acc, dxs, dxr,
    dgm, dgr, dgc, dgn,
    id_s, e_s, du_s, g_s, w_s, dl_s, dr_s, dr_r, xd_s, xd_r, xo_s, xo_r, pd_s, pd_r,
    xa_s, xb_s, xc_s, xa_r, xb_r, xc_r, da_s, db_s, dc_s, da_r, db_r, dc_r,
    ga_s, gb_s, gc_s, ga_r, gb_r, gc_r, h0_s, h0_r, h1_s, h2_s, h3_s, h1_r, h2_r, h3_r,
    no_s, dx_s, dx_r, ox_s, dg_s, dg_r,
):
    me = lax.axis_index("tp")
    c = me % 2
    q = me // 2
    xq = q % 2
    yq = q // 2
    qx = q + 1 - 2 * xq
    qy = q + 2 - 4 * yq
    qd = 3 - q
    part = me + 1 - 2 * c
    dx_ = me + 2 - 4 * xq
    dy_ = me + 4 - 8 * yq
    dd_ = 2 * qd + c
    oc = 1 - c
    d = w_ref.shape[0]
    cw = d // NC
    vl = emb_ref.shape[0]
    tq = xr.shape[2]
    nt = 8 * tq
    th = tq // 2

    def w_copy(k):
        rows = pl.ds(pl.multiple_of(k * cw, cw), cw)
        return pltpu.make_async_copy(w_ref.at[rows], wv.at[k], w_s.at[k])

    def chunk(i):
        return i % 2 * HC + i // 2

    barrier = pltpu.get_barrier_semaphore()
    for dev in (part, dx_, dy_, dd_):
        pl.semaphore_signal(barrier, inc=1, device_id={"tp": dev}, device_id_type=MESH)

    id_copy = pltpu.make_async_copy(ids_ref, idv, id_s)
    du_copy = pltpu.make_async_copy(du_ref, duv, du_s)
    g_copy = pltpu.make_async_copy(g_ref, gv, g_s)
    dl_copy = pltpu.make_async_copy(dres_ref.at[c], drw.at[c], dl_s)
    def e_copy(i):
        cols = pl.ds(pl.multiple_of(chunk(i) * cw, cw), cw)
        return pltpu.make_async_copy(emb_ref.at[:, cols], ev.at[i % 2], e_s.at[i % 2])

    du_copy.start()

    @pl.loop(0, NC)
    def _(i):
        w_copy(chunk(i)).start()

    id_copy.start()
    g_copy.start()
    dl_copy.start()
    e_copy(0).start()
    e_copy(1).start()
    pl.semaphore_wait(barrier, 4)

    def remote(src, dst, ss, rs, dev):
        return pltpu.make_async_remote_copy(
            src_ref=src, dst_ref=dst, send_sem=ss, recv_sem=rs, device_id={"tp": dev}, device_id_type=MESH
        )

    def xd(k):
        return remote(xp.at[k, oc], xr.at[k], xd_s.at[k], xd_r.at[k], part)

    dr = remote(dres_ref.at[oc], drw.at[c], dr_s, dr_r, part)

    def first(k):
        b = k // HC
        return qx + (qy - qx) * b, dx_ + (dy_ - dx_) * b

    def second(k):
        b = k // HC
        return qy + (qx - qy) * b, dy_ + (dx_ - dy_) * b

    def xa(k):
        return remote(xp.at[k, c, qd], xfw.at[k], xa_s.at[k], xa_r.at[k], first(k)[1])

    def xb(k):
        return remote(xp.at[k, c, first(k)[0]], x1.at[k], xb_s.at[k], xb_r.at[k], first(k)[1])

    def xc(k):
        return remote(xp.at[k, c, second(k)[0]], x2.at[k], xc_s.at[k], xc_r.at[k], second(k)[1])

    def da(k):
        return remote(sf.at[k, qd], rf.at[k], da_s.at[k], da_r.at[k], first(k)[1])

    def db(k):
        return remote(sf.at[k, first(k)[0]], r1.at[k], db_s.at[k], db_r.at[k], first(k)[1])

    def dc(k):
        return remote(sf.at[k, second(k)[0]], r2.at[k], dc_s.at[k], dc_r.at[k], second(k)[1])

    def pd(k):
        return remote(pb.at[k, oc], pr.at[k], pd_s.at[k], pd_r.at[k], part)

    def ga(k):
        return remote(nall.at[k, c, q], nall.at[k, c, q], ga_s.at[k], ga_r.at[k], first(k)[1])

    def gb(k):
        return remote(nall.at[k, c, q], nall.at[k, c, q], gb_s.at[k], gb_r.at[k], second(k)[1])

    def gc(k):
        s = first(k)[0]
        return remote(nall.at[k, c, s], nall.at[k, c, s], gc_s.at[k], gc_r.at[k], second(k)[1])

    def over(k, s, ss, rs):
        return remote(nall.at[k, c, s], nall.at[k, c, s], ss.at[k], rs.at[k], part)

    def h1(k):
        return over(k, first(k)[0], h1_s, h1_r)

    def h2(k):
        return over(k, second(k)[0], h2_s, h2_r)

    def h3(k):
        return over(k, qd, h3_s, h3_r)

    h0 = remote(nall.at[:, c, q], nall.at[:, c, q], h0_s, h0_r, part)

    du_copy.wait()

    def matmul(i):
        k = chunk(i)
        w_copy(k).wait()
        p = lax.dot_general(
            duv[...].reshape(nt, -1), wv[k], (((1,), (1,)), ((), ())), preferred_element_type=F32
        )
        pb[k] = p.astype(BF16).reshape(2, 4, tq, cw)
        pd(k).start()

    def combine(i):
        k = chunk(i)
        pd(k).wait_recv()
        for s in range(4):
            sf[k, s] = pb[k, c, s].astype(F32) + pr[k, s].astype(F32)
        da(k).start()

    matmul(0)

    @pl.loop(1, NC)
    def _(i):
        matmul(i)
        combine(i - 1)

    id_copy.wait()
    lo = me * vl
    for b in range(nt // 128):
        m, t0 = divmod(b * 128, 4 * tq)
        row = idv[m : m + 1, t0 : t0 + 128] - lo
        col = jnp.broadcast_to(row, (128, 128)).T

        @pl.loop(0, vl // 128, unroll=8)
        def _(j):
            lanes = lax.broadcasted_iota(jnp.int32, (128, 128), 1) + j * 128
            cols = pl.ds(pl.multiple_of(j * 128, 128), 128)
            oh[b * 128 : (b + 1) * 128, cols] = jnp.where(lanes == col, 1.0, 0.0).astype(BF16)

    combine(NC - 1)
    dr.start()

    def lookup(i):
        k = chunk(i)
        e_copy(i).wait()
        p = jnp.dot(oh[...], ev[i % 2], preferred_element_type=F32)
        xp[k] = p.astype(BF16).reshape(2, 4, tq, cw)
        xd(k).start()

        @pl.when(i + 2 < NC)
        def _():
            e_copy(i + 2).start()

    def pair(i):
        k = chunk(i)
        xd(k).wait_recv()
        xp[k, c] = xp[k, c] + xr[k]
        xa(k).start()
        xb(k).start()

    def forward(i):
        k = chunk(i)
        s = second(k)[0]
        da(k).wait_recv()
        sf[k, s] = sf[k, s] + rf[k]
        dc(k).start()

    db(chunk(0)).start()
    db(chunk(1)).start()
    lookup(0)

    @pl.loop(1, NC)
    def _(i):
        @pl.when(i + 1 < NC)
        def _():
            db(chunk(i + 1)).start()

        @pl.when(i >= NC - EARLY)
        def _():
            forward(i - (NC - EARLY))

        lookup(i)
        pair(i - 1)

    pair(NC - 1)

    @pl.loop(0, NC)
    def _(i):
        k = chunk(i)
        s = second(k)[0]
        xa(k).wait_recv()
        xp[k, c, s] = xp[k, c, s] + xfw[k]
        xc(k).start()

    @pl.loop(EARLY, NC)
    def _(i):
        forward(i)

    acc[...] = jnp.zeros_like(acc)

    g_copy.wait()
    sq = jnp.zeros((tq, 1), F32)
    for k in range(NC):
        xb(k).wait_recv()
        xc(k).wait_recv()
        xk = xp[k, c, q] + x1[k] + x2[k]
        xh[k] = xk
        xk = xk.astype(F32)
        sq = sq + jnp.sum(xk * xk, axis=-1, keepdims=True)
    xo = remote(xh.at[:, pl.ds(pl.multiple_of(oc * th, th), th), :], xpr, xo_s, xo_r, part)
    xo.start()
    rs = lax.rsqrt(sq * (1.0 / d) + EPS)
    for k in (0, 3, 1, 4, 2, 5):
        cols = slice(k * cw, (k + 1) * cw)
        nall[k, c, q] = ((xh[k].astype(F32) * rs) * gv[cols].astype(F32).reshape(1, cw)).astype(BF16)
        ga(k).start()
    for k in (0, 3, 1, 4, 2, 5):
        gb(k).start()
    h0.start()
    for k in range(NC):
        xo_ref[c, :, k * cw : (k + 1) * cw] = xh[k, pl.ds(pl.multiple_of(c * th, th), th), :]
    dl_copy.wait()
    dr.wait_recv()
    xo.wait_recv()
    for k in range(NC):
        xo_ref[oc, :, k * cw : (k + 1) * cw] = xpr[k]

    m = jnp.zeros((tq, 1), F32)
    for k in range(NC):
        cols = slice(k * cw, (k + 1) * cw)
        db(k).wait_recv()
        dc(k).wait_recv()
        dn = sf[k, q] + r1[k] + r2[k]
        r1[k] = dn
        nh = xh[k].astype(F32) * rs
        dnh = dn * nh
        dgm[:, cols] = jnp.sum(dnh, axis=0, keepdims=True)
        m = m + jnp.sum(dnh * gv[cols].astype(F32).reshape(1, cw), axis=-1, keepdims=True)
    dg0 = remote(dgm, dgr, dg_s.at[0], dg_r.at[0], part)
    dg0.start()
    m = m * (1.0 / d)
    for k in range(NC):
        cols = slice(k * cw, (k + 1) * cw)
        nh = xh[k].astype(F32) * rs
        dxn = rs * (gv[cols].astype(F32).reshape(1, cw) * r1[k] - nh * m)
        dxs[k] = (drw[:, :, cols].reshape(tq, cw).astype(F32) + dxn).astype(BF16)
    dxc = remote(dxs, dxr, dx_s, dx_r, part)
    dxc.start()
    ox = pltpu.make_async_copy(dxs, dxo_ref, ox_s.at[0])
    ox.start()
    dg0.wait_recv()
    dgc[...] = dgm[...] + dgr[...]
    dgs = [remote(dgc, dgn.at[j], dg_s.at[1 + j], dg_r.at[1 + j], dev) for j, dev in enumerate((dx_, dy_, dd_))]
    for cp in dgs:
        cp.start()

    @pl.loop(0, NC)
    def _(i):
        k = chunk(i)
        ga(k).wait_recv()
        gc(k).start()
        h1(k).start()

    @pl.loop(0, NC)
    def _(i):
        k = chunk(i)
        gb(k).wait_recv()
        h2(k).start()

    dxc.wait_recv()
    oy = pltpu.make_async_copy(dxr, dxp_ref, ox_s.at[1])
    oy.start()
    for cp in dgs:
        cp.wait_recv()
    dg_ref[...] = (dgc[...] + dgn[0]) + (dgn[1] + dgn[2])

    def n_out(k):
        return pltpu.make_async_copy(nall.at[k], n_ref.at[k], no_s.at[k])

    def arrive(i):
        k = chunk(i)
        gc(k).wait_recv()
        h3(k).start()

    def project(i):
        k = chunk(i)
        h1(k).wait_recv()
        h2(k).wait_recv()
        h3(k).wait_recv()
        n_out(k).start()
        acc[...] += jnp.dot(nall[k].reshape(nt, cw), wv[k], preferred_element_type=F32)

    h0.wait_recv()
    arrive(0)

    @pl.loop(1, NC)
    def _(i):
        arrive(i)
        project(i - 1)

    project(NC - 1)
    u_ref[...] = acc[...].astype(BF16)

    ox.wait()
    oy.wait()
    dr.wait_send()
    xo.wait_send()
    h0.wait_send()
    dg0.wait_send()
    dxc.wait_send()
    for cp in dgs:
        cp.wait_send()

    @pl.loop(0, NC)
    def _(k):
        n_out(k).wait()
        for f in (xd, pd, xa, xb, xc, da, db, dc, ga, gb, gc, h1, h2, h3):
            f(k).wait_send()


def fill_kernel(
    n_ref, du_ref, u_ref, x_ref, dg_ref, dw_ref, de_ref, uo_ref, xo_ref, dgo_ref,
    nv, duv, st, z, uv, xv, gv, n_s, du_s, o_s, z_s, p_s, *, rows,
):
    cw = nv.shape[2]
    zr = z.shape[0]
    du_copy = pltpu.make_async_copy(du_ref, duv, du_s)
    du_copy.start()

    def n_copy(k):
        return pltpu.make_async_copy(n_ref.at[k], nv.at[k], n_s.at[k])

    def out(k):
        r = pl.ds(pl.multiple_of(k * cw, cw), cw)
        return pltpu.make_async_copy(st.at[k % 2], dw_ref.at[r], o_s.at[k % 2])

    def put(i):
        return pltpu.make_async_copy(z, de_ref.at[pl.ds(pl.multiple_of(i * zr, zr), zr)], z_s)

    for k in range(NC):
        n_copy(k).start()
    small = ((u_ref, uv, uo_ref), (x_ref, xv, xo_ref), (dg_ref, gv, dgo_ref))
    ins = [pltpu.make_async_copy(a, v, p_s.at[j]) for j, (a, v, _) in enumerate(small)]
    outs = [pltpu.make_async_copy(v, o, p_s.at[j]) for j, (_, v, o) in enumerate(small)]
    for cp in ins:
        cp.start()
    z[...] = jnp.zeros_like(z)
    per = rows // zr // NC
    du_copy.wait()

    @pl.loop(0, NC)
    def _(k):
        n_copy(k).wait()
        for j in range(per):
            put(k * per + j).start()

        @pl.when(k >= 2)
        def _():
            out(k - 2).wait()

        st[k % 2] = lax.dot_general(nv[k], duv[...], (((0,), (0,)), ((), ())), preferred_element_type=F32)
        out(k).start()

    for cp, co in zip(ins, outs):
        cp.wait()
        co.start()
    for co in outs:
        co.wait()
    out(NC - 2).wait()
    out(NC - 1).wait()

    @pl.loop(0, per * NC)
    def _(i):
        put(i).wait()


def list_kernel(ids_ref, idv_ref, _, row_ref, cnt_ref, sel_ref, de_ref, z, sel, fv, fs, z_s, f_s, *, rows):
    zr = z.shape[0]
    mb, tm = idv_ref.shape
    nt = mb * tm
    vl = de_ref.shape[0]
    left = (vl - rows) // zr
    lo = lax.axis_index("tp") * vl

    def put(i):
        return pltpu.make_async_copy(z, de_ref.at[pl.ds(pl.multiple_of(rows + i * zr, zr), zr)], z_s)

    z[...] = jnp.zeros_like(z)

    @pl.loop(0, left)
    def _(i):
        put(i).start()

    for m in range(mb):
        row = idv_ref[m : m + 1, :] - lo
        later = jnp.zeros((1, tm), jnp.int32)
        for b in range(nt // 128):
            m0, t0 = divmod(b * 128, tm)
            col = jnp.broadcast_to(idv_ref[m0 : m0 + 1, t0 : t0 + 128] - lo, (128, 128)).T
            col = jnp.concatenate([col] * (tm // 128), axis=1)
            pos = lax.broadcasted_iota(jnp.int32, (128, tm), 0) + b * 128
            mine = lax.broadcasted_iota(jnp.int32, (128, tm), 1) + m * tm
            hit = jnp.where((col == row) & (pos < mine), 1, 0)
            later = jnp.maximum(later, jnp.max(hit, axis=0, keepdims=True))
        fv[:, m * tm : (m + 1) * tm] = jnp.where((row >= 0) & (row < vl), 1 - later, 0)
    cp = pltpu.make_async_copy(fv, fs, f_s)
    cp.start()
    sel[...] = jnp.zeros_like(sel)
    cp.wait()

    def scan(t, n):
        row_ref[n] = ids_ref[t // tm, t % tm] - lo
        return n + fs[0, t]

    cnt = lax.fori_loop(0, nt, scan, jnp.int32(0), unroll=8)
    cnt_ref[0] = cnt

    @pl.loop(0, cnt)
    def _(j):
        v = row_ref[j] + lo
        for m in range(mb):
            sel[pl.ds(j, 1), m * tm : (m + 1) * tm] = jnp.where(idv_ref[m : m + 1, :] == v, 1.0, 0.0)

    sel_ref[...] = sel[...].astype(BF16)

    @pl.loop(0, left)
    def _(i):
        put(i).wait()


def rows_kernel(*refs):
    row_ref, cnt_ref, sel_ref = refs[:3]
    dx_refs = refs[3:11]
    _, de_ref, dxv, dxs, o_s = refs[11:]
    nt = sel_ref.shape[0]
    cw = dxv.shape[-1]
    rb = 128
    me = lax.axis_index("tp")
    c = me % 2
    q = me // 2
    qx = q + 1 - 2 * (q % 2)
    qy = q + 2 - 4 * (q // 2)
    where = [(b, s) for b in (c, 1 - c) for s in (q, qx, qy, 3 - q)]
    for r, (b, s) in zip(dx_refs, where):
        dxv[:, b, s] = r[...]
    cnt = cnt_ref[0]

    def put(j):
        return pltpu.make_async_copy(dxs.at[pl.ds(j, 1)], de_ref.at[pl.ds(row_ref[j], 1)], o_s)

    @pl.loop(0, (cnt + rb - 1) // rb)
    def _(b):
        r = pl.ds(pl.multiple_of(b * rb, rb), rb)
        for k in range(NC):
            dxs[r, k * cw : (k + 1) * cw] = jnp.dot(
                sel_ref[r, :], dxv[k].reshape(nt, cw), preferred_element_type=F32
            )

        @pl.loop(b * rb, jnp.minimum(b * rb + rb, cnt))
        def _(j):
            put(j).start()

    @pl.loop(0, cnt)
    def _(j):
        put(j).wait()


def solution(mesh):
    groups = mesh.shape["tp"]

    def shift(bit):
        return [(r, r ^ bit) for r in range(groups)]

    def send(a, bit):
        return lax.ppermute(a, "tp", shift(bit))

    def local(ids, emb, g, w, du, dres):
        mb, t = ids.shape
        vl, d = emb.shape
        f = w.shape[1]
        nt = mb * t
        cw = d // NC
        tq = t // 4
        dma = pltpu.SemaphoreType.DMA
        sds = jax.ShapeDtypeStruct
        vb = lambda *s: pltpu.VMEM(s, BF16)
        vf = lambda *s: pltpu.VMEM(s, F32)
        local_only = pltpu.CompilerParams(vmem_limit_bytes=LIMIT)

        blk = (NC, tq, cw)
        x, n, u, dxo, dxp, dg = pl.pallas_call(
            main_kernel,
            out_shape=(
                sds((2, tq // 2, d), BF16),
                sds((NC, 2, 4, tq, cw), BF16),
                sds((nt, f), BF16),
                sds(blk, BF16),
                sds(blk, BF16),
                sds((1, d), F32),
            ),
            in_specs=[ANY] * 6,
            out_specs=(VM, ANY, VM, ANY, ANY, VM),
            scratch_shapes=[
                pltpu.VMEM((mb, t), jnp.int32), vb(2, vl, cw), vb(nt, vl),
                vb(NC, 2, 4, tq, cw), vb(NC, 4, tq, cw), vb(*blk), vb(*blk), vb(*blk),
                vb(*blk), vb(NC, tq // 2, cw), vb(2, tq // 2, d), vb(d),
                vb(NC, cw, f), vb(2, t, f),
                vb(NC, 2, 4, tq, cw), vb(NC, 4, tq, cw),
                vf(NC, 4, tq, cw), vf(*blk), vf(*blk), vf(*blk),
                vb(NC, 2, 4, tq, cw), vf(nt, f), vb(*blk), vb(*blk),
                vf(1, d), vf(1, d), vf(1, d), vf(3, 1, d),
                dma(()), dma((2,)), dma(()), dma(()), dma((NC,)), dma(()), dma(()), dma(()), dma((NC,)), dma((NC,)),
                dma(()), dma(()), dma((NC,)), dma((NC,)),
            ]
            + [dma((NC,))] * 18
            + [dma(())] * 2
            + [dma((NC,))] * 7
            + [dma(()), dma(()), dma((2,)), dma((4,)), dma((4,))],
            compiler_params=pltpu.CompilerParams(collective_id=0, has_side_effects=True, vmem_limit_bytes=LIMIT),
            name="main",
        )(ids, emb, du, w, g, dres)

        zr = 128
        rows = vl // zr * 9 // 16 // NC * NC * zr
        near = [send(dxo, b) for b in (2, 4, 6)]
        dw, de, u, x, dg = pl.pallas_call(
            functools.partial(fill_kernel, rows=rows),
            out_shape=(sds((d, f), F32), sds((vl, d), F32), sds((nt, f), BF16), sds(x.shape, BF16), sds((1, d), F32)),
            in_specs=[ANY] * 5,
            out_specs=(ANY,) * 5,
            scratch_shapes=[
                vb(NC, nt, cw), vb(nt, f), vf(2, cw, f), vf(zr, d), vb(nt, f), vb(*x.shape), vf(1, d),
                dma((NC,)), dma(()), dma((2,)), dma(()), dma((3,)),
            ],
            compiler_params=local_only,
            cost_estimate=pl.CostEstimate(flops=18_000_000_000, bytes_accessed=vl * d * 4, transcendentals=0),
            name="fill",
        )(n.reshape(NC, nt, cw), du.reshape(nt, f), u, x, dg)
        far = [send(a, 1) for a in near]

        row, cnt, sel, de = pl.pallas_call(
            functools.partial(list_kernel, rows=rows),
            out_shape=(sds((nt + 8,), jnp.int32), sds((1,), jnp.int32), sds((nt, nt), BF16), sds((vl, d), F32)),
            in_specs=[SM, VM, ANY],
            out_specs=(SM, SM, VM, ANY),
            input_output_aliases={2: 3},
            scratch_shapes=[
                vf(zr, d), vf(nt, nt), pltpu.VMEM((1, nt), jnp.int32), pltpu.SMEM((1, nt), jnp.int32),
                dma(()), dma(()),
            ],
            compiler_params=pltpu.CompilerParams(vmem_limit_bytes=16 * 1024 * 1024),
            cost_estimate=pl.CostEstimate(flops=8_000_000_000, bytes_accessed=(vl - rows) * d * 4, transcendentals=0),
            name="list",
        )(ids, ids, de)
        de = pl.pallas_call(
            rows_kernel,
            out_shape=sds((vl, d), F32),
            in_specs=[SM, SM, VM] + [VM] * 8 + [ANY],
            out_specs=ANY,
            input_output_aliases={11: 0},
            scratch_shapes=[vb(NC, 2, 4, tq, cw), vf(nt, d), dma(())],
            compiler_params=pltpu.CompilerParams(vmem_limit_bytes=24 * 1024 * 1024),
            name="rows",
        )(row, cnt, sel, dxo, *near, dxp, *far, de)
        return u.reshape(mb, t, f), x, de, dw, dg.reshape(d)

    return jax.shard_map(
        local,
        mesh=mesh,
        in_specs=(P("dp", None), P("tp", None), P(None), P(None, "tp"), P("dp", None, "tp"), P("dp", "tp", None)),
        out_specs=(P("dp", None, "tp"), P("dp", "tp", None), P(("dp", "tp"), None), P(None, ("dp", "tp")), P("dp")),
        check_vma=False,
    )
```

```python
import functools

import jax
import jax.numpy as jnp
from jax import lax
from jax.experimental import pallas as pl
from jax.experimental.pallas import tpu as pltpu
from jax.sharding import PartitionSpec as P

EPS = 1e-6
MESH = pl.DeviceIdType.MESH
F32 = jnp.float32
BF16 = jnp.bfloat16
ANY = pl.BlockSpec(memory_space=pl.ANY)
VM = pl.BlockSpec(memory_space=pltpu.VMEM)
SM = pl.BlockSpec(memory_space=pltpu.SMEM)
LIMIT = 60 * 1024 * 1024
NC = 6
HC = NC // 2
LATE = 2
EARLY = 2


def main_kernel(
    ids_ref, emb_ref, du_ref, w_ref, g_ref, dres_ref,
    xo_ref, n_ref, u_ref, dxo_ref, dxp_ref, dg_ref,
    idv, ev, oh, xp, xr, xfw, x1, x2, xh, xpr, drw, gv, wv, duv, pb, pr, sf, rf, r1, r2, nall, acc, ub, dxs, dxr,
    dgm, dgr, dgc, dgn,
    id_s, e_s, du_s, g_s, w_s, dl_s, dr_s, dr_r, xd_s, xd_r, xo_s, xo_r, pd_s, pd_r,
    xa_s, xb_s, xc_s, xa_r, xb_r, xc_r, da_s, db_s, dc_s, da_r, db_r, dc_r,
    ga_s, gb_s, gc_s, ga_r, gb_r, gc_r, h0_s, h0_r, h1_s, h2_s, h3_s, h1_r, h2_r, h3_r,
    no_s, uo_s, dx_s, dx_r, ox_s, dg_s, dg_r,
):
    me = lax.axis_index("tp")
    c = me % 2
    q = me // 2
    xq = q % 2
    yq = q // 2
    qx = q + 1 - 2 * xq
    qy = q + 2 - 4 * yq
    qd = 3 - q
    part = me + 1 - 2 * c
    dx_ = me + 2 - 4 * xq
    dy_ = me + 4 - 8 * yq
    dd_ = 2 * qd + c
    oc = 1 - c
    d, f = w_ref.shape
    cw = d // NC
    vl = emb_ref.shape[0]
    tq = xr.shape[2]
    nt = 8 * tq
    th = tq // 2

    def w_copy(k):
        rows = pl.ds(pl.multiple_of(k * cw, cw), cw)
        return pltpu.make_async_copy(w_ref.at[rows], wv.at[k], w_s.at[k])

    def chunk(i):
        return i % 2 * HC + i // 2

    barrier = pltpu.get_barrier_semaphore()
    for dev in (part, dx_, dy_, dd_):
        pl.semaphore_signal(barrier, inc=1, device_id={"tp": dev}, device_id_type=MESH)

    id_copy = pltpu.make_async_copy(ids_ref, idv, id_s)
    du_copy = pltpu.make_async_copy(du_ref, duv, du_s)
    g_copy = pltpu.make_async_copy(g_ref, gv, g_s)
    dl_copy = pltpu.make_async_copy(dres_ref.at[c], drw.at[c], dl_s)
    def e_copy(i):
        cols = pl.ds(pl.multiple_of(chunk(i) * cw, cw), cw)
        return pltpu.make_async_copy(emb_ref.at[:, cols], ev.at[i % 2], e_s.at[i % 2])

    du_copy.start()

    @pl.loop(0, NC)
    def _(i):
        w_copy(chunk(i)).start()

    id_copy.start()
    g_copy.start()
    dl_copy.start()
    e_copy(0).start()
    e_copy(1).start()
    pl.semaphore_wait(barrier, 4)

    def remote(src, dst, ss, rs, dev):
        return pltpu.make_async_remote_copy(
            src_ref=src, dst_ref=dst, send_sem=ss, recv_sem=rs, device_id={"tp": dev}, device_id_type=MESH
        )

    def xd(k):
        return remote(xp.at[k, oc], xr.at[k], xd_s.at[k], xd_r.at[k], part)

    dr = remote(dres_ref.at[oc], drw.at[c], dr_s, dr_r, part)

    def first(k):
        b = k // HC
        return qx + (qy - qx) * b, dx_ + (dy_ - dx_) * b

    def second(k):
        b = k // HC
        return qy + (qx - qy) * b, dy_ + (dx_ - dy_) * b

    def xa(k):
        return remote(xp.at[k, c, qd], xfw.at[k], xa_s.at[k], xa_r.at[k], first(k)[1])

    def xb(k):
        return remote(xp.at[k, c, first(k)[0]], x1.at[k], xb_s.at[k], xb_r.at[k], first(k)[1])

    def xc(k):
        return remote(xp.at[k, c, second(k)[0]], x2.at[k], xc_s.at[k], xc_r.at[k], second(k)[1])

    def da(k):
        return remote(sf.at[k, qd], rf.at[k], da_s.at[k], da_r.at[k], first(k)[1])

    def db(k):
        return remote(sf.at[k, first(k)[0]], r1.at[k], db_s.at[k], db_r.at[k], first(k)[1])

    def dc(k):
        return remote(sf.at[k, second(k)[0]], r2.at[k], dc_s.at[k], dc_r.at[k], second(k)[1])

    def pd(k):
        return remote(pb.at[k, oc], pr.at[k], pd_s.at[k], pd_r.at[k], part)

    def ga(k):
        return remote(nall.at[k, c, q], nall.at[k, c, q], ga_s.at[k], ga_r.at[k], first(k)[1])

    def gb(k):
        return remote(nall.at[k, c, q], nall.at[k, c, q], gb_s.at[k], gb_r.at[k], second(k)[1])

    def gc(k):
        s = first(k)[0]
        return remote(nall.at[k, c, s], nall.at[k, c, s], gc_s.at[k], gc_r.at[k], second(k)[1])

    def over(k, s, ss, rs):
        return remote(nall.at[k, c, s], nall.at[k, c, s], ss.at[k], rs.at[k], part)

    def h1(k):
        return over(k, first(k)[0], h1_s, h1_r)

    def h2(k):
        return over(k, second(k)[0], h2_s, h2_r)

    def h3(k):
        return over(k, qd, h3_s, h3_r)

    h0 = remote(nall.at[:, c, q], nall.at[:, c, q], h0_s, h0_r, part)

    du_copy.wait()

    def matmul(i):
        k = chunk(i)
        w_copy(k).wait()
        p = lax.dot_general(
            duv[...].reshape(nt, -1), wv[k], (((1,), (1,)), ((), ())), preferred_element_type=F32
        )
        pb[k] = p.astype(BF16).reshape(2, 4, tq, cw)
        pd(k).start()

    def combine(i):
        k = chunk(i)
        pd(k).wait_recv()
        for s in range(4):
            sf[k, s] = pb[k, c, s].astype(F32) + pr[k, s].astype(F32)
        da(k).start()

    matmul(0)

    @pl.loop(1, NC)
    def _(i):
        matmul(i)
        combine(i - 1)

    id_copy.wait()
    lo = me * vl
    for b in range(nt // 128):
        m, t0 = divmod(b * 128, 4 * tq)
        row = idv[m : m + 1, t0 : t0 + 128] - lo
        col = jnp.broadcast_to(row, (128, 128)).T

        @pl.loop(0, vl // 128, unroll=8)
        def _(j):
            lanes = lax.broadcasted_iota(jnp.int32, (128, 128), 1) + j * 128
            cols = pl.ds(pl.multiple_of(j * 128, 128), 128)
            oh[b * 128 : (b + 1) * 128, cols] = jnp.where(lanes == col, 1.0, 0.0).astype(BF16)

    combine(NC - 1)
    dr.start()

    def lookup(i):
        k = chunk(i)
        e_copy(i).wait()
        p = jnp.dot(oh[...], ev[i % 2], preferred_element_type=F32)
        xp[k] = p.astype(BF16).reshape(2, 4, tq, cw)
        xd(k).start()

        @pl.when(i + 2 < NC)
        def _():
            e_copy(i + 2).start()

    def pair(i):
        k = chunk(i)
        xd(k).wait_recv()
        xp[k, c] = xp[k, c] + xr[k]
        xa(k).start()
        xb(k).start()

    def forward(i):
        k = chunk(i)
        s = second(k)[0]
        da(k).wait_recv()
        sf[k, s] = sf[k, s] + rf[k]
        dc(k).start()

    db(chunk(0)).start()
    db(chunk(1)).start()
    lookup(0)

    @pl.loop(1, NC)
    def _(i):
        @pl.when(i + 1 < NC)
        def _():
            db(chunk(i + 1)).start()

        @pl.when(i >= NC - EARLY)
        def _():
            forward(i - (NC - EARLY))

        lookup(i)
        pair(i - 1)

    pair(NC - 1)

    @pl.loop(0, NC)
    def _(i):
        k = chunk(i)
        s = second(k)[0]
        xa(k).wait_recv()
        xp[k, c, s] = xp[k, c, s] + xfw[k]
        xc(k).start()

    @pl.loop(EARLY, NC)
    def _(i):
        forward(i)

    acc[...] = jnp.zeros_like(acc)

    g_copy.wait()
    sq = jnp.zeros((tq, 1), F32)
    for k in range(NC):
        xb(k).wait_recv()
        xc(k).wait_recv()
        xk = xp[k, c, q] + x1[k] + x2[k]
        xh[k] = xk
        xk = xk.astype(F32)
        sq = sq + jnp.sum(xk * xk, axis=-1, keepdims=True)
    xo = remote(xh.at[:, pl.ds(pl.multiple_of(oc * th, th), th), :], xpr, xo_s, xo_r, part)
    xo.start()
    rs = lax.rsqrt(sq * (1.0 / d) + EPS)
    for k in (0, 3, 1, 4, 2, 5):
        cols = slice(k * cw, (k + 1) * cw)
        nall[k, c, q] = ((xh[k].astype(F32) * rs) * gv[cols].astype(F32).reshape(1, cw)).astype(BF16)
        ga(k).start()
    for k in (0, 3, 1, 4, 2, 5):
        gb(k).start()
    h0.start()
    for k in range(NC):
        xo_ref[c, :, k * cw : (k + 1) * cw] = xh[k, pl.ds(pl.multiple_of(c * th, th), th), :]
    dl_copy.wait()
    dr.wait_recv()
    xo.wait_recv()
    for k in range(NC):
        xo_ref[oc, :, k * cw : (k + 1) * cw] = xpr[k]

    def piece(k, s):
        acc[:, s] += jnp.dot(nall[k, :, s].reshape(2 * tq, cw), wv[k], preferred_element_type=F32).reshape(2, tq, f)

    def u_out(j, s):
        ub[:, s] = acc[:, s].astype(BF16)
        return pltpu.make_async_copy(ub.at[:, s], u_ref.at[:, s], uo_s.at[j])

    h0.wait_recv()

    @pl.loop(0, NC)
    def _(k):
        piece(k, q)

    uo = [u_out(0, q)]
    uo[0].start()

    m = jnp.zeros((tq, 1), F32)
    for k in (0, 3, 1, 4, 2, 5):
        cols = slice(k * cw, (k + 1) * cw)
        db(k).wait_recv()
        dc(k).wait_recv()
        dn = sf[k, q] + r1[k] + r2[k]
        r1[k] = dn
        nh = xh[k].astype(F32) * rs
        dnh = dn * nh
        dgm[:, cols] = jnp.sum(dnh, axis=0, keepdims=True)
        m = m + jnp.sum(dnh * gv[cols].astype(F32).reshape(1, cw), axis=-1, keepdims=True)
    dg0 = remote(dgm, dgr, dg_s.at[0], dg_r.at[0], part)
    dg0.start()
    m = m * (1.0 / d)
    for k in range(NC):
        cols = slice(k * cw, (k + 1) * cw)
        nh = xh[k].astype(F32) * rs
        dxn = rs * (gv[cols].astype(F32).reshape(1, cw) * r1[k] - nh * m)
        dxs[k] = (drw[:, :, cols].reshape(tq, cw).astype(F32) + dxn).astype(BF16)
    dxc = remote(dxs, dxr, dx_s, dx_r, part)
    dxc.start()
    ox = pltpu.make_async_copy(dxs, dxo_ref, ox_s.at[0])
    ox.start()
    dg0.wait_recv()
    dgc[...] = dgm[...] + dgr[...]
    dgs = [remote(dgc, dgn.at[j], dg_s.at[1 + j], dg_r.at[1 + j], dev) for j, dev in enumerate((dx_, dy_, dd_))]
    for cp in dgs:
        cp.start()

    @pl.loop(0, NC)
    def _(i):
        k = chunk(i)
        ga(k).wait_recv()
        gc(k).start()
        h1(k).start()

    dxc.wait_recv()
    oy = pltpu.make_async_copy(dxr, dxp_ref, ox_s.at[1])
    oy.start()

    @pl.loop(0, NC)
    def _(i):
        k = chunk(i)
        h1(k).wait_recv()
        piece(k, first(k)[0])

    def n_out(k):
        return pltpu.make_async_copy(nall.at[k], n_ref.at[k], no_s.at[k])

    def second_in(i):
        k = chunk(i)
        gb(k).wait_recv()
        h2(k).start()

    def second_use(i):
        k = chunk(i)
        h2(k).wait_recv()
        piece(k, second(k)[0])

    def last_in(i):
        k = chunk(i)
        gc(k).wait_recv()
        h3(k).start()

    def last_use(i):
        k = chunk(i)
        h3(k).wait_recv()
        n_out(k).start()
        piece(k, qd)

    second_in(0)

    @pl.loop(1, NC)
    def _(i):
        second_in(i)
        second_use(i - 1)

    last_in(0)
    second_use(NC - 1)
    for j, s in enumerate((qx, qy)):
        uo.append(u_out(1 + j, s))
        uo[-1].start()

    @pl.loop(1, NC)
    def _(i):
        last_in(i)
        last_use(i - 1)

    last_use(NC - 1)
    uo.append(u_out(3, qd))
    uo[-1].start()
    for cp in dgs:
        cp.wait_recv()
    dg_ref[...] = (dgc[...] + dgn[0]) + (dgn[1] + dgn[2])
    for cp in uo:
        cp.wait()

    ox.wait()
    oy.wait()
    dr.wait_send()
    xo.wait_send()
    h0.wait_send()
    dg0.wait_send()
    dxc.wait_send()
    for cp in dgs:
        cp.wait_send()

    @pl.loop(0, NC)
    def _(k):
        n_out(k).wait()
        for cp in (xd, pd, xa, xb, xc, da, db, dc, ga, gb, gc, h1, h2, h3):
            cp(k).wait_send()


def fill_kernel(
    ids_ref, idv_ref, n_ref, du_ref, u_ref, x_ref, dg_ref,
    row_ref, cnt_ref, sel_ref, dw_ref, de_ref, uo_ref, xo_ref, dgo_ref,
    nv, duv, st, z, uv, xv, gv, sel, fv, fs, n_s, du_s, o_s, z_s, p_s, f_s, *, rows,
):
    cw = nv.shape[2]
    zr = z.shape[0]
    mb, tm = idv_ref.shape
    nt = mb * tm
    vl = de_ref.shape[0]
    lo = lax.axis_index("tp") * vl
    du_copy = pltpu.make_async_copy(du_ref, duv, du_s)
    du_copy.start()

    def n_copy(k):
        return pltpu.make_async_copy(n_ref.at[k], nv.at[k], n_s.at[k])

    def out(k):
        r = pl.ds(pl.multiple_of(k * cw, cw), cw)
        return pltpu.make_async_copy(st.at[k % 2], dw_ref.at[r], o_s.at[k % 2])

    def put(i):
        return pltpu.make_async_copy(z, de_ref.at[pl.ds(pl.multiple_of(i * zr, zr), zr)], z_s)

    for k in range(NC):
        n_copy(k).start()
    small = ((u_ref, uv, uo_ref), (x_ref, xv, xo_ref), (dg_ref, gv, dgo_ref))
    ins = [pltpu.make_async_copy(a, v, p_s.at[j]) for j, (a, v, _) in enumerate(small)]
    outs = [pltpu.make_async_copy(v, o, p_s.at[j]) for j, (_, v, o) in enumerate(small)]
    for cp in ins:
        cp.start()
    z[...] = jnp.zeros_like(z)
    early = rows // zr - NC * LATE

    @pl.loop(0, early)
    def _(i):
        put(i).start()

    for m in range(mb):
        row = idv_ref[m : m + 1, :] - lo
        later = jnp.zeros((1, tm), jnp.int32)
        for b in range(nt // 128):
            m0, t0 = divmod(b * 128, tm)
            col = jnp.broadcast_to(idv_ref[m0 : m0 + 1, t0 : t0 + 128] - lo, (128, 128)).T
            col = jnp.concatenate([col] * (tm // 128), axis=1)
            pos = lax.broadcasted_iota(jnp.int32, (128, tm), 0) + b * 128
            mine = lax.broadcasted_iota(jnp.int32, (128, tm), 1) + m * tm
            hit = jnp.where((col == row) & (pos < mine), 1, 0)
            later = jnp.maximum(later, jnp.max(hit, axis=0, keepdims=True))
        fv[:, m * tm : (m + 1) * tm] = jnp.where((row >= 0) & (row < vl), 1 - later, 0)
    cp = pltpu.make_async_copy(fv, fs, f_s)
    cp.start()
    sel[...] = jnp.zeros_like(sel)
    cp.wait()

    def scan(t, n):
        row_ref[n] = ids_ref[t // tm, t % tm] - lo
        return n + fs[0, t]

    cnt = lax.fori_loop(0, nt, scan, jnp.int32(0), unroll=8)
    cnt_ref[0] = cnt

    @pl.loop(0, cnt)
    def _(j):
        v = row_ref[j] + lo
        for m in range(mb):
            sel[pl.ds(j, 1), m * tm : (m + 1) * tm] = jnp.where(idv_ref[m : m + 1, :] == v, 1.0, 0.0)

    sel_ref[...] = sel[...].astype(BF16)
    for cp, co in zip(ins, outs):
        cp.wait()
        co.start()
    du_copy.wait()

    @pl.loop(0, NC)
    def _(k):
        n_copy(k).wait()
        for j in range(LATE):
            put(early + k * LATE + j).start()

        @pl.when(k >= 2)
        def _():
            out(k - 2).wait()

        st[k % 2] = lax.dot_general(nv[k], duv[...], (((0,), (0,)), ((), ())), preferred_element_type=F32)
        out(k).start()

    for co in outs:
        co.wait()
    out(NC - 2).wait()
    out(NC - 1).wait()

    @pl.loop(0, rows // zr)
    def _(i):
        put(i).wait()


def rest_kernel(_, de_ref, z, z_s, *, rows):
    zr = z.shape[0]
    left = (de_ref.shape[0] - rows) // zr

    def put(i):
        return pltpu.make_async_copy(z, de_ref.at[pl.ds(pl.multiple_of(rows + i * zr, zr), zr)], z_s)

    z[...] = jnp.zeros_like(z)

    @pl.loop(0, left)
    def _(i):
        put(i).start()

    @pl.loop(0, left)
    def _(i):
        put(i).wait()


def rows_kernel(*refs):
    row_ref, cnt_ref, sel_ref = refs[:3]
    dx_refs = refs[3:11]
    _, de_ref, dxv, dxs, o_s = refs[11:]
    nt = sel_ref.shape[0]
    cw = dxv.shape[-1]
    rb = 128
    me = lax.axis_index("tp")
    c = me % 2
    q = me // 2
    qx = q + 1 - 2 * (q % 2)
    qy = q + 2 - 4 * (q // 2)
    where = [(b, s) for b in (c, 1 - c) for s in (q, qx, qy, 3 - q)]
    for r, (b, s) in zip(dx_refs, where):
        dxv[:, b, s] = r[...]
    cnt = cnt_ref[0]

    def put(j):
        return pltpu.make_async_copy(dxs.at[pl.ds(j, 1)], de_ref.at[pl.ds(row_ref[j], 1)], o_s)

    @pl.loop(0, (cnt + rb - 1) // rb)
    def _(b):
        r = pl.ds(pl.multiple_of(b * rb, rb), rb)
        for k in range(NC):
            dxs[r, k * cw : (k + 1) * cw] = jnp.dot(
                sel_ref[r, :], dxv[k].reshape(nt, cw), preferred_element_type=F32
            )

        @pl.loop(b * rb, jnp.minimum(b * rb + rb, cnt))
        def _(j):
            put(j).start()

    @pl.loop(0, cnt)
    def _(j):
        put(j).wait()


def solution(mesh):
    groups = mesh.shape["tp"]

    def shift(bit):
        return [(r, r ^ bit) for r in range(groups)]

    def send(a, bit):
        return lax.ppermute(a, "tp", shift(bit))

    def local(ids, emb, g, w, du, dres):
        mb, t = ids.shape
        vl, d = emb.shape
        f = w.shape[1]
        nt = mb * t
        cw = d // NC
        tq = t // 4
        dma = pltpu.SemaphoreType.DMA
        sds = jax.ShapeDtypeStruct
        vb = lambda *s: pltpu.VMEM(s, BF16)
        vf = lambda *s: pltpu.VMEM(s, F32)
        local_only = pltpu.CompilerParams(vmem_limit_bytes=LIMIT)

        blk = (NC, tq, cw)
        x, n, u, dxo, dxp, dg = pl.pallas_call(
            main_kernel,
            out_shape=(
                sds((2, tq // 2, d), BF16),
                sds((NC, 2, 4, tq, cw), BF16),
                sds((2, 4, tq, f), BF16),
                sds(blk, BF16),
                sds(blk, BF16),
                sds((1, d), F32),
            ),
            in_specs=[ANY] * 6,
            out_specs=(VM, ANY, ANY, ANY, ANY, VM),
            scratch_shapes=[
                pltpu.VMEM((mb, t), jnp.int32), vb(2, vl, cw), vb(nt, vl),
                vb(NC, 2, 4, tq, cw), vb(NC, 4, tq, cw), vb(*blk), vb(*blk), vb(*blk),
                vb(*blk), vb(NC, tq // 2, cw), vb(2, tq // 2, d), vb(d),
                vb(NC, cw, f), vb(2, t, f),
                vb(NC, 2, 4, tq, cw), vb(NC, 4, tq, cw),
                vf(NC, 4, tq, cw), vf(*blk), vf(*blk), vf(*blk),
                vb(NC, 2, 4, tq, cw), vf(2, 4, tq, f), vb(2, 4, tq, f), vb(*blk), vb(*blk),
                vf(1, d), vf(1, d), vf(1, d), vf(3, 1, d),
                dma(()), dma((2,)), dma(()), dma(()), dma((NC,)), dma(()), dma(()), dma(()), dma((NC,)), dma((NC,)),
                dma(()), dma(()), dma((NC,)), dma((NC,)),
            ]
            + [dma((NC,))] * 18
            + [dma(())] * 2
            + [dma((NC,))] * 7
            + [dma((4,)), dma(()), dma(()), dma((2,)), dma((4,)), dma((4,))],
            compiler_params=pltpu.CompilerParams(collective_id=0, has_side_effects=True, vmem_limit_bytes=LIMIT),
            name="main",
        )(ids, emb, du, w, g, dres)

        zr = 128
        rows = vl // zr * 11 // 16 * zr
        near = [send(dxo, b) for b in (2, 4, 6)]
        row, cnt, sel, dw, de, u, x, dg = pl.pallas_call(
            functools.partial(fill_kernel, rows=rows),
            out_shape=(
                sds((nt + 8,), jnp.int32), sds((1,), jnp.int32), sds((nt, nt), BF16),
                sds((d, f), F32), sds((vl, d), F32), sds((nt, f), BF16), sds(x.shape, BF16), sds((1, d), F32),
            ),
            in_specs=[SM, VM] + [ANY] * 5,
            out_specs=(SM, SM, VM) + (ANY,) * 5,
            scratch_shapes=[
                vb(NC, nt, cw), vb(nt, f), vf(2, cw, f), vf(zr, d), vb(nt, f), vb(*x.shape), vf(1, d),
                vf(nt, nt), pltpu.VMEM((1, nt), jnp.int32), pltpu.SMEM((1, nt), jnp.int32),
                dma((NC,)), dma(()), dma((2,)), dma(()), dma((3,)), dma(()),
            ],
            compiler_params=local_only,
            cost_estimate=pl.CostEstimate(flops=18_000_000_000, bytes_accessed=vl * d * 4, transcendentals=0),
            name="fill",
        )(ids, ids, n.reshape(NC, nt, cw), du.reshape(nt, f), u.reshape(nt, f), x, dg)
        far = [send(a, 1) for a in near]

        de = pl.pallas_call(
            functools.partial(rest_kernel, rows=rows),
            out_shape=sds((vl, d), F32),
            in_specs=[ANY],
            out_specs=ANY,
            input_output_aliases={0: 0},
            scratch_shapes=[vf(zr, d), dma(())],
            compiler_params=pltpu.CompilerParams(vmem_limit_bytes=16 * 1024 * 1024),
            cost_estimate=pl.CostEstimate(flops=8_000_000_000, bytes_accessed=(vl - rows) * d * 4, transcendentals=0),
            name="rest",
        )(de)
        de = pl.pallas_call(
            rows_kernel,
            out_shape=sds((vl, d), F32),
            in_specs=[SM, SM, VM] + [VM] * 8 + [ANY],
            out_specs=ANY,
            input_output_aliases={11: 0},
            scratch_shapes=[vb(NC, 2, 4, tq, cw), vf(nt, d), dma(())],
            compiler_params=pltpu.CompilerParams(vmem_limit_bytes=24 * 1024 * 1024),
            name="rows",
        )(row, cnt, sel, dxo, *near, dxp, *far, de)
        return u.reshape(mb, t, f), x, de, dw, dg.reshape(d)

    return jax.shard_map(
        local,
        mesh=mesh,
        in_specs=(P("dp", None), P("tp", None), P(None), P(None, "tp"), P("dp", None, "tp"), P("dp", "tp", None)),
        out_specs=(P("dp", None, "tp"), P("dp", "tp", None), P(("dp", "tp"), None), P(None, ("dp", "tp")), P("dp")),
        check_vma=False,
    )
```

```python
import functools

import jax
import jax.numpy as jnp
from jax import lax
from jax.experimental import pallas as pl
from jax.experimental.pallas import tpu as pltpu
from jax.sharding import PartitionSpec as P

EPS = 1e-6
MESH = pl.DeviceIdType.MESH
F32 = jnp.float32
BF16 = jnp.bfloat16
ANY = pl.BlockSpec(memory_space=pl.ANY)
VM = pl.BlockSpec(memory_space=pltpu.VMEM)
SM = pl.BlockSpec(memory_space=pltpu.SMEM)
LIMIT = 60 * 1024 * 1024
NC = 6
HC = NC // 2
LATE = 2
FIRST = 4


def main_kernel(
    ids_ref, emb_ref, du_ref, w_ref, g_ref, dres_ref,
    xo_ref, n_ref, u_ref, dxo_ref, dxp_ref, dg_ref,
    idv, ev, oh, xp, xr, xfw, x1, x2, xh, xpr, drw, gv, wv, duv, pb, pr, sf, rf, r1, r2, nall, acc, ub, dxs, dxr,
    dgm, dgr, dgc, dgn,
    id_s, e_s, du_s, g_s, w_s, dl_s, dr_s, dr_r, xd_s, xd_r, xo_s, xo_r, pd_s, pd_r,
    xa_s, xb_s, xc_s, xa_r, xb_r, xc_r, da_s, db_s, dc_s, da_r, db_r, dc_r,
    ga_s, gb_s, gc_s, ga_r, gb_r, gc_r, h0_s, h0_r, h1_s, h2_s, h3_s, h1_r, h2_r, h3_r,
    no_s, uo_s, dx_s, dx_r, ox_s, dg_s, dg_r,
):
    me = lax.axis_index("tp")
    c = me % 2
    q = me // 2
    xq = q % 2
    yq = q // 2
    qx = q + 1 - 2 * xq
    qy = q + 2 - 4 * yq
    qd = 3 - q
    part = me + 1 - 2 * c
    dx_ = me + 2 - 4 * xq
    dy_ = me + 4 - 8 * yq
    dd_ = 2 * qd + c
    oc = 1 - c
    d, f = w_ref.shape
    cw = d // NC
    vl = emb_ref.shape[0]
    tq = xr.shape[2]
    nt = 8 * tq
    th = tq // 2

    def w_copy(k):
        rows = pl.ds(pl.multiple_of(k * cw, cw), cw)
        return pltpu.make_async_copy(w_ref.at[rows], wv.at[k], w_s.at[k])

    def chunk(i):
        return i % 2 * HC + i // 2

    barrier = pltpu.get_barrier_semaphore()
    for dev in (part, dx_, dy_, dd_):
        pl.semaphore_signal(barrier, inc=1, device_id={"tp": dev}, device_id_type=MESH)

    id_copy = pltpu.make_async_copy(ids_ref, idv, id_s)
    du_copy = pltpu.make_async_copy(du_ref, duv, du_s)
    g_copy = pltpu.make_async_copy(g_ref, gv, g_s)
    dl_copy = pltpu.make_async_copy(dres_ref.at[c], drw.at[c], dl_s)
    def e_copy(i):
        cols = pl.ds(pl.multiple_of(chunk(i) * cw, cw), cw)
        return pltpu.make_async_copy(emb_ref.at[:, cols], ev.at[i % 2], e_s.at[i % 2])

    du_copy.start()

    @pl.loop(0, NC)
    def _(i):
        w_copy(chunk(i)).start()

    id_copy.start()
    g_copy.start()
    dl_copy.start()
    e_copy(0).start()
    e_copy(1).start()
    pl.semaphore_wait(barrier, 4)

    def remote(src, dst, ss, rs, dev):
        return pltpu.make_async_remote_copy(
            src_ref=src, dst_ref=dst, send_sem=ss, recv_sem=rs, device_id={"tp": dev}, device_id_type=MESH
        )

    def xd(k):
        return remote(xp.at[k, oc], xr.at[k], xd_s.at[k], xd_r.at[k], part)

    dr = remote(dres_ref.at[oc], drw.at[c], dr_s, dr_r, part)

    def first(k):
        b = k // HC
        return qx + (qy - qx) * b, dx_ + (dy_ - dx_) * b

    def second(k):
        b = k // HC
        return qy + (qx - qy) * b, dy_ + (dx_ - dy_) * b

    def xa(k):
        return remote(xp.at[k, c, qd], xfw.at[k], xa_s.at[k], xa_r.at[k], first(k)[1])

    def xb(k):
        return remote(xp.at[k, c, first(k)[0]], x1.at[k], xb_s.at[k], xb_r.at[k], first(k)[1])

    def xc(k):
        return remote(xp.at[k, c, second(k)[0]], x2.at[k], xc_s.at[k], xc_r.at[k], second(k)[1])

    def da(k):
        return remote(sf.at[k, qd], rf.at[k], da_s.at[k], da_r.at[k], first(k)[1])

    def db(k):
        return remote(sf.at[k, first(k)[0]], r1.at[k], db_s.at[k], db_r.at[k], first(k)[1])

    def dc(k):
        return remote(sf.at[k, second(k)[0]], r2.at[k], dc_s.at[k], dc_r.at[k], second(k)[1])

    def pd(k):
        return remote(pb.at[k, oc], pr.at[k], pd_s.at[k], pd_r.at[k], part)

    def ga(k):
        return remote(nall.at[k, c, q], nall.at[k, c, q], ga_s.at[k], ga_r.at[k], first(k)[1])

    def gb(k):
        return remote(nall.at[k, c, q], nall.at[k, c, q], gb_s.at[k], gb_r.at[k], second(k)[1])

    def gc(k):
        s = first(k)[0]
        return remote(nall.at[k, c, s], nall.at[k, c, s], gc_s.at[k], gc_r.at[k], second(k)[1])

    def over(k, s, ss, rs):
        return remote(nall.at[k, c, s], nall.at[k, c, s], ss.at[k], rs.at[k], part)

    def h1(k):
        return over(k, first(k)[0], h1_s, h1_r)

    def h2(k):
        return over(k, second(k)[0], h2_s, h2_r)

    def h3(k):
        return over(k, qd, h3_s, h3_r)

    h0 = remote(nall.at[:, c, q], nall.at[:, c, q], h0_s, h0_r, part)

    du_copy.wait()

    def matmul(i):
        k = chunk(i)
        w_copy(k).wait()
        p = lax.dot_general(
            duv[...].reshape(nt, -1), wv[k], (((1,), (1,)), ((), ())), preferred_element_type=F32
        )
        pb[k] = p.astype(BF16).reshape(2, 4, tq, cw)
        pd(k).start()

    def combine(i):
        k = chunk(i)
        pd(k).wait_recv()
        for s in range(4):
            sf[k, s] = pb[k, c, s].astype(F32) + pr[k, s].astype(F32)
        da(k).start()

    matmul(0)

    @pl.loop(1, NC)
    def _(i):
        matmul(i)
        combine(i - 1)

    id_copy.wait()
    lo = me * vl
    for b in range(nt // 128):
        m, t0 = divmod(b * 128, 4 * tq)
        row = idv[m : m + 1, t0 : t0 + 128] - lo
        col = jnp.broadcast_to(row, (128, 128)).T

        @pl.loop(0, vl // 128, unroll=8)
        def _(j):
            lanes = lax.broadcasted_iota(jnp.int32, (128, 128), 1) + j * 128
            cols = pl.ds(pl.multiple_of(j * 128, 128), 128)
            oh[b * 128 : (b + 1) * 128, cols] = jnp.where(lanes == col, 1.0, 0.0).astype(BF16)

    combine(NC - 1)
    dr.start()

    def lookup(i):
        k = chunk(i)
        e_copy(i).wait()
        p = jnp.dot(oh[...], ev[i % 2], preferred_element_type=F32)
        xp[k] = p.astype(BF16).reshape(2, 4, tq, cw)
        xd(k).start()

        @pl.when(i + 2 < NC)
        def _():
            e_copy(i + 2).start()

    def pair(i):
        k = chunk(i)
        xd(k).wait_recv()
        xp[k, c] = xp[k, c] + xr[k]
        xa(k).start()
        xb(k).start()

    def forward(i):
        k = chunk(i)
        s = second(k)[0]
        da(k).wait_recv()
        sf[k, s] = sf[k, s] + rf[k]
        dc(k).start()

    db(chunk(0)).start()
    db(chunk(1)).start()
    lookup(0)

    @pl.loop(1, NC)
    def _(i):
        @pl.when(i + 1 < NC)
        def _():
            db(chunk(i + 1)).start()

        lookup(i)
        pair(i - 1)

    pair(NC - 1)

    @pl.loop(0, NC)
    def _(i):
        k = chunk(i)
        s = second(k)[0]
        xa(k).wait_recv()
        xp[k, c, s] = xp[k, c, s] + xfw[k]
        xc(k).start()

    acc[...] = jnp.zeros_like(acc)

    @pl.loop(0, NC)
    def _(i):
        xc(chunk(i)).wait_send()

    @pl.loop(0, FIRST)
    def _(i):
        forward(i)

    g_copy.wait()
    sq = jnp.zeros((tq, 1), F32)
    for k in range(NC):
        xb(k).wait_recv()
        xc(k).wait_recv()
        xk = xp[k, c, q] + x1[k] + x2[k]
        xh[k] = xk
        xk = xk.astype(F32)
        sq = sq + jnp.sum(xk * xk, axis=-1, keepdims=True)
    xo = remote(xh.at[:, pl.ds(pl.multiple_of(oc * th, th), th), :], xpr, xo_s, xo_r, part)
    xo.start()
    rs = lax.rsqrt(sq * (1.0 / d) + EPS)
    for k in (0, 3, 1, 4, 2, 5):
        cols = slice(k * cw, (k + 1) * cw)
        nall[k, c, q] = ((xh[k].astype(F32) * rs) * gv[cols].astype(F32).reshape(1, cw)).astype(BF16)
        ga(k).start()
    h0.start()
    for k in range(NC):
        xo_ref[c, :, k * cw : (k + 1) * cw] = xh[k, pl.ds(pl.multiple_of(c * th, th), th), :]
    dl_copy.wait()
    dr.wait_recv()
    xo.wait_recv()
    for k in range(NC):
        xo_ref[oc, :, k * cw : (k + 1) * cw] = xpr[k]

    def piece(k, s):
        acc[:, s] += jnp.dot(nall[k, :, s].reshape(2 * tq, cw), wv[k], preferred_element_type=F32).reshape(2, tq, f)

    def u_out(j, s):
        ub[:, s] = acc[:, s].astype(BF16)
        return pltpu.make_async_copy(ub.at[:, s], u_ref.at[:, s], uo_s.at[j])

    h0.wait_recv()

    @pl.loop(0, NC)
    def _(k):
        piece(k, q)

    uo = [u_out(0, q)]
    uo[0].start()

    @pl.loop(0, NC)
    def _(i):
        ga(chunk(i)).wait_send()

    @pl.loop(FIRST, NC)
    def _(i):
        forward(i)

    @pl.loop(0, NC)
    def _(i):
        gb(chunk(i)).start()

    @pl.loop(0, NC)
    def _(i):
        k = chunk(i)
        ga(k).wait_recv()
        gc(k).start()
        h1(k).start()

    @pl.loop(0, NC)
    def _(i):
        k = chunk(i)
        h1(k).wait_recv()
        piece(k, first(k)[0])

    m = jnp.zeros((tq, 1), F32)
    for k in (0, 3, 1, 4, 2, 5):
        cols = slice(k * cw, (k + 1) * cw)
        db(k).wait_recv()
        dc(k).wait_recv()
        dn = sf[k, q] + r1[k] + r2[k]
        r1[k] = dn
        nh = xh[k].astype(F32) * rs
        dnh = dn * nh
        dgm[:, cols] = jnp.sum(dnh, axis=0, keepdims=True)
        m = m + jnp.sum(dnh * gv[cols].astype(F32).reshape(1, cw), axis=-1, keepdims=True)
    dg0 = remote(dgm, dgr, dg_s.at[0], dg_r.at[0], part)
    dg0.start()
    m = m * (1.0 / d)
    for k in range(NC):
        cols = slice(k * cw, (k + 1) * cw)
        nh = xh[k].astype(F32) * rs
        dxn = rs * (gv[cols].astype(F32).reshape(1, cw) * r1[k] - nh * m)
        dxs[k] = (drw[:, :, cols].reshape(tq, cw).astype(F32) + dxn).astype(BF16)
    dxc = remote(dxs, dxr, dx_s, dx_r, part)
    dxc.start()
    ox = pltpu.make_async_copy(dxs, dxo_ref, ox_s.at[0])
    ox.start()
    dg0.wait_recv()
    dgc[...] = dgm[...] + dgr[...]
    dgs = [remote(dgc, dgn.at[j], dg_s.at[1 + j], dg_r.at[1 + j], dev) for j, dev in enumerate((dx_, dy_, dd_))]
    for cp in dgs:
        cp.start()

    dxc.wait_recv()
    oy = pltpu.make_async_copy(dxr, dxp_ref, ox_s.at[1])
    oy.start()

    def n_out(k):
        return pltpu.make_async_copy(nall.at[k], n_ref.at[k], no_s.at[k])

    def second_in(i):
        k = chunk(i)
        gb(k).wait_recv()
        h2(k).start()

    def second_use(i):
        k = chunk(i)
        h2(k).wait_recv()
        piece(k, second(k)[0])

    def last_in(i):
        k = chunk(i)
        gc(k).wait_recv()
        h3(k).start()

    def last_use(i):
        k = chunk(i)
        h3(k).wait_recv()
        n_out(k).start()
        piece(k, qd)

    second_in(0)

    @pl.loop(1, NC)
    def _(i):
        second_in(i)
        second_use(i - 1)

    last_in(0)
    second_use(NC - 1)
    for j, s in enumerate((qx, qy)):
        uo.append(u_out(1 + j, s))
        uo[-1].start()

    @pl.loop(1, NC)
    def _(i):
        last_in(i)
        last_use(i - 1)

    last_use(NC - 1)
    uo.append(u_out(3, qd))
    uo[-1].start()
    for cp in dgs:
        cp.wait_recv()
    dg_ref[...] = (dgc[...] + dgn[0]) + (dgn[1] + dgn[2])
    for cp in uo:
        cp.wait()

    ox.wait()
    oy.wait()
    dr.wait_send()
    xo.wait_send()
    h0.wait_send()
    dg0.wait_send()
    dxc.wait_send()
    for cp in dgs:
        cp.wait_send()

    @pl.loop(0, NC)
    def _(k):
        n_out(k).wait()
        for cp in (xd, pd, xa, xb, da, db, dc, gb, gc, h1, h2, h3):
            cp(k).wait_send()


def fill_kernel(
    ids_ref, idv_ref, n_ref, du_ref, u_ref, x_ref, dg_ref,
    row_ref, cnt_ref, sel_ref, dw_ref, de_ref, uo_ref, xo_ref, dgo_ref,
    nv, duv, st, z, uv, xv, gv, sel, fv, fs, n_s, du_s, o_s, z_s, p_s, f_s, *, rows,
):
    cw = nv.shape[2]
    zr = z.shape[0]
    mb, tm = idv_ref.shape
    nt = mb * tm
    vl = de_ref.shape[0]
    lo = lax.axis_index("tp") * vl
    du_copy = pltpu.make_async_copy(du_ref, duv, du_s)
    du_copy.start()

    def n_copy(k):
        return pltpu.make_async_copy(n_ref.at[k], nv.at[k], n_s.at[k])

    def out(k):
        r = pl.ds(pl.multiple_of(k * cw, cw), cw)
        return pltpu.make_async_copy(st.at[k % 2], dw_ref.at[r], o_s.at[k % 2])

    def put(i):
        return pltpu.make_async_copy(z, de_ref.at[pl.ds(pl.multiple_of(i * zr, zr), zr)], z_s)

    for k in range(NC):
        n_copy(k).start()
    small = ((u_ref, uv, uo_ref), (x_ref, xv, xo_ref), (dg_ref, gv, dgo_ref))
    ins = [pltpu.make_async_copy(a, v, p_s.at[j]) for j, (a, v, _) in enumerate(small)]
    outs = [pltpu.make_async_copy(v, o, p_s.at[j]) for j, (_, v, o) in enumerate(small)]
    for cp in ins:
        cp.start()
    z[...] = jnp.zeros_like(z)
    early = rows // zr - NC * LATE

    @pl.loop(0, early)
    def _(i):
        put(i).start()

    for m in range(mb):
        row = idv_ref[m : m + 1, :] - lo
        later = jnp.zeros((1, tm), jnp.int32)
        for b in range(nt // 128):
            m0, t0 = divmod(b * 128, tm)
            col = jnp.broadcast_to(idv_ref[m0 : m0 + 1, t0 : t0 + 128] - lo, (128, 128)).T
            col = jnp.concatenate([col] * (tm // 128), axis=1)
            pos = lax.broadcasted_iota(jnp.int32, (128, tm), 0) + b * 128
            mine = lax.broadcasted_iota(jnp.int32, (128, tm), 1) + m * tm
            hit = jnp.where((col == row) & (pos < mine), 1, 0)
            later = jnp.maximum(later, jnp.max(hit, axis=0, keepdims=True))
        fv[:, m * tm : (m + 1) * tm] = jnp.where((row >= 0) & (row < vl), 1 - later, 0)
    cp = pltpu.make_async_copy(fv, fs, f_s)
    cp.start()
    sel[...] = jnp.zeros_like(sel)
    cp.wait()

    def scan(t, n):
        row_ref[n] = ids_ref[t // tm, t % tm] - lo
        return n + fs[0, t]

    cnt = lax.fori_loop(0, nt, scan, jnp.int32(0), unroll=8)
    cnt_ref[0] = cnt

    @pl.loop(0, cnt)
    def _(j):
        v = row_ref[j] + lo
        for m in range(mb):
            sel[pl.ds(j, 1), m * tm : (m + 1) * tm] = jnp.where(idv_ref[m : m + 1, :] == v, 1.0, 0.0)

    sel_ref[...] = sel[...].astype(BF16)
    for cp, co in zip(ins, outs):
        cp.wait()
        co.start()
    du_copy.wait()

    @pl.loop(0, NC)
    def _(k):
        n_copy(k).wait()
        for j in range(LATE):
            put(early + k * LATE + j).start()

        @pl.when(k >= 2)
        def _():
            out(k - 2).wait()

        st[k % 2] = lax.dot_general(nv[k], duv[...], (((0,), (0,)), ((), ())), preferred_element_type=F32)
        out(k).start()

    for co in outs:
        co.wait()
    out(NC - 2).wait()
    out(NC - 1).wait()

    @pl.loop(0, rows // zr)
    def _(i):
        put(i).wait()


def rest_kernel(_, de_ref, z, z_s, *, rows):
    zr = z.shape[0]
    left = (de_ref.shape[0] - rows) // zr

    def put(i):
        return pltpu.make_async_copy(z, de_ref.at[pl.ds(pl.multiple_of(rows + i * zr, zr), zr)], z_s)

    z[...] = jnp.zeros_like(z)

    @pl.loop(0, left)
    def _(i):
        put(i).start()

    @pl.loop(0, left)
    def _(i):
        put(i).wait()


def rows_kernel(*refs):
    row_ref, cnt_ref, sel_ref = refs[:3]
    dx_refs = refs[3:11]
    _, de_ref, dxv, dxs, o_s = refs[11:]
    nt = sel_ref.shape[0]
    cw = dxv.shape[-1]
    rb = 128
    me = lax.axis_index("tp")
    c = me % 2
    q = me // 2
    qx = q + 1 - 2 * (q % 2)
    qy = q + 2 - 4 * (q // 2)
    where = [(b, s) for b in (c, 1 - c) for s in (q, qx, qy, 3 - q)]
    for r, (b, s) in zip(dx_refs, where):
        dxv[:, b, s] = r[...]
    cnt = cnt_ref[0]

    def put(j):
        return pltpu.make_async_copy(dxs.at[pl.ds(j, 1)], de_ref.at[pl.ds(row_ref[j], 1)], o_s)

    @pl.loop(0, (cnt + rb - 1) // rb)
    def _(b):
        r = pl.ds(pl.multiple_of(b * rb, rb), rb)
        for k in range(NC):
            dxs[r, k * cw : (k + 1) * cw] = jnp.dot(
                sel_ref[r, :], dxv[k].reshape(nt, cw), preferred_element_type=F32
            )

        @pl.loop(b * rb, jnp.minimum(b * rb + rb, cnt))
        def _(j):
            put(j).start()

    @pl.loop(0, cnt)
    def _(j):
        put(j).wait()


def solution(mesh):
    groups = mesh.shape["tp"]

    def shift(bit):
        return [(r, r ^ bit) for r in range(groups)]

    def send(a, bit):
        return lax.ppermute(a, "tp", shift(bit))

    def local(ids, emb, g, w, du, dres):
        mb, t = ids.shape
        vl, d = emb.shape
        f = w.shape[1]
        nt = mb * t
        cw = d // NC
        tq = t // 4
        dma = pltpu.SemaphoreType.DMA
        sds = jax.ShapeDtypeStruct
        vb = lambda *s: pltpu.VMEM(s, BF16)
        vf = lambda *s: pltpu.VMEM(s, F32)
        local_only = pltpu.CompilerParams(vmem_limit_bytes=LIMIT)

        blk = (NC, tq, cw)
        x, n, u, dxo, dxp, dg = pl.pallas_call(
            main_kernel,
            out_shape=(
                sds((2, tq // 2, d), BF16),
                sds((NC, 2, 4, tq, cw), BF16),
                sds((2, 4, tq, f), BF16),
                sds(blk, BF16),
                sds(blk, BF16),
                sds((1, d), F32),
            ),
            in_specs=[ANY] * 6,
            out_specs=(VM, ANY, ANY, ANY, ANY, VM),
            scratch_shapes=[
                pltpu.VMEM((mb, t), jnp.int32), vb(2, vl, cw), vb(nt, vl),
                vb(NC, 2, 4, tq, cw), vb(NC, 4, tq, cw), vb(*blk), vb(*blk), vb(*blk),
                vb(*blk), vb(NC, tq // 2, cw), vb(2, tq // 2, d), vb(d),
                vb(NC, cw, f), vb(2, t, f),
                vb(NC, 2, 4, tq, cw), vb(NC, 4, tq, cw),
                vf(NC, 4, tq, cw), vf(*blk), vf(*blk), vf(*blk),
                vb(NC, 2, 4, tq, cw), vf(2, 4, tq, f), vb(2, 4, tq, f), vb(*blk), vb(*blk),
                vf(1, d), vf(1, d), vf(1, d), vf(3, 1, d),
                dma(()), dma((2,)), dma(()), dma(()), dma((NC,)), dma(()), dma(()), dma(()), dma((NC,)), dma((NC,)),
                dma(()), dma(()), dma((NC,)), dma((NC,)),
            ]
            + [dma((NC,))] * 18
            + [dma(())] * 2
            + [dma((NC,))] * 7
            + [dma((4,)), dma(()), dma(()), dma((2,)), dma((4,)), dma((4,))],
            compiler_params=pltpu.CompilerParams(collective_id=0, has_side_effects=True, vmem_limit_bytes=LIMIT),
            name="main",
        )(ids, emb, du, w, g, dres)

        zr = 128
        rows = vl // zr * 11 // 16 * zr
        near = [send(dxo, b) for b in (2, 4, 6)]
        row, cnt, sel, dw, de, u, x, dg = pl.pallas_call(
            functools.partial(fill_kernel, rows=rows),
            out_shape=(
                sds((nt + 8,), jnp.int32), sds((1,), jnp.int32), sds((nt, nt), BF16),
                sds((d, f), F32), sds((vl, d), F32), sds((nt, f), BF16), sds(x.shape, BF16), sds((1, d), F32),
            ),
            in_specs=[SM, VM] + [ANY] * 5,
            out_specs=(SM, SM, VM) + (ANY,) * 5,
            scratch_shapes=[
                vb(NC, nt, cw), vb(nt, f), vf(2, cw, f), vf(zr, d), vb(nt, f), vb(*x.shape), vf(1, d),
                vf(nt, nt), pltpu.VMEM((1, nt), jnp.int32), pltpu.SMEM((1, nt), jnp.int32),
                dma((NC,)), dma(()), dma((2,)), dma(()), dma((3,)), dma(()),
            ],
            compiler_params=local_only,
            cost_estimate=pl.CostEstimate(flops=18_000_000_000, bytes_accessed=vl * d * 4, transcendentals=0),
            name="fill",
        )(ids, ids, n.reshape(NC, nt, cw), du.reshape(nt, f), u.reshape(nt, f), x, dg)
        far = [send(a, 1) for a in near]

        de = pl.pallas_call(
            functools.partial(rest_kernel, rows=rows),
            out_shape=sds((vl, d), F32),
            in_specs=[ANY],
            out_specs=ANY,
            input_output_aliases={0: 0},
            scratch_shapes=[vf(zr, d), dma(())],
            compiler_params=pltpu.CompilerParams(vmem_limit_bytes=16 * 1024 * 1024),
            cost_estimate=pl.CostEstimate(flops=8_000_000_000, bytes_accessed=(vl - rows) * d * 4, transcendentals=0),
            name="rest",
        )(de)
        de = pl.pallas_call(
            rows_kernel,
            out_shape=sds((vl, d), F32),
            in_specs=[SM, SM, VM] + [VM] * 8 + [ANY],
            out_specs=ANY,
            input_output_aliases={11: 0},
            scratch_shapes=[vb(NC, 2, 4, tq, cw), vf(nt, d), dma(())],
            compiler_params=pltpu.CompilerParams(vmem_limit_bytes=24 * 1024 * 1024),
            name="rows",
        )(row, cnt, sel, dxo, *near, dxp, *far, de)
        return u.reshape(mb, t, f), x, de, dw, dg.reshape(d)

    return jax.shard_map(
        local,
        mesh=mesh,
        in_specs=(P("dp", None), P("tp", None), P(None), P(None, "tp"), P("dp", None, "tp"), P("dp", "tp", None)),
        out_specs=(P("dp", None, "tp"), P("dp", "tp", None), P(("dp", "tp"), None), P(None, ("dp", "tp")), P("dp")),
        check_vma=False,
    )
```

```python
import functools

import jax
import jax.numpy as jnp
from jax import lax
from jax.experimental import pallas as pl
from jax.experimental.pallas import tpu as pltpu
from jax.sharding import PartitionSpec as P

EPS = 1e-6
MESH = pl.DeviceIdType.MESH
F32 = jnp.float32
BF16 = jnp.bfloat16
ANY = pl.BlockSpec(memory_space=pl.ANY)
VM = pl.BlockSpec(memory_space=pltpu.VMEM)
SM = pl.BlockSpec(memory_space=pltpu.SMEM)
LIMIT = 60 * 1024 * 1024
NC = 6
HC = NC // 2
LATE = 1
FIRST = 4


def main_kernel(
    ids_ref, emb_ref, du_ref, w_ref, g_ref, dres_ref,
    xo_ref, n_ref, u_ref, dxo_ref, dxp_ref, dg_ref,
    idv, ev, oh, xp, xr, xfw, x1, x2, xh, xpr, drw, gv, wv, duv, pb, pr, sf, rf, r1, r2, nall, acc, ub, dxs, dxr,
    dgm, dgr, dgc, dgn,
    id_s, e_s, du_s, g_s, w_s, dl_s, dr_s, dr_r, xd_s, xd_r, xo_s, xo_r, pd_s, pd_r,
    xa_s, xb_s, xc_s, xa_r, xb_r, xc_r, da_s, db_s, dc_s, da_r, db_r, dc_r,
    ga_s, gb_s, gc_s, ga_r, gb_r, gc_r, h0_s, h0_r, h1_s, h2_s, h3_s, h1_r, h2_r, h3_r,
    no_s, uo_s, dx_s, dx_r, ox_s, dg_s, dg_r,
):
    me = lax.axis_index("tp")
    c = me % 2
    q = me // 2
    xq = q % 2
    yq = q // 2
    qx = q + 1 - 2 * xq
    qy = q + 2 - 4 * yq
    qd = 3 - q
    part = me + 1 - 2 * c
    dx_ = me + 2 - 4 * xq
    dy_ = me + 4 - 8 * yq
    dd_ = 2 * qd + c
    oc = 1 - c
    d, f = w_ref.shape
    cw = d // NC
    vl = emb_ref.shape[0]
    tq = xr.shape[2]
    nt = 8 * tq
    th = tq // 2

    def w_copy(k):
        rows = pl.ds(pl.multiple_of(k * cw, cw), cw)
        return pltpu.make_async_copy(w_ref.at[rows], wv.at[k], w_s.at[k])

    def chunk(i):
        return i % 2 * HC + i // 2

    barrier = pltpu.get_barrier_semaphore()
    for dev in (part, dx_, dy_, dd_):
        pl.semaphore_signal(barrier, inc=1, device_id={"tp": dev}, device_id_type=MESH)

    id_copy = pltpu.make_async_copy(ids_ref, idv, id_s)
    du_copy = pltpu.make_async_copy(du_ref, duv, du_s)
    g_copy = pltpu.make_async_copy(g_ref, gv, g_s)
    dl_copy = pltpu.make_async_copy(dres_ref.at[c], drw.at[c], dl_s)
    def e_copy(i):
        cols = pl.ds(pl.multiple_of(chunk(i) * cw, cw), cw)
        return pltpu.make_async_copy(emb_ref.at[:, cols], ev.at[i % 2], e_s.at[i % 2])

    du_copy.start()

    @pl.loop(0, NC)
    def _(i):
        w_copy(chunk(i)).start()

    id_copy.start()
    g_copy.start()
    dl_copy.start()
    e_copy(0).start()
    e_copy(1).start()
    pl.semaphore_wait(barrier, 4)

    def remote(src, dst, ss, rs, dev):
        return pltpu.make_async_remote_copy(
            src_ref=src, dst_ref=dst, send_sem=ss, recv_sem=rs, device_id={"tp": dev}, device_id_type=MESH
        )

    def xd(k):
        return remote(xp.at[k, oc], xr.at[k], xd_s.at[k], xd_r.at[k], part)

    dr = remote(dres_ref.at[oc], drw.at[c], dr_s, dr_r, part)

    def first(k):
        b = k // HC
        return qx + (qy - qx) * b, dx_ + (dy_ - dx_) * b

    def second(k):
        b = k // HC
        return qy + (qx - qy) * b, dy_ + (dx_ - dy_) * b

    def xa(k):
        return remote(xp.at[k, c, qd], xfw.at[k], xa_s.at[k], xa_r.at[k], first(k)[1])

    def xb(k):
        return remote(xp.at[k, c, first(k)[0]], x1.at[k], xb_s.at[k], xb_r.at[k], first(k)[1])

    def xc(k):
        return remote(xp.at[k, c, second(k)[0]], x2.at[k], xc_s.at[k], xc_r.at[k], second(k)[1])

    def da(k):
        return remote(sf.at[k, qd], rf.at[k], da_s.at[k], da_r.at[k], first(k)[1])

    def db(k):
        return remote(sf.at[k, first(k)[0]], r1.at[k], db_s.at[k], db_r.at[k], first(k)[1])

    def dc(k):
        return remote(sf.at[k, second(k)[0]], r2.at[k], dc_s.at[k], dc_r.at[k], second(k)[1])

    def pd(k):
        return remote(pb.at[k, oc], pr.at[k], pd_s.at[k], pd_r.at[k], part)

    def ga(k):
        return remote(nall.at[k, c, q], nall.at[k, c, q], ga_s.at[k], ga_r.at[k], first(k)[1])

    def gb(k):
        return remote(nall.at[k, c, q], nall.at[k, c, q], gb_s.at[k], gb_r.at[k], second(k)[1])

    def gc(k):
        s = first(k)[0]
        return remote(nall.at[k, c, s], nall.at[k, c, s], gc_s.at[k], gc_r.at[k], second(k)[1])

    def over(k, s, ss, rs):
        return remote(nall.at[k, c, s], nall.at[k, c, s], ss.at[k], rs.at[k], part)

    def h1(k):
        return over(k, first(k)[0], h1_s, h1_r)

    def h2(k):
        return over(k, second(k)[0], h2_s, h2_r)

    def h3(k):
        return over(k, qd, h3_s, h3_r)

    h0 = remote(nall.at[:, c, q], nall.at[:, c, q], h0_s, h0_r, part)

    du_copy.wait()

    def matmul(i):
        k = chunk(i)
        w_copy(k).wait()
        p = lax.dot_general(
            duv[...].reshape(nt, -1), wv[k], (((1,), (1,)), ((), ())), preferred_element_type=F32
        )
        pb[k] = p.astype(BF16).reshape(2, 4, tq, cw)
        pd(k).start()

    def combine(i):
        k = chunk(i)
        pd(k).wait_recv()
        for s in range(4):
            sf[k, s] = pb[k, c, s].astype(F32) + pr[k, s].astype(F32)
        da(k).start()

    matmul(0)

    @pl.loop(1, NC)
    def _(i):
        matmul(i)
        combine(i - 1)

    id_copy.wait()
    lo = me * vl
    for b in range(nt // 128):
        m, t0 = divmod(b * 128, 4 * tq)
        row = idv[m : m + 1, t0 : t0 + 128] - lo
        col = jnp.broadcast_to(row, (128, 128)).T

        @pl.loop(0, vl // 128, unroll=8)
        def _(j):
            lanes = lax.broadcasted_iota(jnp.int32, (128, 128), 1) + j * 128
            cols = pl.ds(pl.multiple_of(j * 128, 128), 128)
            oh[b * 128 : (b + 1) * 128, cols] = jnp.where(lanes == col, 1.0, 0.0).astype(BF16)

    combine(NC - 1)
    dr.start()

    def lookup(i):
        k = chunk(i)
        e_copy(i).wait()
        p = jnp.dot(oh[...], ev[i % 2], preferred_element_type=F32)
        xp[k] = p.astype(BF16).reshape(2, 4, tq, cw)
        xd(k).start()

        @pl.when(i + 2 < NC)
        def _():
            e_copy(i + 2).start()

    def pair(i):
        k = chunk(i)
        xd(k).wait_recv()
        xp[k, c] = xp[k, c] + xr[k]
        xa(k).start()
        xb(k).start()

    def forward(i):
        k = chunk(i)
        s = second(k)[0]
        da(k).wait_recv()
        sf[k, s] = sf[k, s] + rf[k]
        dc(k).start()

    db(chunk(0)).start()
    db(chunk(1)).start()
    lookup(0)

    @pl.loop(1, NC)
    def _(i):
        @pl.when(i + 1 < NC)
        def _():
            db(chunk(i + 1)).start()

        lookup(i)
        pair(i - 1)

    pair(NC - 1)

    @pl.loop(0, NC)
    def _(i):
        k = chunk(i)
        s = second(k)[0]
        xa(k).wait_recv()
        xp[k, c, s] = xp[k, c, s] + xfw[k]
        xc(k).start()

    acc[...] = jnp.zeros_like(acc)

    @pl.loop(0, NC)
    def _(i):
        xc(chunk(i)).wait_send()

    @pl.loop(0, FIRST)
    def _(i):
        forward(i)

    g_copy.wait()
    sq = jnp.zeros((tq, 1), F32)
    for k in range(NC):
        xb(k).wait_recv()
        xc(k).wait_recv()
        xk = xp[k, c, q] + x1[k] + x2[k]
        xh[k] = xk
        xk = xk.astype(F32)
        sq = sq + jnp.sum(xk * xk, axis=-1, keepdims=True)
    xo = remote(xh.at[:, pl.ds(pl.multiple_of(oc * th, th), th), :], xpr, xo_s, xo_r, part)
    xo.start()
    rs = lax.rsqrt(sq * (1.0 / d) + EPS)
    for k in (0, 3, 1, 4, 2, 5):
        cols = slice(k * cw, (k + 1) * cw)
        nall[k, c, q] = ((xh[k].astype(F32) * rs) * gv[cols].astype(F32).reshape(1, cw)).astype(BF16)
        ga(k).start()
    h0.start()
    for k in range(NC):
        xo_ref[c, :, k * cw : (k + 1) * cw] = xh[k, pl.ds(pl.multiple_of(c * th, th), th), :]
    dl_copy.wait()
    dr.wait_recv()
    xo.wait_recv()
    for k in range(NC):
        xo_ref[oc, :, k * cw : (k + 1) * cw] = xpr[k]

    def piece(k, s):
        acc[:, s] += jnp.dot(nall[k, :, s].reshape(2 * tq, cw), wv[k], preferred_element_type=F32).reshape(2, tq, f)

    def u_out(j, s):
        ub[:, s] = acc[:, s].astype(BF16)
        return pltpu.make_async_copy(ub.at[:, s], u_ref.at[:, s], uo_s.at[j])

    h0.wait_recv()

    @pl.loop(0, NC)
    def _(k):
        piece(k, q)

    uo = [u_out(0, q)]
    uo[0].start()

    @pl.loop(0, NC)
    def _(i):
        ga(chunk(i)).wait_send()

    @pl.loop(FIRST, NC)
    def _(i):
        forward(i)

    @pl.loop(0, NC)
    def _(i):
        gb(chunk(i)).start()

    @pl.loop(0, NC)
    def _(i):
        k = chunk(i)
        ga(k).wait_recv()
        gc(k).start()
        h1(k).start()

    @pl.loop(0, NC)
    def _(i):
        k = chunk(i)
        h1(k).wait_recv()
        piece(k, first(k)[0])

    m = jnp.zeros((tq, 1), F32)
    for k in (0, 3, 1, 4, 2, 5):
        cols = slice(k * cw, (k + 1) * cw)
        db(k).wait_recv()
        dc(k).wait_recv()
        dn = sf[k, q] + r1[k] + r2[k]
        r1[k] = dn
        nh = xh[k].astype(F32) * rs
        dnh = dn * nh
        dgm[:, cols] = jnp.sum(dnh, axis=0, keepdims=True)
        m = m + jnp.sum(dnh * gv[cols].astype(F32).reshape(1, cw), axis=-1, keepdims=True)
    dg0 = remote(dgm, dgr, dg_s.at[0], dg_r.at[0], part)
    dg0.start()
    m = m * (1.0 / d)
    for k in range(NC):
        cols = slice(k * cw, (k + 1) * cw)
        nh = xh[k].astype(F32) * rs
        dxn = rs * (gv[cols].astype(F32).reshape(1, cw) * r1[k] - nh * m)
        dxs[k] = (drw[:, :, cols].reshape(tq, cw).astype(F32) + dxn).astype(BF16)
    dxc = remote(dxs, dxr, dx_s, dx_r, part)
    dxc.start()
    ox = pltpu.make_async_copy(dxs, dxo_ref, ox_s.at[0])
    ox.start()
    def n_out(k):
        return pltpu.make_async_copy(nall.at[k], n_ref.at[k], no_s.at[k])

    @pl.loop(0, NC)
    def _(i):
        k = chunk(i)
        gb(k).wait_recv()
        h2(k).start()

    dg0.wait_recv()
    dgc[...] = dgm[...] + dgr[...]
    dgs = [remote(dgc, dgn.at[j], dg_s.at[1 + j], dg_r.at[1 + j], dev) for j, dev in enumerate((dx_, dy_, dd_))]
    for cp in dgs:
        cp.start()
    dxc.wait_recv()
    oy = pltpu.make_async_copy(dxr, dxp_ref, ox_s.at[1])
    oy.start()

    def last_in(i):
        k = chunk(i)
        gc(k).wait_recv()
        h3(k).start()

    def last_use(i):
        k = chunk(i)
        s = second(k)[0]
        h2(k).wait_recv()
        h3(k).wait_recv()
        n_out(k).start()
        rows = jnp.concatenate([nall[k, :, s].reshape(2 * tq, cw), nall[k, :, qd].reshape(2 * tq, cw)])
        p = jnp.dot(rows, wv[k], preferred_element_type=F32).reshape(2, 2, tq, f)
        acc[:, s] += p[0]
        acc[:, qd] += p[1]

    last_in(0)

    @pl.loop(1, NC)
    def _(i):
        last_in(i)
        last_use(i - 1)

    last_use(NC - 1)
    for j, s in enumerate((qx, qy)):
        uo.append(u_out(1 + j, s))
        uo[-1].start()
    uo.append(u_out(3, qd))
    uo[-1].start()
    for cp in dgs:
        cp.wait_recv()
    dg_ref[...] = (dgc[...] + dgn[0]) + (dgn[1] + dgn[2])
    for cp in uo:
        cp.wait()

    ox.wait()
    oy.wait()
    dr.wait_send()
    xo.wait_send()
    h0.wait_send()
    dg0.wait_send()
    dxc.wait_send()
    for cp in dgs:
        cp.wait_send()

    @pl.loop(0, NC)
    def _(k):
        n_out(k).wait()
        for cp in (xd, pd, xa, xb, da, db, dc, gb, gc, h1, h2, h3):
            cp(k).wait_send()


def fill_kernel(
    ids_ref, idv_ref, n_ref, du_ref, u_ref, x_ref, dg_ref,
    row_ref, cnt_ref, sel_ref, dw_ref, de_ref, uo_ref, xo_ref, dgo_ref,
    nv, duv, st, z, uv, xv, gv, sel, fv, fs, n_s, du_s, o_s, z_s, p_s, f_s, *, rows,
):
    cw = nv.shape[2]
    zr = z.shape[0]
    mb, tm = idv_ref.shape
    nt = mb * tm
    vl = de_ref.shape[0]
    lo = lax.axis_index("tp") * vl
    du_copy = pltpu.make_async_copy(du_ref, duv, du_s)
    du_copy.start()

    def n_copy(k):
        return pltpu.make_async_copy(n_ref.at[k], nv.at[k], n_s.at[k])

    def out(k):
        r = pl.ds(pl.multiple_of(k * cw, cw), cw)
        return pltpu.make_async_copy(st.at[k % 2], dw_ref.at[r], o_s.at[k % 2])

    def put(i):
        return pltpu.make_async_copy(z, de_ref.at[pl.ds(pl.multiple_of(i * zr, zr), zr)], z_s)

    for k in range(NC):
        n_copy(k).start()
    small = ((u_ref, uv, uo_ref), (x_ref, xv, xo_ref), (dg_ref, gv, dgo_ref))
    ins = [pltpu.make_async_copy(a, v, p_s.at[j]) for j, (a, v, _) in enumerate(small)]
    outs = [pltpu.make_async_copy(v, o, p_s.at[j]) for j, (_, v, o) in enumerate(small)]
    for cp in ins:
        cp.start()
    z[...] = jnp.zeros_like(z)
    early = rows // zr - NC * LATE

    @pl.loop(0, early)
    def _(i):
        put(i).start()

    for m in range(mb):
        row = idv_ref[m : m + 1, :] - lo
        later = jnp.zeros((1, tm), jnp.int32)
        for b in range(nt // 128):
            m0, t0 = divmod(b * 128, tm)
            col = jnp.broadcast_to(idv_ref[m0 : m0 + 1, t0 : t0 + 128] - lo, (128, 128)).T
            col = jnp.concatenate([col] * (tm // 128), axis=1)
            pos = lax.broadcasted_iota(jnp.int32, (128, tm), 0) + b * 128
            mine = lax.broadcasted_iota(jnp.int32, (128, tm), 1) + m * tm
            hit = jnp.where((col == row) & (pos < mine), 1, 0)
            later = jnp.maximum(later, jnp.max(hit, axis=0, keepdims=True))
        fv[:, m * tm : (m + 1) * tm] = jnp.where((row >= 0) & (row < vl), 1 - later, 0)
    cp = pltpu.make_async_copy(fv, fs, f_s)
    cp.start()
    sel[...] = jnp.zeros_like(sel)
    cp.wait()

    def scan(t, n):
        row_ref[n] = ids_ref[t // tm, t % tm] - lo
        return n + fs[0, t]

    cnt = lax.fori_loop(0, nt, scan, jnp.int32(0), unroll=8)
    cnt_ref[0] = cnt

    @pl.loop(0, cnt)
    def _(j):
        v = row_ref[j] + lo
        for m in range(mb):
            sel[pl.ds(j, 1), m * tm : (m + 1) * tm] = jnp.where(idv_ref[m : m + 1, :] == v, 1.0, 0.0)

    sel_ref[...] = sel[...].astype(BF16)
    for cp, co in zip(ins, outs):
        cp.wait()
        co.start()
    du_copy.wait()

    @pl.loop(0, NC)
    def _(k):
        n_copy(k).wait()
        for j in range(LATE):
            put(early + k * LATE + j).start()

        @pl.when(k >= 2)
        def _():
            out(k - 2).wait()

        st[k % 2] = lax.dot_general(nv[k], duv[...], (((0,), (0,)), ((), ())), preferred_element_type=F32)
        out(k).start()

    for co in outs:
        co.wait()
    out(NC - 2).wait()
    out(NC - 1).wait()

    @pl.loop(0, rows // zr)
    def _(i):
        put(i).wait()


def rest_kernel(_, de_ref, z, z_s, *, rows):
    zr = z.shape[0]
    left = (de_ref.shape[0] - rows) // zr

    def put(i):
        return pltpu.make_async_copy(z, de_ref.at[pl.ds(pl.multiple_of(rows + i * zr, zr), zr)], z_s)

    z[...] = jnp.zeros_like(z)

    @pl.loop(0, left)
    def _(i):
        put(i).start()

    @pl.loop(0, left)
    def _(i):
        put(i).wait()


def rows_kernel(*refs):
    row_ref, cnt_ref, sel_ref = refs[:3]
    dx_refs = refs[3:11]
    _, de_ref, dxv, dxs, o_s = refs[11:]
    nt = sel_ref.shape[0]
    cw = dxv.shape[-1]
    rb = 128
    me = lax.axis_index("tp")
    c = me % 2
    q = me // 2
    qx = q + 1 - 2 * (q % 2)
    qy = q + 2 - 4 * (q // 2)
    where = [(b, s) for b in (c, 1 - c) for s in (q, qx, qy, 3 - q)]
    for r, (b, s) in zip(dx_refs, where):
        dxv[:, b, s] = r[...]
    cnt = cnt_ref[0]

    def put(j):
        return pltpu.make_async_copy(dxs.at[pl.ds(j, 1)], de_ref.at[pl.ds(row_ref[j], 1)], o_s)

    @pl.loop(0, (cnt + rb - 1) // rb)
    def _(b):
        r = pl.ds(pl.multiple_of(b * rb, rb), rb)
        for k in range(NC):
            dxs[r, k * cw : (k + 1) * cw] = jnp.dot(
                sel_ref[r, :], dxv[k].reshape(nt, cw), preferred_element_type=F32
            )

        @pl.loop(b * rb, jnp.minimum(b * rb + rb, cnt))
        def _(j):
            put(j).start()

    @pl.loop(0, cnt)
    def _(j):
        put(j).wait()


def solution(mesh):
    groups = mesh.shape["tp"]

    def shift(bit):
        return [(r, r ^ bit) for r in range(groups)]

    def send(a, bit):
        return lax.ppermute(a, "tp", shift(bit))

    def local(ids, emb, g, w, du, dres):
        mb, t = ids.shape
        vl, d = emb.shape
        f = w.shape[1]
        nt = mb * t
        cw = d // NC
        tq = t // 4
        dma = pltpu.SemaphoreType.DMA
        sds = jax.ShapeDtypeStruct
        vb = lambda *s: pltpu.VMEM(s, BF16)
        vf = lambda *s: pltpu.VMEM(s, F32)
        local_only = pltpu.CompilerParams(vmem_limit_bytes=LIMIT)

        blk = (NC, tq, cw)
        x, n, u, dxo, dxp, dg = pl.pallas_call(
            main_kernel,
            out_shape=(
                sds((2, tq // 2, d), BF16),
                sds((NC, 2, 4, tq, cw), BF16),
                sds((2, 4, tq, f), BF16),
                sds(blk, BF16),
                sds(blk, BF16),
                sds((1, d), F32),
            ),
            in_specs=[ANY] * 6,
            out_specs=(VM, ANY, ANY, ANY, ANY, VM),
            scratch_shapes=[
                pltpu.VMEM((mb, t), jnp.int32), vb(2, vl, cw), vb(nt, vl),
                vb(NC, 2, 4, tq, cw), vb(NC, 4, tq, cw), vb(*blk), vb(*blk), vb(*blk),
                vb(*blk), vb(NC, tq // 2, cw), vb(2, tq // 2, d), vb(d),
                vb(NC, cw, f), vb(2, t, f),
                vb(NC, 2, 4, tq, cw), vb(NC, 4, tq, cw),
                vf(NC, 4, tq, cw), vf(*blk), vf(*blk), vf(*blk),
                vb(NC, 2, 4, tq, cw), vf(2, 4, tq, f), vb(2, 4, tq, f), vb(*blk), vb(*blk),
                vf(1, d), vf(1, d), vf(1, d), vf(3, 1, d),
                dma(()), dma((2,)), dma(()), dma(()), dma((NC,)), dma(()), dma(()), dma(()), dma((NC,)), dma((NC,)),
                dma(()), dma(()), dma((NC,)), dma((NC,)),
            ]
            + [dma((NC,))] * 18
            + [dma(())] * 2
            + [dma((NC,))] * 7
            + [dma((4,)), dma(()), dma(()), dma((2,)), dma((4,)), dma((4,))],
            compiler_params=pltpu.CompilerParams(collective_id=0, has_side_effects=True, vmem_limit_bytes=LIMIT),
            name="main",
        )(ids, emb, du, w, g, dres)

        zr = 128
        rows = vl // zr * 11 // 16 * zr
        near = [send(dxo, b) for b in (2, 4, 6)]
        row, cnt, sel, dw, de, u, x, dg = pl.pallas_call(
            functools.partial(fill_kernel, rows=rows),
            out_shape=(
                sds((nt + 8,), jnp.int32), sds((1,), jnp.int32), sds((nt, nt), BF16),
                sds((d, f), F32), sds((vl, d), F32), sds((nt, f), BF16), sds(x.shape, BF16), sds((1, d), F32),
            ),
            in_specs=[SM, VM] + [ANY] * 5,
            out_specs=(SM, SM, VM) + (ANY,) * 5,
            scratch_shapes=[
                vb(NC, nt, cw), vb(nt, f), vf(2, cw, f), vf(zr, d), vb(nt, f), vb(*x.shape), vf(1, d),
                vf(nt, nt), pltpu.VMEM((1, nt), jnp.int32), pltpu.SMEM((1, nt), jnp.int32),
                dma((NC,)), dma(()), dma((2,)), dma(()), dma((3,)), dma(()),
            ],
            compiler_params=local_only,
            cost_estimate=pl.CostEstimate(flops=18_000_000_000, bytes_accessed=vl * d * 4, transcendentals=0),
            name="fill",
        )(ids, ids, n.reshape(NC, nt, cw), du.reshape(nt, f), u.reshape(nt, f), x, dg)
        far = [send(a, 1) for a in near]

        de = pl.pallas_call(
            functools.partial(rest_kernel, rows=rows),
            out_shape=sds((vl, d), F32),
            in_specs=[ANY],
            out_specs=ANY,
            input_output_aliases={0: 0},
            scratch_shapes=[vf(zr, d), dma(())],
            compiler_params=pltpu.CompilerParams(vmem_limit_bytes=16 * 1024 * 1024),
            cost_estimate=pl.CostEstimate(flops=8_000_000_000, bytes_accessed=(vl - rows) * d * 4, transcendentals=0),
            name="rest",
        )(de)
        de = pl.pallas_call(
            rows_kernel,
            out_shape=sds((vl, d), F32),
            in_specs=[SM, SM, VM] + [VM] * 8 + [ANY],
            out_specs=ANY,
            input_output_aliases={11: 0},
            scratch_shapes=[vb(NC, 2, 4, tq, cw), vf(nt, d), dma(())],
            compiler_params=pltpu.CompilerParams(vmem_limit_bytes=24 * 1024 * 1024),
            name="rows",
        )(row, cnt, sel, dxo, *near, dxp, *far, de)
        return u.reshape(mb, t, f), x, de, dw, dg.reshape(d)

    return jax.shard_map(
        local,
        mesh=mesh,
        in_specs=(P("dp", None), P("tp", None), P(None), P(None, "tp"), P("dp", None, "tp"), P("dp", "tp", None)),
        out_specs=(P("dp", None, "tp"), P("dp", "tp", None), P(("dp", "tp"), None), P(None, ("dp", "tp")), P("dp")),
        check_vma=False,
    )
```

```python
import functools

import jax
import jax.numpy as jnp
from jax import lax
from jax.experimental import pallas as pl
from jax.experimental.pallas import tpu as pltpu
from jax.sharding import PartitionSpec as P

EPS = 1e-6
MESH = pl.DeviceIdType.MESH
F32 = jnp.float32
BF16 = jnp.bfloat16
ANY = pl.BlockSpec(memory_space=pl.ANY)
VM = pl.BlockSpec(memory_space=pltpu.VMEM)
SM = pl.BlockSpec(memory_space=pltpu.SMEM)
LIMIT = 60 * 1024 * 1024
NC = 6
HC = NC // 2
LATE = 1
EARLY = 2


def main_kernel(
    ids_ref, emb_ref, du_ref, w_ref, g_ref, dres_ref,
    xo_ref, n_ref, u_ref, dxo_ref, dxp_ref, dg_ref,
    idv, ev, oh, xp, xr, xfw, x1, x2, xh, xpr, drw, gv, wv, duv, pb, pr, sf, rf, r1, r2, nall, acc, ub, dxs, dxr,
    dgm, dgr, dgc, dgn,
    id_s, e_s, du_s, g_s, w_s, dl_s, dr_s, dr_r, xd_s, xd_r, xo_s, xo_r, pd_s, pd_r,
    xa_s, xb_s, xc_s, xa_r, xb_r, xc_r, da_s, db_s, dc_s, da_r, db_r, dc_r,
    ga_s, gb_s, gc_s, ga_r, gb_r, gc_r, h0_s, h0_r, h1_s, h2_s, h3_s, h1_r, h2_r, h3_r,
    no_s, uo_s, dx_s, dx_r, ox_s, dg_s, dg_r,
):
    me = lax.axis_index("tp")
    c = me % 2
    q = me // 2
    xq = q % 2
    yq = q // 2
    qx = q + 1 - 2 * xq
    qy = q + 2 - 4 * yq
    qd = 3 - q
    part = me + 1 - 2 * c
    dx_ = me + 2 - 4 * xq
    dy_ = me + 4 - 8 * yq
    dd_ = 2 * qd + c
    oc = 1 - c
    d, f = w_ref.shape
    cw = d // NC
    vl = emb_ref.shape[0]
    tq = xr.shape[2]
    nt = 8 * tq
    th = tq // 2

    def w_copy(k):
        rows = pl.ds(pl.multiple_of(k * cw, cw), cw)
        return pltpu.make_async_copy(w_ref.at[rows], wv.at[k], w_s.at[k])

    def chunk(i):
        return i % 2 * HC + i // 2

    barrier = pltpu.get_barrier_semaphore()
    for dev in (part, dx_, dy_, dd_):
        pl.semaphore_signal(barrier, inc=1, device_id={"tp": dev}, device_id_type=MESH)

    id_copy = pltpu.make_async_copy(ids_ref, idv, id_s)
    du_copy = pltpu.make_async_copy(du_ref, duv, du_s)
    g_copy = pltpu.make_async_copy(g_ref, gv, g_s)
    dl_copy = pltpu.make_async_copy(dres_ref.at[c], drw.at[c], dl_s)
    def e_copy(i):
        cols = pl.ds(pl.multiple_of(chunk(i) * cw, cw), cw)
        return pltpu.make_async_copy(emb_ref.at[:, cols], ev.at[i % 2], e_s.at[i % 2])

    du_copy.start()

    @pl.loop(0, NC)
    def _(i):
        w_copy(chunk(i)).start()

    id_copy.start()
    g_copy.start()
    dl_copy.start()
    e_copy(0).start()
    e_copy(1).start()
    pl.semaphore_wait(barrier, 4)

    def remote(src, dst, ss, rs, dev):
        return pltpu.make_async_remote_copy(
            src_ref=src, dst_ref=dst, send_sem=ss, recv_sem=rs, device_id={"tp": dev}, device_id_type=MESH
        )

    def xd(k):
        return remote(xp.at[k, oc], xr.at[k], xd_s.at[k], xd_r.at[k], part)

    dr = remote(dres_ref.at[oc], drw.at[c], dr_s, dr_r, part)

    def first(k):
        b = k // HC
        return qx + (qy - qx) * b, dx_ + (dy_ - dx_) * b

    def second(k):
        b = k // HC
        return qy + (qx - qy) * b, dy_ + (dx_ - dy_) * b

    def xa(k):
        return remote(xp.at[k, c, qd], xfw.at[k], xa_s.at[k], xa_r.at[k], first(k)[1])

    def xb(k):
        return remote(xp.at[k, c, first(k)[0]], x1.at[k], xb_s.at[k], xb_r.at[k], first(k)[1])

    def xc(k):
        return remote(xp.at[k, c, second(k)[0]], x2.at[k], xc_s.at[k], xc_r.at[k], second(k)[1])

    def da(k):
        return remote(sf.at[k, qd], rf.at[k], da_s.at[k], da_r.at[k], first(k)[1])

    def db(k):
        return remote(sf.at[k, first(k)[0]], r1.at[k], db_s.at[k], db_r.at[k], first(k)[1])

    def dc(k):
        return remote(sf.at[k, second(k)[0]], r2.at[k], dc_s.at[k], dc_r.at[k], second(k)[1])

    def pd(k):
        return remote(pb.at[k, oc], pr.at[k], pd_s.at[k], pd_r.at[k], part)

    def ga(k):
        return remote(nall.at[k, c, q], nall.at[k, c, q], ga_s.at[k], ga_r.at[k], first(k)[1])

    def gb(k):
        return remote(nall.at[k, c, q], nall.at[k, c, q], gb_s.at[k], gb_r.at[k], second(k)[1])

    def gc(k):
        s = first(k)[0]
        return remote(nall.at[k, c, s], nall.at[k, c, s], gc_s.at[k], gc_r.at[k], second(k)[1])

    def over(k, s, ss, rs):
        return remote(nall.at[k, c, s], nall.at[k, c, s], ss.at[k], rs.at[k], part)

    def h1(k):
        return over(k, first(k)[0], h1_s, h1_r)

    def h2(k):
        return over(k, second(k)[0], h2_s, h2_r)

    def h3(k):
        return over(k, qd, h3_s, h3_r)

    h0 = remote(nall.at[:, c, q], nall.at[:, c, q], h0_s, h0_r, part)

    du_copy.wait()

    def matmul(i):
        k = chunk(i)
        w_copy(k).wait()
        p = lax.dot_general(
            duv[...].reshape(nt, -1), wv[k], (((1,), (1,)), ((), ())), preferred_element_type=F32
        )
        pb[k] = p.astype(BF16).reshape(2, 4, tq, cw)
        pd(k).start()

    def combine(i):
        k = chunk(i)
        pd(k).wait_recv()
        for s in range(4):
            sf[k, s] = pb[k, c, s].astype(F32) + pr[k, s].astype(F32)
        da(k).start()

    matmul(0)

    @pl.loop(1, NC)
    def _(i):
        matmul(i)
        combine(i - 1)

    id_copy.wait()
    lo = me * vl
    for b in range(nt // 128):
        m, t0 = divmod(b * 128, 4 * tq)
        row = idv[m : m + 1, t0 : t0 + 128] - lo
        col = jnp.broadcast_to(row, (128, 128)).T

        @pl.loop(0, vl // 128, unroll=8)
        def _(j):
            lanes = lax.broadcasted_iota(jnp.int32, (128, 128), 1) + j * 128
            cols = pl.ds(pl.multiple_of(j * 128, 128), 128)
            oh[b * 128 : (b + 1) * 128, cols] = jnp.where(lanes == col, 1.0, 0.0).astype(BF16)

    combine(NC - 1)
    dr.start()

    def lookup(i):
        k = chunk(i)
        e_copy(i).wait()
        p = jnp.dot(oh[...], ev[i % 2], preferred_element_type=F32)
        xp[k] = p.astype(BF16).reshape(2, 4, tq, cw)
        xd(k).start()

        @pl.when(i + 2 < NC)
        def _():
            e_copy(i + 2).start()

    def pair(i):
        k = chunk(i)
        xd(k).wait_recv()
        xp[k, c] = xp[k, c] + xr[k]
        xa(k).start()
        xb(k).start()

    def forward(i):
        k = chunk(i)
        s = second(k)[0]
        da(k).wait_recv()
        sf[k, s] = sf[k, s] + rf[k]
        dc(k).start()

    db(chunk(0)).start()
    db(chunk(1)).start()
    lookup(0)

    @pl.loop(1, NC)
    def _(i):
        @pl.when(i <= NC // 2)
        def _():
            db(chunk(i + 2)).start()

        @pl.when(i == 1)
        def _():
            db(chunk(2)).start()

        @pl.when(i == 2)
        def _():
            forward(0)

        @pl.when(i == 4)
        def _():
            forward(1)

        lookup(i)
        pair(i - 1)

    pair(NC - 1)

    @pl.loop(0, NC)
    def _(i):
        k = chunk(i)
        s = second(k)[0]
        xa(k).wait_recv()
        xp[k, c, s] = xp[k, c, s] + xfw[k]
        xc(k).start()

    @pl.loop(EARLY, NC)
    def _(i):
        forward(i)

    acc[...] = jnp.zeros_like(acc)

    g_copy.wait()
    sq = jnp.zeros((tq, 1), F32)
    for k in range(NC):
        xb(k).wait_recv()
        xc(k).wait_recv()
        xk = xp[k, c, q] + x1[k] + x2[k]
        xh[k] = xk
        xk = xk.astype(F32)
        sq = sq + jnp.sum(xk * xk, axis=-1, keepdims=True)
    xo = remote(xh.at[:, pl.ds(pl.multiple_of(oc * th, th), th), :], xpr, xo_s, xo_r, part)
    xo.start()
    rs = lax.rsqrt(sq * (1.0 / d) + EPS)
    for k in (0, 3, 1, 4, 2, 5):
        cols = slice(k * cw, (k + 1) * cw)
        nall[k, c, q] = ((xh[k].astype(F32) * rs) * gv[cols].astype(F32).reshape(1, cw)).astype(BF16)
        ga(k).start()
    for k in (0, 3, 1, 4, 2, 5):
        gb(k).start()
    h0.start()
    for k in range(NC):
        xo_ref[c, :, k * cw : (k + 1) * cw] = xh[k, pl.ds(pl.multiple_of(c * th, th), th), :]
    dl_copy.wait()
    dr.wait_recv()
    xo.wait_recv()
    for k in range(NC):
        xo_ref[oc, :, k * cw : (k + 1) * cw] = xpr[k]

    def piece(k, s):
        acc[:, s] += jnp.dot(nall[k, :, s].reshape(2 * tq, cw), wv[k], preferred_element_type=F32).reshape(2, tq, f)

    def u_out(j, s):
        ub[:, s] = acc[:, s].astype(BF16)
        return pltpu.make_async_copy(ub.at[:, s], u_ref.at[:, s], uo_s.at[j])

    h0.wait_recv()

    @pl.loop(0, NC)
    def _(k):
        piece(k, q)

    uo = [u_out(0, q)]
    uo[0].start()

    m = jnp.zeros((tq, 1), F32)
    for k in (0, 3, 1, 4, 2, 5):
        cols = slice(k * cw, (k + 1) * cw)
        db(k).wait_recv()
        dc(k).wait_recv()
        dn = sf[k, q] + r1[k] + r2[k]
        r1[k] = dn
        nh = xh[k].astype(F32) * rs
        dnh = dn * nh
        dgm[:, cols] = jnp.sum(dnh, axis=0, keepdims=True)
        m = m + jnp.sum(dnh * gv[cols].astype(F32).reshape(1, cw), axis=-1, keepdims=True)
    dg0 = remote(dgm, dgr, dg_s.at[0], dg_r.at[0], part)
    dg0.start()
    m = m * (1.0 / d)
    for k in range(NC):
        cols = slice(k * cw, (k + 1) * cw)
        nh = xh[k].astype(F32) * rs
        dxn = rs * (gv[cols].astype(F32).reshape(1, cw) * r1[k] - nh * m)
        dxs[k] = (drw[:, :, cols].reshape(tq, cw).astype(F32) + dxn).astype(BF16)
    dxc = remote(dxs, dxr, dx_s, dx_r, part)
    dxc.start()
    ox = pltpu.make_async_copy(dxs, dxo_ref, ox_s.at[0])
    ox.start()
    dg0.wait_recv()
    dgc[...] = dgm[...] + dgr[...]
    dgs = [remote(dgc, dgn.at[j], dg_s.at[1 + j], dg_r.at[1 + j], dev) for j, dev in enumerate((dx_, dy_, dd_))]
    for cp in dgs:
        cp.start()

    @pl.loop(0, NC)
    def _(i):
        k = chunk(i)
        ga(k).wait_recv()
        gc(k).start()
        h1(k).start()

    dxc.wait_recv()
    oy = pltpu.make_async_copy(dxr, dxp_ref, ox_s.at[1])
    oy.start()

    @pl.loop(0, NC)
    def _(i):
        k = chunk(i)
        h1(k).wait_recv()
        piece(k, first(k)[0])

    def n_out(k):
        return pltpu.make_async_copy(nall.at[k], n_ref.at[k], no_s.at[k])

    def second_in(i):
        k = chunk(i)
        gb(k).wait_recv()
        h2(k).start()

    def second_use(i):
        k = chunk(i)
        h2(k).wait_recv()
        piece(k, second(k)[0])

    def last_in(i):
        k = chunk(i)
        gc(k).wait_recv()
        h3(k).start()

    def last_use(i):
        k = chunk(i)
        h3(k).wait_recv()
        n_out(k).start()
        piece(k, qd)

    second_in(0)

    @pl.loop(1, NC)
    def _(i):
        second_in(i)
        second_use(i - 1)

    last_in(0)
    second_use(NC - 1)
    for j, s in enumerate((qx, qy)):
        uo.append(u_out(1 + j, s))
        uo[-1].start()

    @pl.loop(1, NC)
    def _(i):
        last_in(i)
        last_use(i - 1)

    last_use(NC - 1)
    uo.append(u_out(3, qd))
    uo[-1].start()
    for cp in dgs:
        cp.wait_recv()
    dg_ref[...] = (dgc[...] + dgn[0]) + (dgn[1] + dgn[2])
    for cp in uo:
        cp.wait()

    ox.wait()
    oy.wait()
    dr.wait_send()
    xo.wait_send()
    h0.wait_send()
    dg0.wait_send()
    dxc.wait_send()
    for cp in dgs:
        cp.wait_send()

    @pl.loop(0, NC)
    def _(k):
        n_out(k).wait()
        for cp in (xd, pd, xa, xb, xc, da, db, dc, ga, gb, gc, h1, h2, h3):
            cp(k).wait_send()


def fill_kernel(
    ids_ref, idv_ref, n_ref, du_ref, u_ref, x_ref, dg_ref,
    row_ref, cnt_ref, sel_ref, dw_ref, de_ref, uo_ref, xo_ref, dgo_ref,
    nv, duv, st, z, uv, xv, gv, sel, fv, fs, n_s, du_s, o_s, z_s, p_s, f_s, *, rows,
):
    cw = nv.shape[2]
    zr = z.shape[0]
    mb, tm = idv_ref.shape
    nt = mb * tm
    vl = de_ref.shape[0]
    lo = lax.axis_index("tp") * vl
    du_copy = pltpu.make_async_copy(du_ref, duv, du_s)
    du_copy.start()

    def n_copy(k):
        return pltpu.make_async_copy(n_ref.at[k], nv.at[k], n_s.at[k])

    def out(k):
        r = pl.ds(pl.multiple_of(k * cw, cw), cw)
        return pltpu.make_async_copy(st.at[k % 2], dw_ref.at[r], o_s.at[k % 2])

    def put(i):
        return pltpu.make_async_copy(z, de_ref.at[pl.ds(pl.multiple_of(i * zr, zr), zr)], z_s)

    for k in range(NC):
        n_copy(k).start()
    small = ((u_ref, uv, uo_ref), (x_ref, xv, xo_ref), (dg_ref, gv, dgo_ref))
    ins = [pltpu.make_async_copy(a, v, p_s.at[j]) for j, (a, v, _) in enumerate(small)]
    outs = [pltpu.make_async_copy(v, o, p_s.at[j]) for j, (_, v, o) in enumerate(small)]
    for cp in ins:
        cp.start()
    z[...] = jnp.zeros_like(z)
    early = rows // zr - NC * LATE

    @pl.loop(0, early)
    def _(i):
        put(i).start()

    for m in range(mb):
        row = idv_ref[m : m + 1, :] - lo
        later = jnp.zeros((1, tm), jnp.int32)
        for b in range(nt // 128):
            m0, t0 = divmod(b * 128, tm)
            col = jnp.broadcast_to(idv_ref[m0 : m0 + 1, t0 : t0 + 128] - lo, (128, 128)).T
            col = jnp.concatenate([col] * (tm // 128), axis=1)
            pos = lax.broadcasted_iota(jnp.int32, (128, tm), 0) + b * 128
            mine = lax.broadcasted_iota(jnp.int32, (128, tm), 1) + m * tm
            hit = jnp.where((col == row) & (pos < mine), 1, 0)
            later = jnp.maximum(later, jnp.max(hit, axis=0, keepdims=True))
        fv[:, m * tm : (m + 1) * tm] = jnp.where((row >= 0) & (row < vl), 1 - later, 0)
    cp = pltpu.make_async_copy(fv, fs, f_s)
    cp.start()
    sel[...] = jnp.zeros_like(sel)
    cp.wait()

    def scan(t, n):
        row_ref[n] = ids_ref[t // tm, t % tm] - lo
        return n + fs[0, t]

    cnt = lax.fori_loop(0, nt, scan, jnp.int32(0), unroll=8)
    cnt_ref[0] = cnt

    @pl.loop(0, cnt)
    def _(j):
        v = row_ref[j] + lo
        for m in range(mb):
            sel[pl.ds(j, 1), m * tm : (m + 1) * tm] = jnp.where(idv_ref[m : m + 1, :] == v, 1.0, 0.0)

    sel_ref[...] = sel[...].astype(BF16)
    for cp, co in zip(ins, outs):
        cp.wait()
        co.start()
    du_copy.wait()

    @pl.loop(0, NC)
    def _(k):
        n_copy(k).wait()
        for j in range(LATE):
            put(early + k * LATE + j).start()

        @pl.when(k >= 2)
        def _():
            out(k - 2).wait()

        st[k % 2] = lax.dot_general(nv[k], duv[...], (((0,), (0,)), ((), ())), preferred_element_type=F32)
        out(k).start()

    for co in outs:
        co.wait()
    out(NC - 2).wait()
    out(NC - 1).wait()

    @pl.loop(0, rows // zr)
    def _(i):
        put(i).wait()


def rest_kernel(_, de_ref, z, z_s, *, rows):
    zr = z.shape[0]
    left = (de_ref.shape[0] - rows) // zr

    def put(i):
        return pltpu.make_async_copy(z, de_ref.at[pl.ds(pl.multiple_of(rows + i * zr, zr), zr)], z_s)

    z[...] = jnp.zeros_like(z)

    @pl.loop(0, left)
    def _(i):
        put(i).start()

    @pl.loop(0, left)
    def _(i):
        put(i).wait()


def rows_kernel(*refs):
    row_ref, cnt_ref, sel_ref = refs[:3]
    dx_refs = refs[3:11]
    _, de_ref, dxv, dxs, o_s = refs[11:]
    nt = sel_ref.shape[0]
    cw = dxv.shape[-1]
    rb = 128
    me = lax.axis_index("tp")
    c = me % 2
    q = me // 2
    qx = q + 1 - 2 * (q % 2)
    qy = q + 2 - 4 * (q // 2)
    where = [(b, s) for b in (c, 1 - c) for s in (q, qx, qy, 3 - q)]
    for r, (b, s) in zip(dx_refs, where):
        dxv[:, b, s] = r[...]
    cnt = cnt_ref[0]

    def put(j):
        return pltpu.make_async_copy(dxs.at[pl.ds(j, 1)], de_ref.at[pl.ds(row_ref[j], 1)], o_s)

    @pl.loop(0, (cnt + rb - 1) // rb)
    def _(b):
        r = pl.ds(pl.multiple_of(b * rb, rb), rb)
        for k in range(NC):
            dxs[r, k * cw : (k + 1) * cw] = jnp.dot(
                sel_ref[r, :], dxv[k].reshape(nt, cw), preferred_element_type=F32
            )

        @pl.loop(b * rb, jnp.minimum(b * rb + rb, cnt))
        def _(j):
            put(j).start()

    @pl.loop(0, cnt)
    def _(j):
        put(j).wait()


def solution(mesh):
    groups = mesh.shape["tp"]

    def shift(bit):
        return [(r, r ^ bit) for r in range(groups)]

    def send(a, bit):
        return lax.ppermute(a, "tp", shift(bit))

    def local(ids, emb, g, w, du, dres):
        mb, t = ids.shape
        vl, d = emb.shape
        f = w.shape[1]
        nt = mb * t
        cw = d // NC
        tq = t // 4
        dma = pltpu.SemaphoreType.DMA
        sds = jax.ShapeDtypeStruct
        vb = lambda *s: pltpu.VMEM(s, BF16)
        vf = lambda *s: pltpu.VMEM(s, F32)
        local_only = pltpu.CompilerParams(vmem_limit_bytes=LIMIT)

        blk = (NC, tq, cw)
        x, n, u, dxo, dxp, dg = pl.pallas_call(
            main_kernel,
            out_shape=(
                sds((2, tq // 2, d), BF16),
                sds((NC, 2, 4, tq, cw), BF16),
                sds((2, 4, tq, f), BF16),
                sds(blk, BF16),
                sds(blk, BF16),
                sds((1, d), F32),
            ),
            in_specs=[ANY] * 6,
            out_specs=(VM, ANY, ANY, ANY, ANY, VM),
            scratch_shapes=[
                pltpu.VMEM((mb, t), jnp.int32), vb(2, vl, cw), vb(nt, vl),
                vb(NC, 2, 4, tq, cw), vb(NC, 4, tq, cw), vb(*blk), vb(*blk), vb(*blk),
                vb(*blk), vb(NC, tq // 2, cw), vb(2, tq // 2, d), vb(d),
                vb(NC, cw, f), vb(2, t, f),
                vb(NC, 2, 4, tq, cw), vb(NC, 4, tq, cw),
                vf(NC, 4, tq, cw), vf(*blk), vf(*blk), vf(*blk),
                vb(NC, 2, 4, tq, cw), vf(2, 4, tq, f), vb(2, 4, tq, f), vb(*blk), vb(*blk),
                vf(1, d), vf(1, d), vf(1, d), vf(3, 1, d),
                dma(()), dma((2,)), dma(()), dma(()), dma((NC,)), dma(()), dma(()), dma(()), dma((NC,)), dma((NC,)),
                dma(()), dma(()), dma((NC,)), dma((NC,)),
            ]
            + [dma((NC,))] * 18
            + [dma(())] * 2
            + [dma((NC,))] * 7
            + [dma((4,)), dma(()), dma(()), dma((2,)), dma((4,)), dma((4,))],
            compiler_params=pltpu.CompilerParams(collective_id=0, has_side_effects=True, vmem_limit_bytes=LIMIT),
            name="main",
        )(ids, emb, du, w, g, dres)

        zr = 128
        rows = vl // zr * 11 // 16 * zr
        near = [send(dxo, b) for b in (2, 4, 6)]
        row, cnt, sel, dw, de, u, x, dg = pl.pallas_call(
            functools.partial(fill_kernel, rows=rows),
            out_shape=(
                sds((nt + 8,), jnp.int32), sds((1,), jnp.int32), sds((nt, nt), BF16),
                sds((d, f), F32), sds((vl, d), F32), sds((nt, f), BF16), sds(x.shape, BF16), sds((1, d), F32),
            ),
            in_specs=[SM, VM] + [ANY] * 5,
            out_specs=(SM, SM, VM) + (ANY,) * 5,
            scratch_shapes=[
                vb(NC, nt, cw), vb(nt, f), vf(2, cw, f), vf(zr, d), vb(nt, f), vb(*x.shape), vf(1, d),
                vf(nt, nt), pltpu.VMEM((1, nt), jnp.int32), pltpu.SMEM((1, nt), jnp.int32),
                dma((NC,)), dma(()), dma((2,)), dma(()), dma((3,)), dma(()),
            ],
            compiler_params=local_only,
            cost_estimate=pl.CostEstimate(flops=18_000_000_000, bytes_accessed=vl * d * 4, transcendentals=0),
            name="fill",
        )(ids, ids, n.reshape(NC, nt, cw), du.reshape(nt, f), u.reshape(nt, f), x, dg)
        far = [send(a, 1) for a in near]

        de = pl.pallas_call(
            functools.partial(rest_kernel, rows=rows),
            out_shape=sds((vl, d), F32),
            in_specs=[ANY],
            out_specs=ANY,
            input_output_aliases={0: 0},
            scratch_shapes=[vf(zr, d), dma(())],
            compiler_params=pltpu.CompilerParams(vmem_limit_bytes=16 * 1024 * 1024),
            cost_estimate=pl.CostEstimate(flops=8_000_000_000, bytes_accessed=(vl - rows) * d * 4, transcendentals=0),
            name="rest",
        )(de)
        de = pl.pallas_call(
            rows_kernel,
            out_shape=sds((vl, d), F32),
            in_specs=[SM, SM, VM] + [VM] * 8 + [ANY],
            out_specs=ANY,
            input_output_aliases={11: 0},
            scratch_shapes=[vb(NC, 2, 4, tq, cw), vf(nt, d), dma(())],
            compiler_params=pltpu.CompilerParams(vmem_limit_bytes=24 * 1024 * 1024),
            name="rows",
        )(row, cnt, sel, dxo, *near, dxp, *far, de)
        return u.reshape(mb, t, f), x, de, dw, dg.reshape(d)

    return jax.shard_map(
        local,
        mesh=mesh,
        in_specs=(P("dp", None), P("tp", None), P(None), P(None, "tp"), P("dp", None, "tp"), P("dp", "tp", None)),
        out_specs=(P("dp", None, "tp"), P("dp", "tp", None), P(("dp", "tp"), None), P(None, ("dp", "tp")), P("dp")),
        check_vma=False,
    )
```

```python
import functools

import jax
import jax.numpy as jnp
from jax import lax
from jax.experimental import pallas as pl
from jax.experimental.pallas import tpu as pltpu
from jax.sharding import PartitionSpec as P

EPS = 1e-6
MESH = pl.DeviceIdType.MESH
F32 = jnp.float32
BF16 = jnp.bfloat16
ANY = pl.BlockSpec(memory_space=pl.ANY)
VM = pl.BlockSpec(memory_space=pltpu.VMEM)
SM = pl.BlockSpec(memory_space=pltpu.SMEM)
LIMIT = 60 * 1024 * 1024
NC = 6
HC = NC // 2
LATE = 1
EARLY = 2


def main_kernel(
    ids_ref, emb_ref, du_ref, w_ref, g_ref, dres_ref,
    xo_ref, n_ref, u_ref, dxo_ref, dxp_ref, dg_ref,
    idv, ev, oh, xp, xr, xfw, x1, x2, xh, xpr, drw, gv, wv, duv, pb, pr, sf, rf, r1, r2, nall, acc, ub, dxs, dxr, xov, dgo,
    dgm, dgr, dgc, dgn,
    id_s, e_s, du_s, g_s, w_s, dl_s, dr_s, dr_r, xd_s, xd_r, xo_s, xo_r, pd_s, pd_r,
    xa_s, xb_s, xc_s, xa_r, xb_r, xc_r, da_s, db_s, dc_s, da_r, db_r, dc_r,
    ga_s, gb_s, gc_s, ga_r, gb_r, gc_r, h0_s, h0_r, h1_s, h2_s, h3_s, h1_r, h2_r, h3_r,
    no_s, uo_s, dx_s, dx_r, ox_s, dg_s, dg_r,
):
    me = lax.axis_index("tp")
    c = me % 2
    q = me // 2
    xq = q % 2
    yq = q // 2
    qx = q + 1 - 2 * xq
    qy = q + 2 - 4 * yq
    qd = 3 - q
    part = me + 1 - 2 * c
    dx_ = me + 2 - 4 * xq
    dy_ = me + 4 - 8 * yq
    dd_ = 2 * qd + c
    oc = 1 - c
    d, f = w_ref.shape
    cw = d // NC
    vl = emb_ref.shape[0]
    tq = xr.shape[2]
    nt = 8 * tq
    th = tq // 2

    def w_copy(k):
        rows = pl.ds(pl.multiple_of(k * cw, cw), cw)
        return pltpu.make_async_copy(w_ref.at[rows], wv.at[k], w_s.at[k])

    def chunk(i):
        return i % 2 * HC + i // 2

    barrier = pltpu.get_barrier_semaphore()
    for dev in (part, dx_, dy_, dd_):
        pl.semaphore_signal(barrier, inc=1, device_id={"tp": dev}, device_id_type=MESH)

    id_copy = pltpu.make_async_copy(ids_ref, idv, id_s)
    du_copy = pltpu.make_async_copy(du_ref, duv, du_s)
    g_copy = pltpu.make_async_copy(g_ref, gv, g_s)
    dl_copy = pltpu.make_async_copy(dres_ref.at[c], drw.at[c], dl_s)
    def e_copy(i):
        cols = pl.ds(pl.multiple_of(chunk(i) * cw, cw), cw)
        return pltpu.make_async_copy(emb_ref.at[:, cols], ev.at[i % 2], e_s.at[i % 2])

    du_copy.start()

    @pl.loop(0, NC)
    def _(i):
        w_copy(chunk(i)).start()

    id_copy.start()
    g_copy.start()
    dl_copy.start()
    e_copy(0).start()
    e_copy(1).start()

    def remote(src, dst, ss, rs, dev):
        return pltpu.make_async_remote_copy(
            src_ref=src, dst_ref=dst, send_sem=ss, recv_sem=rs, device_id={"tp": dev}, device_id_type=MESH
        )

    def xd(k):
        return remote(xp.at[k, oc], xr.at[k], xd_s.at[k], xd_r.at[k], part)

    dr = remote(dres_ref.at[oc], drw.at[c], dr_s, dr_r, part)

    def first(k):
        b = k // HC
        return qx + (qy - qx) * b, dx_ + (dy_ - dx_) * b

    def second(k):
        b = k // HC
        return qy + (qx - qy) * b, dy_ + (dx_ - dy_) * b

    def xa(k):
        return remote(xp.at[k, c, qd], xfw.at[k], xa_s.at[k], xa_r.at[k], first(k)[1])

    def xb(k):
        return remote(xp.at[k, c, first(k)[0]], x1.at[k], xb_s.at[k], xb_r.at[k], first(k)[1])

    def xc(k):
        return remote(xp.at[k, c, second(k)[0]], x2.at[k], xc_s.at[k], xc_r.at[k], second(k)[1])

    def da(k):
        return remote(sf.at[k, qd], rf.at[k], da_s.at[k], da_r.at[k], first(k)[1])

    def db(k):
        return remote(sf.at[k, first(k)[0]], r1.at[k], db_s.at[k], db_r.at[k], first(k)[1])

    def dc(k):
        return remote(sf.at[k, second(k)[0]], r2.at[k], dc_s.at[k], dc_r.at[k], second(k)[1])

    def pd(k):
        return remote(pb.at[k, oc], pr.at[k], pd_s.at[k], pd_r.at[k], part)

    def ga(k):
        return remote(nall.at[k, c, q], nall.at[k, c, q], ga_s.at[k], ga_r.at[k], first(k)[1])

    def gb(k):
        return remote(nall.at[k, c, q], nall.at[k, c, q], gb_s.at[k], gb_r.at[k], second(k)[1])

    def gc(k):
        s = first(k)[0]
        return remote(nall.at[k, c, s], nall.at[k, c, s], gc_s.at[k], gc_r.at[k], second(k)[1])

    def over(k, s, ss, rs):
        return remote(nall.at[k, c, s], nall.at[k, c, s], ss.at[k], rs.at[k], part)

    def h1(k):
        return over(k, first(k)[0], h1_s, h1_r)

    def h2(k):
        return over(k, second(k)[0], h2_s, h2_r)

    def h3(k):
        return over(k, qd, h3_s, h3_r)

    h0 = remote(nall.at[:, c, q], nall.at[:, c, q], h0_s, h0_r, part)

    du_copy.wait()

    def matmul(i):
        k = chunk(i)
        w_copy(k).wait()
        p = lax.dot_general(
            duv[...].reshape(nt, -1), wv[k], (((1,), (1,)), ((), ())), preferred_element_type=F32
        )
        pb[k] = p.astype(BF16).reshape(2, 4, tq, cw)
        pd(k).start()

    def combine(i):
        k = chunk(i)
        pd(k).wait_recv()
        for s in range(4):
            sf[k, s] = pb[k, c, s].astype(F32) + pr[k, s].astype(F32)
        da(k).start()

    k0 = chunk(0)
    w_copy(k0).wait()
    for m in (oc, c):
        p = lax.dot_general(duv[m], wv[k0], (((1,), (1,)), ((), ())), preferred_element_type=F32)
        pb[k0, m] = p.astype(BF16).reshape(4, tq, cw)
        if m is oc:
            pl.semaphore_wait(barrier, 4)
            pd(k0).start()

    @pl.loop(1, NC)
    def _(i):
        matmul(i)
        combine(i - 1)

    id_copy.wait()
    lo = me * vl
    for b in range(nt // 128):
        m, t0 = divmod(b * 128, 4 * tq)
        row = idv[m : m + 1, t0 : t0 + 128] - lo
        col = jnp.broadcast_to(row, (128, 128)).T

        @pl.loop(0, vl // 128, unroll=8)
        def _(j):
            lanes = lax.broadcasted_iota(jnp.int32, (128, 128), 1) + j * 128
            cols = pl.ds(pl.multiple_of(j * 128, 128), 128)
            oh[b * 128 : (b + 1) * 128, cols] = jnp.where(lanes == col, 1.0, 0.0).astype(BF16)

    combine(NC - 1)
    dr.start()

    def lookup(i):
        k = chunk(i)
        e_copy(i).wait()
        p = jnp.dot(oh[...], ev[i % 2], preferred_element_type=F32)
        xp[k] = p.astype(BF16).reshape(2, 4, tq, cw)
        xd(k).start()

        @pl.when(i + 2 < NC)
        def _():
            e_copy(i + 2).start()

    def pair(i):
        k = chunk(i)
        xd(k).wait_recv()
        xp[k, c] = xp[k, c] + xr[k]
        xa(k).start()
        xb(k).start()

    def forward(i):
        k = chunk(i)
        s = second(k)[0]
        da(k).wait_recv()
        sf[k, s] = sf[k, s] + rf[k]
        dc(k).start()

    db(chunk(0)).start()
    db(chunk(1)).start()
    lookup(0)

    @pl.loop(1, NC)
    def _(i):
        @pl.when(i <= NC // 2)
        def _():
            db(chunk(i + 2)).start()

        @pl.when(i == 1)
        def _():
            db(chunk(2)).start()

        @pl.when(i == 2)
        def _():
            forward(0)

        @pl.when(i == 4)
        def _():
            forward(1)

        lookup(i)
        pair(i - 1)

    pair(NC - 1)

    @pl.loop(0, NC)
    def _(i):
        k = chunk(i)
        s = second(k)[0]
        xa(k).wait_recv()
        xp[k, c, s] = xp[k, c, s] + xfw[k]
        xc(k).start()

    @pl.loop(EARLY, NC)
    def _(i):
        forward(i)

    acc[...] = jnp.zeros_like(acc)

    g_copy.wait()
    sq = jnp.zeros((tq, 1), F32)
    for k in range(NC):
        xb(k).wait_recv()
        xc(k).wait_recv()
        xk = xp[k, c, q] + x1[k] + x2[k]
        xh[k] = xk
        xk = xk.astype(F32)
        sq = sq + jnp.sum(xk * xk, axis=-1, keepdims=True)
    xo = remote(xh.at[:, pl.ds(pl.multiple_of(oc * th, th), th), :], xpr, xo_s, xo_r, part)
    xo.start()
    rs = lax.rsqrt(sq * (1.0 / d) + EPS)
    for k in (0, 3, 1, 4, 2, 5):
        cols = slice(k * cw, (k + 1) * cw)
        nall[k, c, q] = ((xh[k].astype(F32) * rs) * gv[cols].astype(F32).reshape(1, cw)).astype(BF16)
        ga(k).start()
    for k in (0, 3, 1, 4, 2, 5):
        gb(k).start()
    h0.start()
    for k in range(NC):
        xov[c, :, k * cw : (k + 1) * cw] = xh[k, pl.ds(pl.multiple_of(c * th, th), th), :]
    dl_copy.wait()
    dr.wait_recv()
    xo.wait_recv()
    for k in range(NC):
        xov[oc, :, k * cw : (k + 1) * cw] = xpr[k]
    oz = pltpu.make_async_copy(xov, xo_ref, ox_s.at[2])
    oz.start()

    def piece(k, s):
        acc[:, s] += jnp.dot(nall[k, :, s].reshape(2 * tq, cw), wv[k], preferred_element_type=F32).reshape(2, tq, f)

    def u_out(j, s):
        ub[:, s] = acc[:, s].astype(BF16)
        return pltpu.make_async_copy(ub.at[:, s], u_ref.at[:, s], uo_s.at[j])

    h0.wait_recv()

    @pl.loop(0, NC)
    def _(k):
        piece(k, q)

    uo = [u_out(0, q)]
    uo[0].start()

    m = jnp.zeros((tq, 1), F32)
    for k in (0, 3, 1, 4, 2, 5):
        cols = slice(k * cw, (k + 1) * cw)
        db(k).wait_recv()
        dc(k).wait_recv()
        dn = sf[k, q] + r1[k] + r2[k]
        r1[k] = dn
        nh = xh[k].astype(F32) * rs
        dnh = dn * nh
        dgm[:, cols] = jnp.sum(dnh, axis=0, keepdims=True)
        m = m + jnp.sum(dnh * gv[cols].astype(F32).reshape(1, cw), axis=-1, keepdims=True)
    dg0 = remote(dgm, dgr, dg_s.at[0], dg_r.at[0], part)
    dg0.start()
    m = m * (1.0 / d)
    for k in range(NC):
        cols = slice(k * cw, (k + 1) * cw)
        nh = xh[k].astype(F32) * rs
        dxn = rs * (gv[cols].astype(F32).reshape(1, cw) * r1[k] - nh * m)
        dxs[k] = (drw[:, :, cols].reshape(tq, cw).astype(F32) + dxn).astype(BF16)
    dxc = remote(dxs, dxr, dx_s, dx_r, part)
    dxc.start()
    ox = pltpu.make_async_copy(dxs, dxo_ref, ox_s.at[0])
    ox.start()
    dg0.wait_recv()
    dgc[...] = dgm[...] + dgr[...]
    dgs = [remote(dgc, dgn.at[j], dg_s.at[1 + j], dg_r.at[1 + j], dev) for j, dev in enumerate((dx_, dy_, dd_))]
    for cp in dgs:
        cp.start()

    @pl.loop(0, NC)
    def _(i):
        k = chunk(i)
        ga(k).wait_recv()
        gc(k).start()
        h1(k).start()

    dxc.wait_recv()
    oy = pltpu.make_async_copy(dxr, dxp_ref, ox_s.at[1])
    oy.start()

    @pl.loop(0, NC)
    def _(i):
        k = chunk(i)
        h1(k).wait_recv()
        piece(k, first(k)[0])

    def n_out(k):
        return pltpu.make_async_copy(nall.at[k], n_ref.at[k], no_s.at[k])

    def second_in(i):
        k = chunk(i)
        gb(k).wait_recv()
        h2(k).start()

    def second_use(i):
        k = chunk(i)
        h2(k).wait_recv()
        piece(k, second(k)[0])

    def last_in(i):
        k = chunk(i)
        gc(k).wait_recv()
        h3(k).start()

    def last_use(i):
        k = chunk(i)
        h3(k).wait_recv()
        n_out(k).start()
        piece(k, qd)

    second_in(0)

    @pl.loop(1, NC)
    def _(i):
        second_in(i)
        second_use(i - 1)

    last_in(0)
    second_use(NC - 1)
    for j, s in enumerate((qx, qy)):
        uo.append(u_out(1 + j, s))
        uo[-1].start()

    @pl.loop(1, NC)
    def _(i):
        last_in(i)
        last_use(i - 1)

    for cp in dgs:
        cp.wait_recv()
    dgo[...] = (dgc[...] + dgn[0]) + (dgn[1] + dgn[2])
    og = pltpu.make_async_copy(dgo, dg_ref, ox_s.at[3])
    og.start()
    last_use(NC - 1)
    uo.append(u_out(3, qd))
    uo[-1].start()
    for cp in uo:
        cp.wait()

    for cp in (ox, oy, oz, og):
        cp.wait()
    dr.wait_send()
    xo.wait_send()
    h0.wait_send()
    dg0.wait_send()
    dxc.wait_send()
    for cp in dgs:
        cp.wait_send()

    @pl.loop(0, NC)
    def _(k):
        n_out(k).wait()
        for cp in (xd, pd, xa, xb, xc, da, db, dc, ga, gb, gc, h1, h2, h3):
            cp(k).wait_send()


def fill_kernel(
    ids_ref, idv_ref, n_ref, du_ref, u_ref, x_ref, dg_ref,
    row_ref, cnt_ref, sel_ref, dw_ref, de_ref, uo_ref, xo_ref, dgo_ref,
    nv, duv, st, z, uv, xv, gv, sel, fv, fs, n_s, du_s, o_s, z_s, p_s, f_s, *, rows,
):
    cw = nv.shape[2]
    zr = z.shape[0]
    mb, tm = idv_ref.shape
    nt = mb * tm
    vl = de_ref.shape[0]
    lo = lax.axis_index("tp") * vl
    du_copy = pltpu.make_async_copy(du_ref, duv, du_s)
    du_copy.start()

    def n_copy(k):
        return pltpu.make_async_copy(n_ref.at[k], nv.at[k], n_s.at[k])

    def out(k):
        r = pl.ds(pl.multiple_of(k * cw, cw), cw)
        return pltpu.make_async_copy(st.at[k % 2], dw_ref.at[r], o_s.at[k % 2])

    def put(i):
        return pltpu.make_async_copy(z, de_ref.at[pl.ds(pl.multiple_of(i * zr, zr), zr)], z_s)

    for k in range(NC):
        n_copy(k).start()
    small = ((u_ref, uv, uo_ref), (x_ref, xv, xo_ref), (dg_ref, gv, dgo_ref))
    ins = [pltpu.make_async_copy(a, v, p_s.at[j]) for j, (a, v, _) in enumerate(small)]
    outs = [pltpu.make_async_copy(v, o, p_s.at[j]) for j, (_, v, o) in enumerate(small)]
    for cp in ins:
        cp.start()
    z[...] = jnp.zeros_like(z)
    early = rows // zr - NC * LATE

    @pl.loop(0, early)
    def _(i):
        put(i).start()

    for m in range(mb):
        row = idv_ref[m : m + 1, :] - lo
        later = jnp.zeros((1, tm), jnp.int32)
        for b in range(nt // 128):
            m0, t0 = divmod(b * 128, tm)
            col = jnp.broadcast_to(idv_ref[m0 : m0 + 1, t0 : t0 + 128] - lo, (128, 128)).T
            col = jnp.concatenate([col] * (tm // 128), axis=1)
            pos = lax.broadcasted_iota(jnp.int32, (128, tm), 0) + b * 128
            mine = lax.broadcasted_iota(jnp.int32, (128, tm), 1) + m * tm
            hit = jnp.where((col == row) & (pos < mine), 1, 0)
            later = jnp.maximum(later, jnp.max(hit, axis=0, keepdims=True))
        fv[:, m * tm : (m + 1) * tm] = jnp.where((row >= 0) & (row < vl), 1 - later, 0)
    cp = pltpu.make_async_copy(fv, fs, f_s)
    cp.start()
    sel[...] = jnp.zeros_like(sel)
    cp.wait()

    def scan(t, n):
        row_ref[n] = ids_ref[t // tm, t % tm] - lo
        return n + fs[0, t]

    cnt = lax.fori_loop(0, nt, scan, jnp.int32(0), unroll=8)
    cnt_ref[0] = cnt

    @pl.loop(0, cnt)
    def _(j):
        v = row_ref[j] + lo
        for m in range(mb):
            sel[pl.ds(j, 1), m * tm : (m + 1) * tm] = jnp.where(idv_ref[m : m + 1, :] == v, 1.0, 0.0)

    sel_ref[...] = sel[...].astype(BF16)
    for cp, co in zip(ins, outs):
        cp.wait()
        co.start()
    du_copy.wait()

    @pl.loop(0, NC)
    def _(k):
        n_copy(k).wait()
        for j in range(LATE):
            put(early + k * LATE + j).start()

        @pl.when(k >= 2)
        def _():
            out(k - 2).wait()

        st[k % 2] = lax.dot_general(nv[k], duv[...], (((0,), (0,)), ((), ())), preferred_element_type=F32)
        out(k).start()

    for co in outs:
        co.wait()
    out(NC - 2).wait()
    out(NC - 1).wait()

    @pl.loop(0, rows // zr)
    def _(i):
        put(i).wait()


def rest_kernel(_, de_ref, z, z_s, *, rows):
    zr = z.shape[0]
    left = (de_ref.shape[0] - rows) // zr

    def put(i):
        return pltpu.make_async_copy(z, de_ref.at[pl.ds(pl.multiple_of(rows + i * zr, zr), zr)], z_s)

    z[...] = jnp.zeros_like(z)

    @pl.loop(0, left)
    def _(i):
        put(i).start()

    @pl.loop(0, left)
    def _(i):
        put(i).wait()


def rows_kernel(*refs):
    row_ref, cnt_ref, sel_ref = refs[:3]
    dx_refs = refs[3:11]
    _, de_ref, dxv, dxs, o_s = refs[11:]
    nt = sel_ref.shape[0]
    cw = dxv.shape[-1]
    rb = 128
    me = lax.axis_index("tp")
    c = me % 2
    q = me // 2
    qx = q + 1 - 2 * (q % 2)
    qy = q + 2 - 4 * (q // 2)
    where = [(b, s) for b in (c, 1 - c) for s in (q, qx, qy, 3 - q)]
    for r, (b, s) in zip(dx_refs, where):
        dxv[:, b, s] = r[...]
    cnt = cnt_ref[0]

    def put(j):
        return pltpu.make_async_copy(dxs.at[pl.ds(j, 1)], de_ref.at[pl.ds(row_ref[j], 1)], o_s)

    @pl.loop(0, (cnt + rb - 1) // rb)
    def _(b):
        r = pl.ds(pl.multiple_of(b * rb, rb), rb)
        for k in range(NC):
            dxs[r, k * cw : (k + 1) * cw] = jnp.dot(
                sel_ref[r, :], dxv[k].reshape(nt, cw), preferred_element_type=F32
            )

        @pl.loop(b * rb, jnp.minimum(b * rb + rb, cnt))
        def _(j):
            put(j).start()

    @pl.loop(0, cnt)
    def _(j):
        put(j).wait()


def solution(mesh):
    groups = mesh.shape["tp"]

    def shift(bit):
        return [(r, r ^ bit) for r in range(groups)]

    def send(a, bit):
        return lax.ppermute(a, "tp", shift(bit))

    def local(ids, emb, g, w, du, dres):
        mb, t = ids.shape
        vl, d = emb.shape
        f = w.shape[1]
        nt = mb * t
        cw = d // NC
        tq = t // 4
        dma = pltpu.SemaphoreType.DMA
        sds = jax.ShapeDtypeStruct
        vb = lambda *s: pltpu.VMEM(s, BF16)
        vf = lambda *s: pltpu.VMEM(s, F32)
        local_only = pltpu.CompilerParams(vmem_limit_bytes=LIMIT)

        blk = (NC, tq, cw)
        x, n, u, dxo, dxp, dg = pl.pallas_call(
            main_kernel,
            out_shape=(
                sds((2, tq // 2, d), BF16),
                sds((NC, 2, 4, tq, cw), BF16),
                sds((2, 4, tq, f), BF16),
                sds(blk, BF16),
                sds(blk, BF16),
                sds((1, d), F32),
            ),
            in_specs=[ANY] * 6,
            out_specs=(ANY,) * 6,
            scratch_shapes=[
                pltpu.VMEM((mb, t), jnp.int32), vb(2, vl, cw), vb(nt, vl),
                vb(NC, 2, 4, tq, cw), vb(NC, 4, tq, cw), vb(*blk), vb(*blk), vb(*blk),
                vb(*blk), vb(NC, tq // 2, cw), vb(2, tq // 2, d), vb(d),
                vb(NC, cw, f), vb(2, t, f),
                vb(NC, 2, 4, tq, cw), vb(NC, 4, tq, cw),
                vf(NC, 4, tq, cw), vf(*blk), vf(*blk), vf(*blk),
                vb(NC, 2, 4, tq, cw), vf(2, 4, tq, f), vb(2, 4, tq, f), vb(*blk), vb(*blk), vb(2, tq // 2, d), vf(1, d),
                vf(1, d), vf(1, d), vf(1, d), vf(3, 1, d),
                dma(()), dma((2,)), dma(()), dma(()), dma((NC,)), dma(()), dma(()), dma(()), dma((NC,)), dma((NC,)),
                dma(()), dma(()), dma((NC,)), dma((NC,)),
            ]
            + [dma((NC,))] * 18
            + [dma(())] * 2
            + [dma((NC,))] * 7
            + [dma((4,)), dma(()), dma(()), dma((4,)), dma((4,)), dma((4,))],
            compiler_params=pltpu.CompilerParams(collective_id=0, has_side_effects=True, vmem_limit_bytes=LIMIT),
            name="main",
        )(ids, emb, du, w, g, dres)

        zr = 128
        rows = vl // zr * 11 // 16 * zr
        near = [send(dxo, b) for b in (2, 4, 6)]
        row, cnt, sel, dw, de, u, x, dg = pl.pallas_call(
            functools.partial(fill_kernel, rows=rows),
            out_shape=(
                sds((nt + 8,), jnp.int32), sds((1,), jnp.int32), sds((nt, nt), BF16),
                sds((d, f), F32), sds((vl, d), F32), sds((nt, f), BF16), sds(x.shape, BF16), sds((1, d), F32),
            ),
            in_specs=[SM, VM] + [ANY] * 5,
            out_specs=(SM, SM, VM) + (ANY,) * 5,
            scratch_shapes=[
                vb(NC, nt, cw), vb(nt, f), vf(2, cw, f), vf(zr, d), vb(nt, f), vb(*x.shape), vf(1, d),
                vf(nt, nt), pltpu.VMEM((1, nt), jnp.int32), pltpu.SMEM((1, nt), jnp.int32),
                dma((NC,)), dma(()), dma((2,)), dma(()), dma((3,)), dma(()),
            ],
            compiler_params=local_only,
            cost_estimate=pl.CostEstimate(flops=18_000_000_000, bytes_accessed=vl * d * 4, transcendentals=0),
            name="fill",
        )(ids, ids, n.reshape(NC, nt, cw), du.reshape(nt, f), u.reshape(nt, f), x, dg)
        far = [send(a, 1) for a in near]

        de = pl.pallas_call(
            functools.partial(rest_kernel, rows=rows),
            out_shape=sds((vl, d), F32),
            in_specs=[ANY],
            out_specs=ANY,
            input_output_aliases={0: 0},
            scratch_shapes=[vf(zr, d), dma(())],
            compiler_params=pltpu.CompilerParams(vmem_limit_bytes=16 * 1024 * 1024),
            cost_estimate=pl.CostEstimate(flops=8_000_000_000, bytes_accessed=(vl - rows) * d * 4, transcendentals=0),
            name="rest",
        )(de)
        de = pl.pallas_call(
            rows_kernel,
            out_shape=sds((vl, d), F32),
            in_specs=[SM, SM, VM] + [VM] * 8 + [ANY],
            out_specs=ANY,
            input_output_aliases={11: 0},
            scratch_shapes=[vb(NC, 2, 4, tq, cw), vf(nt, d), dma(())],
            compiler_params=pltpu.CompilerParams(vmem_limit_bytes=24 * 1024 * 1024),
            name="rows",
        )(row, cnt, sel, dxo, *near, dxp, *far, de)
        return u.reshape(mb, t, f), x, de, dw, dg.reshape(d)

    return jax.shard_map(
        local,
        mesh=mesh,
        in_specs=(P("dp", None), P("tp", None), P(None), P(None, "tp"), P("dp", None, "tp"), P("dp", "tp", None)),
        out_specs=(P("dp", None, "tp"), P("dp", "tp", None), P(("dp", "tp"), None), P(None, ("dp", "tp")), P("dp")),
        check_vma=False,
    )
```

```python
import functools

import jax
import jax.numpy as jnp
from jax import lax
from jax.experimental import pallas as pl
from jax.experimental.pallas import tpu as pltpu
from jax.sharding import PartitionSpec as P

EPS = 1e-6
MESH = pl.DeviceIdType.MESH
F32 = jnp.float32
BF16 = jnp.bfloat16
ANY = pl.BlockSpec(memory_space=pl.ANY)
VM = pl.BlockSpec(memory_space=pltpu.VMEM)
SM = pl.BlockSpec(memory_space=pltpu.SMEM)
LIMIT = 60 * 1024 * 1024
NC = 6
HC = NC // 2
LATE = 1
EARLY = 2


def main_kernel(
    ids_ref, emb_ref, du_ref, w_ref, g_ref, dres_ref,
    xo_ref, n_ref, u_ref, dxo_ref, dxp_ref, dg_ref,
    idv, ev, oh, xp, xr, xfw, x1, x2, xh, xpr, drw, gv, wv, duv, pb, pr, sf, rf, r1, r2, nall, acc, ub, dxs, dxr, xov, dgo,
    dgm, dgr, dgc, dgn,
    id_s, e_s, du_s, g_s, w_s, dl_s, dr_s, dr_r, xd_s, xd_r, xo_s, xo_r, pd_s, pd_r,
    xa_s, xb_s, xc_s, xa_r, xb_r, xc_r, da_s, db_s, dc_s, da_r, db_r, dc_r,
    ga_s, gb_s, gc_s, ga_r, gb_r, gc_r, h0_s, h0_r, h1_s, h2_s, h3_s, h1_r, h2_r, h3_r,
    no_s, uo_s, dx_s, dx_r, ox_s, dg_s, dg_r,
):
    me = lax.axis_index("tp")
    c = me % 2
    q = me // 2
    xq = q % 2
    yq = q // 2
    qx = q + 1 - 2 * xq
    qy = q + 2 - 4 * yq
    qd = 3 - q
    part = me + 1 - 2 * c
    dx_ = me + 2 - 4 * xq
    dy_ = me + 4 - 8 * yq
    dd_ = 2 * qd + c
    oc = 1 - c
    d, f = w_ref.shape
    cw = d // NC
    vl = emb_ref.shape[0]
    tq = xr.shape[2]
    nt = 8 * tq
    th = tq // 2

    def w_copy(k):
        rows = pl.ds(pl.multiple_of(k * cw, cw), cw)
        return pltpu.make_async_copy(w_ref.at[rows], wv.at[k], w_s.at[k])

    def chunk(i):
        return i % 2 * HC + i // 2

    barrier = pltpu.get_barrier_semaphore()
    for dev in (part, dx_, dy_, dd_):
        pl.semaphore_signal(barrier, inc=1, device_id={"tp": dev}, device_id_type=MESH)

    id_copy = pltpu.make_async_copy(ids_ref, idv, id_s)
    def du_copy(m):
        return pltpu.make_async_copy(du_ref.at[m], duv.at[m], du_s.at[m])

    g_copy = pltpu.make_async_copy(g_ref, gv, g_s)
    dl_copy = pltpu.make_async_copy(dres_ref.at[c], drw.at[c], dl_s)
    def e_copy(i):
        cols = pl.ds(pl.multiple_of(chunk(i) * cw, cw), cw)
        return pltpu.make_async_copy(emb_ref.at[:, cols], ev.at[i % 2], e_s.at[i % 2])

    du_copy(oc).start()
    w_copy(chunk(0)).start()
    du_copy(c).start()
    w_copy(chunk(1)).start()
    id_copy.start()
    g_copy.start()
    dl_copy.start()

    def remote(src, dst, ss, rs, dev):
        return pltpu.make_async_remote_copy(
            src_ref=src, dst_ref=dst, send_sem=ss, recv_sem=rs, device_id={"tp": dev}, device_id_type=MESH
        )

    def xd(k):
        return remote(xp.at[k, oc], xr.at[k], xd_s.at[k], xd_r.at[k], part)

    dr = remote(dres_ref.at[oc], drw.at[c], dr_s, dr_r, part)

    def first(k):
        b = k // HC
        return qx + (qy - qx) * b, dx_ + (dy_ - dx_) * b

    def second(k):
        b = k // HC
        return qy + (qx - qy) * b, dy_ + (dx_ - dy_) * b

    def xa(k):
        return remote(xp.at[k, c, qd], xfw.at[k], xa_s.at[k], xa_r.at[k], first(k)[1])

    def xb(k):
        return remote(xp.at[k, c, first(k)[0]], x1.at[k], xb_s.at[k], xb_r.at[k], first(k)[1])

    def xc(k):
        return remote(xp.at[k, c, second(k)[0]], x2.at[k], xc_s.at[k], xc_r.at[k], second(k)[1])

    def da(k):
        return remote(sf.at[k, qd], rf.at[k], da_s.at[k], da_r.at[k], first(k)[1])

    def db(k):
        return remote(sf.at[k, first(k)[0]], r1.at[k], db_s.at[k], db_r.at[k], first(k)[1])

    def dc(k):
        return remote(sf.at[k, second(k)[0]], r2.at[k], dc_s.at[k], dc_r.at[k], second(k)[1])

    def pd(k):
        return remote(pb.at[k, oc], pr.at[k], pd_s.at[k], pd_r.at[k], part)

    def ga(k):
        return remote(nall.at[k, c, q], nall.at[k, c, q], ga_s.at[k], ga_r.at[k], first(k)[1])

    def gb(k):
        return remote(nall.at[k, c, q], nall.at[k, c, q], gb_s.at[k], gb_r.at[k], second(k)[1])

    def gc(k):
        s = first(k)[0]
        return remote(nall.at[k, c, s], nall.at[k, c, s], gc_s.at[k], gc_r.at[k], second(k)[1])

    def over(k, s, ss, rs):
        return remote(nall.at[k, c, s], nall.at[k, c, s], ss.at[k], rs.at[k], part)

    def h1(k):
        return over(k, first(k)[0], h1_s, h1_r)

    def h2(k):
        return over(k, second(k)[0], h2_s, h2_r)

    def h3(k):
        return over(k, qd, h3_s, h3_r)

    h0 = remote(nall.at[:, c, q], nall.at[:, c, q], h0_s, h0_r, part)

    def matmul(i):
        k = chunk(i)
        w_copy(k).wait()
        p = lax.dot_general(
            duv[...].reshape(nt, -1), wv[k], (((1,), (1,)), ((), ())), preferred_element_type=F32
        )
        pb[k] = p.astype(BF16).reshape(2, 4, tq, cw)
        pd(k).start()

    def combine(i):
        k = chunk(i)
        pd(k).wait_recv()
        for s in range(4):
            sf[k, s] = pb[k, c, s].astype(F32) + pr[k, s].astype(F32)
        da(k).start()

    k0 = chunk(0)
    w_copy(k0).wait()

    @pl.loop(2, NC)
    def _(i):
        w_copy(chunk(i)).start()

    for m in (oc, c):
        du_copy(m).wait()
        p = lax.dot_general(duv[m], wv[k0], (((1,), (1,)), ((), ())), preferred_element_type=F32)
        pb[k0, m] = p.astype(BF16).reshape(4, tq, cw)
        if m is oc:
            pl.semaphore_wait(barrier, 4)
            pd(k0).start()
            e_copy(0).start()
            e_copy(1).start()

    @pl.loop(1, NC)
    def _(i):
        matmul(i)
        combine(i - 1)

    id_copy.wait()
    lo = me * vl
    for b in range(nt // 128):
        m, t0 = divmod(b * 128, 4 * tq)
        row = idv[m : m + 1, t0 : t0 + 128] - lo
        col = jnp.broadcast_to(row, (128, 128)).T

        @pl.loop(0, vl // 128, unroll=8)
        def _(j):
            lanes = lax.broadcasted_iota(jnp.int32, (128, 128), 1) + j * 128
            cols = pl.ds(pl.multiple_of(j * 128, 128), 128)
            oh[b * 128 : (b + 1) * 128, cols] = jnp.where(lanes == col, 1.0, 0.0).astype(BF16)

    combine(NC - 1)
    dr.start()

    def lookup(i):
        k = chunk(i)
        e_copy(i).wait()
        p = jnp.dot(oh[...], ev[i % 2], preferred_element_type=F32)
        xp[k] = p.astype(BF16).reshape(2, 4, tq, cw)
        xd(k).start()

        @pl.when(i + 2 < NC)
        def _():
            e_copy(i + 2).start()

    def pair(i):
        k = chunk(i)
        xd(k).wait_recv()
        xp[k, c] = xp[k, c] + xr[k]
        xa(k).start()
        xb(k).start()

    def forward(i):
        k = chunk(i)
        s = second(k)[0]
        da(k).wait_recv()
        sf[k, s] = sf[k, s] + rf[k]
        dc(k).start()

    db(chunk(0)).start()
    db(chunk(1)).start()
    lookup(0)

    @pl.loop(1, NC)
    def _(i):
        @pl.when(i <= NC // 2)
        def _():
            db(chunk(i + 2)).start()

        @pl.when(i == 1)
        def _():
            db(chunk(2)).start()

        @pl.when(i == 2)
        def _():
            forward(0)

        @pl.when(i == 4)
        def _():
            forward(1)

        lookup(i)
        pair(i - 1)

    pair(NC - 1)

    @pl.loop(0, NC)
    def _(i):
        k = chunk(i)
        s = second(k)[0]
        xa(k).wait_recv()
        xp[k, c, s] = xp[k, c, s] + xfw[k]
        xc(k).start()

    @pl.loop(EARLY, NC)
    def _(i):
        forward(i)

    acc[...] = jnp.zeros_like(acc)

    g_copy.wait()
    sq = jnp.zeros((tq, 1), F32)
    for k in range(NC):
        xb(k).wait_recv()
        xc(k).wait_recv()
        xk = xp[k, c, q] + x1[k] + x2[k]
        xh[k] = xk
        xk = xk.astype(F32)
        sq = sq + jnp.sum(xk * xk, axis=-1, keepdims=True)
    xo = remote(xh.at[:, pl.ds(pl.multiple_of(oc * th, th), th), :], xpr, xo_s, xo_r, part)
    xo.start()
    rs = lax.rsqrt(sq * (1.0 / d) + EPS)
    for k in (0, 3, 1, 4, 2, 5):
        cols = slice(k * cw, (k + 1) * cw)
        nall[k, c, q] = ((xh[k].astype(F32) * rs) * gv[cols].astype(F32).reshape(1, cw)).astype(BF16)
        ga(k).start()
    for k in (0, 3, 1, 4, 2, 5):
        gb(k).start()
    h0.start()
    for k in range(NC):
        xov[c, :, k * cw : (k + 1) * cw] = xh[k, pl.ds(pl.multiple_of(c * th, th), th), :]
    dl_copy.wait()
    dr.wait_recv()
    xo.wait_recv()
    for k in range(NC):
        xov[oc, :, k * cw : (k + 1) * cw] = xpr[k]
    oz = pltpu.make_async_copy(xov, xo_ref, ox_s.at[2])
    oz.start()

    def piece(k, s):
        acc[:, s] += jnp.dot(nall[k, :, s].reshape(2 * tq, cw), wv[k], preferred_element_type=F32).reshape(2, tq, f)

    def u_out(j, s):
        ub[:, s] = acc[:, s].astype(BF16)
        return pltpu.make_async_copy(ub.at[:, s], u_ref.at[:, s], uo_s.at[j])

    h0.wait_recv()

    @pl.loop(0, NC)
    def _(k):
        piece(k, q)

    uo = [u_out(0, q)]
    uo[0].start()

    m = jnp.zeros((tq, 1), F32)
    for k in (0, 3, 1, 4, 2, 5):
        cols = slice(k * cw, (k + 1) * cw)
        db(k).wait_recv()
        dc(k).wait_recv()
        dn = sf[k, q] + r1[k] + r2[k]
        r1[k] = dn
        nh = xh[k].astype(F32) * rs
        dnh = dn * nh
        dgm[:, cols] = jnp.sum(dnh, axis=0, keepdims=True)
        m = m + jnp.sum(dnh * gv[cols].astype(F32).reshape(1, cw), axis=-1, keepdims=True)
    dg0 = remote(dgm, dgr, dg_s.at[0], dg_r.at[0], part)
    dg0.start()
    m = m * (1.0 / d)
    for k in range(NC):
        cols = slice(k * cw, (k + 1) * cw)
        nh = xh[k].astype(F32) * rs
        dxn = rs * (gv[cols].astype(F32).reshape(1, cw) * r1[k] - nh * m)
        dxs[k] = (drw[:, :, cols].reshape(tq, cw).astype(F32) + dxn).astype(BF16)
    dxc = remote(dxs, dxr, dx_s, dx_r, part)
    dxc.start()
    ox = pltpu.make_async_copy(dxs, dxo_ref, ox_s.at[0])
    ox.start()
    dg0.wait_recv()
    dgc[...] = dgm[...] + dgr[...]
    dgs = [remote(dgc, dgn.at[j], dg_s.at[1 + j], dg_r.at[1 + j], dev) for j, dev in enumerate((dx_, dy_, dd_))]
    for cp in dgs:
        cp.start()

    @pl.loop(0, NC)
    def _(i):
        k = chunk(i)
        ga(k).wait_recv()
        gc(k).start()
        h1(k).start()

    dxc.wait_recv()
    oy = pltpu.make_async_copy(dxr, dxp_ref, ox_s.at[1])
    oy.start()

    @pl.loop(0, NC)
    def _(i):
        k = chunk(i)
        h1(k).wait_recv()
        piece(k, first(k)[0])

    def n_out(k):
        return pltpu.make_async_copy(nall.at[k], n_ref.at[k], no_s.at[k])

    def second_in(i):
        k = chunk(i)
        gb(k).wait_recv()
        h2(k).start()

    def second_use(i):
        k = chunk(i)
        h2(k).wait_recv()
        piece(k, second(k)[0])

    def last_in(i):
        k = chunk(i)
        gc(k).wait_recv()
        h3(k).start()

    def last_use(i):
        k = chunk(i)
        h3(k).wait_recv()
        n_out(k).start()
        piece(k, qd)

    second_in(0)

    @pl.loop(1, NC)
    def _(i):
        second_in(i)
        second_use(i - 1)

    last_in(0)
    second_use(NC - 1)
    for j, s in enumerate((qx, qy)):
        uo.append(u_out(1 + j, s))
        uo[-1].start()

    @pl.loop(1, NC)
    def _(i):
        last_in(i)
        last_use(i - 1)

    for cp in dgs:
        cp.wait_recv()
    dgo[...] = (dgc[...] + dgn[0]) + (dgn[1] + dgn[2])
    og = pltpu.make_async_copy(dgo, dg_ref, ox_s.at[3])
    og.start()
    last_use(NC - 1)
    uo.append(u_out(3, qd))
    uo[-1].start()
    for cp in uo:
        cp.wait()

    for cp in (ox, oy, oz, og):
        cp.wait()
    dr.wait_send()
    xo.wait_send()
    h0.wait_send()
    dg0.wait_send()
    dxc.wait_send()
    for cp in dgs:
        cp.wait_send()

    @pl.loop(0, NC)
    def _(k):
        n_out(k).wait()
        for cp in (xd, pd, xa, xb, xc, da, db, dc, ga, gb, gc, h1, h2, h3):
            cp(k).wait_send()


def fill_kernel(
    ids_ref, idv_ref, n_ref, du_ref, u_ref, x_ref, dg_ref,
    row_ref, cnt_ref, sel_ref, dw_ref, de_ref, uo_ref, xo_ref, dgo_ref,
    nv, duv, st, z, uv, xv, gv, sel, fv, fs, n_s, du_s, o_s, z_s, p_s, f_s, *, rows,
):
    cw = nv.shape[2]
    zr = z.shape[0]
    mb, tm = idv_ref.shape
    nt = mb * tm
    vl = de_ref.shape[0]
    lo = lax.axis_index("tp") * vl
    du_copy = pltpu.make_async_copy(du_ref, duv, du_s)
    du_copy.start()

    def n_copy(k):
        return pltpu.make_async_copy(n_ref.at[k], nv.at[k], n_s.at[k])

    def out(k):
        r = pl.ds(pl.multiple_of(k * cw, cw), cw)
        return pltpu.make_async_copy(st.at[k % 2], dw_ref.at[r], o_s.at[k % 2])

    def put(i):
        return pltpu.make_async_copy(z, de_ref.at[pl.ds(pl.multiple_of(i * zr, zr), zr)], z_s)

    for k in range(NC):
        n_copy(k).start()
    small = ((u_ref, uv, uo_ref), (x_ref, xv, xo_ref), (dg_ref, gv, dgo_ref))
    ins = [pltpu.make_async_copy(a, v, p_s.at[j]) for j, (a, v, _) in enumerate(small)]
    outs = [pltpu.make_async_copy(v, o, p_s.at[j]) for j, (_, v, o) in enumerate(small)]
    for cp in ins:
        cp.start()
    z[...] = jnp.zeros_like(z)
    early = rows // zr - NC * LATE

    @pl.loop(0, early)
    def _(i):
        put(i).start()

    for m in range(mb):
        row = idv_ref[m : m + 1, :] - lo
        later = jnp.zeros((1, tm), jnp.int32)
        for b in range(nt // 128):
            m0, t0 = divmod(b * 128, tm)
            col = jnp.broadcast_to(idv_ref[m0 : m0 + 1, t0 : t0 + 128] - lo, (128, 128)).T
            col = jnp.concatenate([col] * (tm // 128), axis=1)
            pos = lax.broadcasted_iota(jnp.int32, (128, tm), 0) + b * 128
            mine = lax.broadcasted_iota(jnp.int32, (128, tm), 1) + m * tm
            hit = jnp.where((col == row) & (pos < mine), 1, 0)
            later = jnp.maximum(later, jnp.max(hit, axis=0, keepdims=True))
        fv[:, m * tm : (m + 1) * tm] = jnp.where((row >= 0) & (row < vl), 1 - later, 0)
    cp = pltpu.make_async_copy(fv, fs, f_s)
    cp.start()
    sel[...] = jnp.zeros_like(sel)
    cp.wait()

    def scan(t, n):
        row_ref[n] = ids_ref[t // tm, t % tm] - lo
        return n + fs[0, t]

    cnt = lax.fori_loop(0, nt, scan, jnp.int32(0), unroll=8)
    cnt_ref[0] = cnt

    @pl.loop(0, cnt)
    def _(j):
        v = row_ref[j] + lo
        for m in range(mb):
            sel[pl.ds(j, 1), m * tm : (m + 1) * tm] = jnp.where(idv_ref[m : m + 1, :] == v, 1.0, 0.0)

    sel_ref[...] = sel[...].astype(BF16)
    for cp, co in zip(ins, outs):
        cp.wait()
        co.start()
    du_copy.wait()

    @pl.loop(0, NC)
    def _(k):
        n_copy(k).wait()
        for j in range(LATE):
            put(early + k * LATE + j).start()

        @pl.when(k >= 2)
        def _():
            out(k - 2).wait()

        st[k % 2] = lax.dot_general(nv[k], duv[...], (((0,), (0,)), ((), ())), preferred_element_type=F32)
        out(k).start()

    for co in outs:
        co.wait()
    out(NC - 2).wait()
    out(NC - 1).wait()

    @pl.loop(0, rows // zr)
    def _(i):
        put(i).wait()


def rest_kernel(_, de_ref, z, z_s, *, rows):
    zr = z.shape[0]
    left = (de_ref.shape[0] - rows) // zr

    def put(i):
        return pltpu.make_async_copy(z, de_ref.at[pl.ds(pl.multiple_of(rows + i * zr, zr), zr)], z_s)

    z[...] = jnp.zeros_like(z)

    @pl.loop(0, left)
    def _(i):
        put(i).start()

    @pl.loop(0, left)
    def _(i):
        put(i).wait()


def rows_kernel(*refs):
    row_ref, cnt_ref, sel_ref = refs[:3]
    dx_refs = refs[3:11]
    _, de_ref, dxv, dxs, o_s = refs[11:]
    nt = sel_ref.shape[0]
    cw = dxv.shape[-1]
    rb = 128
    me = lax.axis_index("tp")
    c = me % 2
    q = me // 2
    qx = q + 1 - 2 * (q % 2)
    qy = q + 2 - 4 * (q // 2)
    where = [(b, s) for b in (c, 1 - c) for s in (q, qx, qy, 3 - q)]
    for r, (b, s) in zip(dx_refs, where):
        dxv[:, b, s] = r[...]
    cnt = cnt_ref[0]

    def put(j):
        return pltpu.make_async_copy(dxs.at[pl.ds(j, 1)], de_ref.at[pl.ds(row_ref[j], 1)], o_s)

    @pl.loop(0, (cnt + rb - 1) // rb)
    def _(b):
        r = pl.ds(pl.multiple_of(b * rb, rb), rb)
        for k in range(NC):
            dxs[r, k * cw : (k + 1) * cw] = jnp.dot(
                sel_ref[r, :], dxv[k].reshape(nt, cw), preferred_element_type=F32
            )

        @pl.loop(b * rb, jnp.minimum(b * rb + rb, cnt))
        def _(j):
            put(j).start()

    @pl.loop(0, cnt)
    def _(j):
        put(j).wait()


def solution(mesh):
    groups = mesh.shape["tp"]

    def shift(bit):
        return [(r, r ^ bit) for r in range(groups)]

    def send(a, bit):
        return lax.ppermute(a, "tp", shift(bit))

    def local(ids, emb, g, w, du, dres):
        mb, t = ids.shape
        vl, d = emb.shape
        f = w.shape[1]
        nt = mb * t
        cw = d // NC
        tq = t // 4
        dma = pltpu.SemaphoreType.DMA
        sds = jax.ShapeDtypeStruct
        vb = lambda *s: pltpu.VMEM(s, BF16)
        vf = lambda *s: pltpu.VMEM(s, F32)
        local_only = pltpu.CompilerParams(vmem_limit_bytes=LIMIT)

        blk = (NC, tq, cw)
        x, n, u, dxo, dxp, dg = pl.pallas_call(
            main_kernel,
            out_shape=(
                sds((2, tq // 2, d), BF16),
                sds((NC, 2, 4, tq, cw), BF16),
                sds((2, 4, tq, f), BF16),
                sds(blk, BF16),
                sds(blk, BF16),
                sds((1, d), F32),
            ),
            in_specs=[ANY] * 6,
            out_specs=(ANY,) * 6,
            scratch_shapes=[
                pltpu.VMEM((mb, t), jnp.int32), vb(2, vl, cw), vb(nt, vl),
                vb(NC, 2, 4, tq, cw), vb(NC, 4, tq, cw), vb(*blk), vb(*blk), vb(*blk),
                vb(*blk), vb(NC, tq // 2, cw), vb(2, tq // 2, d), vb(d),
                vb(NC, cw, f), vb(2, t, f),
                vb(NC, 2, 4, tq, cw), vb(NC, 4, tq, cw),
                vf(NC, 4, tq, cw), vf(*blk), vf(*blk), vf(*blk),
                vb(NC, 2, 4, tq, cw), vf(2, 4, tq, f), vb(2, 4, tq, f), vb(*blk), vb(*blk), vb(2, tq // 2, d), vf(1, d),
                vf(1, d), vf(1, d), vf(1, d), vf(3, 1, d),
                dma(()), dma((2,)), dma((2,)), dma(()), dma((NC,)), dma(()), dma(()), dma(()), dma((NC,)), dma((NC,)),
                dma(()), dma(()), dma((NC,)), dma((NC,)),
            ]
            + [dma((NC,))] * 18
            + [dma(())] * 2
            + [dma((NC,))] * 7
            + [dma((4,)), dma(()), dma(()), dma((4,)), dma((4,)), dma((4,))],
            compiler_params=pltpu.CompilerParams(collective_id=0, has_side_effects=True, vmem_limit_bytes=LIMIT),
            name="main",
        )(ids, emb, du, w, g, dres)

        zr = 128
        rows = vl // zr * 11 // 16 * zr
        near = [send(dxo, b) for b in (2, 4, 6)]
        row, cnt, sel, dw, de, u, x, dg = pl.pallas_call(
            functools.partial(fill_kernel, rows=rows),
            out_shape=(
                sds((nt + 8,), jnp.int32), sds((1,), jnp.int32), sds((nt, nt), BF16),
                sds((d, f), F32), sds((vl, d), F32), sds((nt, f), BF16), sds(x.shape, BF16), sds((1, d), F32),
            ),
            in_specs=[SM, VM] + [ANY] * 5,
            out_specs=(SM, SM, VM) + (ANY,) * 5,
            scratch_shapes=[
                vb(NC, nt, cw), vb(nt, f), vf(2, cw, f), vf(zr, d), vb(nt, f), vb(*x.shape), vf(1, d),
                vf(nt, nt), pltpu.VMEM((1, nt), jnp.int32), pltpu.SMEM((1, nt), jnp.int32),
                dma((NC,)), dma(()), dma((2,)), dma(()), dma((3,)), dma(()),
            ],
            compiler_params=local_only,
            cost_estimate=pl.CostEstimate(flops=18_000_000_000, bytes_accessed=vl * d * 4, transcendentals=0),
            name="fill",
        )(ids, ids, n.reshape(NC, nt, cw), du.reshape(nt, f), u.reshape(nt, f), x, dg)
        far = [send(a, 1) for a in near]

        de = pl.pallas_call(
            functools.partial(rest_kernel, rows=rows),
            out_shape=sds((vl, d), F32),
            in_specs=[ANY],
            out_specs=ANY,
            input_output_aliases={0: 0},
            scratch_shapes=[vf(zr, d), dma(())],
            compiler_params=pltpu.CompilerParams(vmem_limit_bytes=16 * 1024 * 1024),
            cost_estimate=pl.CostEstimate(flops=8_000_000_000, bytes_accessed=(vl - rows) * d * 4, transcendentals=0),
            name="rest",
        )(de)
        de = pl.pallas_call(
            rows_kernel,
            out_shape=sds((vl, d), F32),
            in_specs=[SM, SM, VM] + [VM] * 8 + [ANY],
            out_specs=ANY,
            input_output_aliases={11: 0},
            scratch_shapes=[vb(NC, 2, 4, tq, cw), vf(nt, d), dma(())],
            compiler_params=pltpu.CompilerParams(vmem_limit_bytes=24 * 1024 * 1024),
            name="rows",
        )(row, cnt, sel, dxo, *near, dxp, *far, de)
        return u.reshape(mb, t, f), x, de, dw, dg.reshape(d)

    return jax.shard_map(
        local,
        mesh=mesh,
        in_specs=(P("dp", None), P("tp", None), P(None), P(None, "tp"), P("dp", None, "tp"), P("dp", "tp", None)),
        out_specs=(P("dp", None, "tp"), P("dp", "tp", None), P(("dp", "tp"), None), P(None, ("dp", "tp")), P("dp")),
        check_vma=False,
    )
```
